32 devices in a mesh: lon: 2 (over x), lat: 4 (over y, core), head: 4 (over z).
Axes of the slice: x: 2, y: 2, z: 4, core: 2. Of those that a mesh axis runs over, the one named last changes fastest.
Arguments:
- features: bfloat16 [8, 24, 24, 384], P(None, 'lat', 'lon'), may hold values from -6 to 6
- attend_weight: bfloat16 [3, 384, 384], P(None, None, 'head'), may hold values from -0.3125 to 0.3125
- output_weight: bfloat16 [384, 384], P('head'), may hold values from -0.3125 to 0.3125
- bias_table: float32 [64, 12, 3312], P(None, 'head'), may hold values from -3 to 304
- bias_type: int32 [4, 4], P(None, 'lat'), may hold values from 0 to 63
- window_shift: int32 [1], replicated, may hold values from 1 to 11
- grad_out: bfloat16 [8, 24, 24, 384], P(None, 'lat', 'lon'), may hold values from -6 to 6
Outputs:
- feature_grad: bfloat16 [8, 24, 24, 384], P(None, 'lat', 'lon', 'head')
- attend_grad: float32 [3, 384, 384], P(None, None, 'head')
- output_grad: float32 [384, 384], P('head')
- bias_grad: float32 [64, 12, 3312], P(None, 'head')
The draws below stay inside these ranges and needn't reach their ends.
All inputs are finite; a program needn't handle non-finite values.
Results may differ from the reference program's by a relative error of at most 0.01.
Values may be sent and summed in bfloat16 or wider, within the bound.
No kernel may reach another device: no remote copies, remote signals or barrier semaphores. Data moves between devices by JAX's collectives and lax.ppermute only.
A program may use at most 128 MiB of HBM per device.

```python
import jax
import jax.numpy as jnp
import numpy as np
from jax import lax

D = 384
HEADS = 12
TYPES = 64
WIN_LEVEL = 2
WIN_LAT = 6
WIN_LON = 12
REL_COUNT = 3312
LEVELS = 8
LAT = 24
LON = 24
LEVEL_WINS = 4
LAT_WINS = 4
N_HEAD = 4


def draw_bias_table(key, part):
    base_key = jax.random.fold_in(key, 11)
    first_key = jax.random.fold_in(base_key, 0)
    table = jnp.clip(jax.random.normal(first_key, (TYPES, HEADS, REL_COUNT), jnp.float32), -3.0, 3.0)
    return table


def with_ends(values, key, smallest, top_value):
    spot = [jax.random.randint(jax.random.fold_in(key, axis), (), 0, length) for axis, length in enumerate(values.shape)]
    main_axis = values.shape.index(max(values.shape))
    next_to = spot[:main_axis] + [(spot[main_axis] + 1) % values.shape[main_axis]] + spot[main_axis + 1:]
    return values.at[tuple(spot)].set(smallest).at[tuple(next_to)].set(top_value)


def levels(rng, extent, shards, least, high):
    gain, own = 1.0, jax.random.fold_in(rng, 6)
    for dim, shards_of in shards:
        heights = jnp.exp(jax.random.uniform(jax.random.fold_in(own, dim), (shards_of,), jnp.float32, least / len(shards), high / len(shards)))
        gain = gain * jnp.repeat(heights, extent[dim] // shards_of).reshape([-1 if axis == dim else 1 for axis in range(len(extent))])
    return gain


def centred(own_key, dims, width, most, cuts=(), held_as=jnp.bfloat16):
    gain = levels(own_key, dims, cuts, -0.22, 0.18) if cuts else 1.0
    entries = jax.random.normal(own_key, dims, jnp.float32) * width * gain
    return jnp.minimum(jnp.maximum(entries, -most), most).astype(held_as)


def setup_inputs(seed: int = 0) -> dict:
    seeds = jax.random.split(jax.random.key(seed), 8)
    return {
        "features": centred(seeds[0], (LEVELS, LAT, LON, D), 1.0, 6.0, ((1, 4), (2, 2))),
        "attend_weight": centred(seeds[1], (3, D, D), D ** -0.5, 0.3125, ((2, 4),)),
        "output_weight": centred(seeds[2], (D, D), D ** -0.5, 0.3125, ((0, 4),)),
        "bias_table": draw_bias_table(jax.random.fold_in(seeds[7], 71), 0),
        "bias_type": with_ends(jax.random.randint(seeds[4], (LEVEL_WINS, LAT_WINS), 0, TYPES), jax.random.fold_in(seeds[4], 1), 0, TYPES - 1).astype(jnp.int32),
        "window_shift": jax.random.randint(seeds[5], (1,), 1, WIN_LON).astype(jnp.int32),
        "grad_out": centred(seeds[6], (LEVELS, LAT, LON, D), 1.0, 6.0, ((1, 4), (2, 2))),
    }


def relative_index(win_level, win_lat, win_lon):
    level_pos, lat_pos, lon_pos = np.meshgrid(np.arange(win_level), np.arange(win_lat), np.arange(win_lon), indexing="ij")
    level_pos = level_pos.reshape(-1)
    lat_pos = lat_pos.reshape(-1)
    lon_pos = lon_pos.reshape(-1)
    pair_level = level_pos[:, None] * win_level + level_pos[None, :]
    pair_lat = lat_pos[:, None] * win_lat + lat_pos[None, :]
    offset_lon = lon_pos[:, None] - lon_pos[None, :] + win_lon - 1
    combined = (pair_level * win_lat * win_lat + pair_lat) * (2 * win_lon - 1) + offset_lon
    return jnp.asarray(combined.reshape(-1).astype(np.int32))


def halve(values):
    return lax.optimization_barrier(values.astype(jnp.bfloat16)).astype(jnp.float32)


def attend_backward(tokens, grad_rows, window_types, attend_weight, output_weight, bias_table, relation):
    outer_count, inner_count, win_tokens, model_width = tokens.shape
    head_count = bias_table.shape[1]
    head_size = attend_weight.shape[2] // head_count
    scaling = head_size ** -0.5
    tokens_full = tokens.astype(jnp.float32)
    grad_full = grad_rows.astype(jnp.float32)
    projected = halve(jnp.einsum("abnd,cdk->cabnk", tokens_full, attend_weight.astype(jnp.float32)))
    split = projected.reshape(3, outer_count, inner_count, win_tokens, head_count, head_size)
    queries, key_rows, values = split[0], split[1], split[2]
    table_rows = jnp.take(bias_table, window_types, axis=0)
    bias_full = jnp.take(table_rows, relation, axis=2).reshape(outer_count, head_count, win_tokens, win_tokens)
    scores = jnp.einsum("abihe,abjhe->abhij", queries, key_rows) * scaling + bias_full[:, None]
    softened = jax.nn.softmax(scores, axis=-1)
    softened_half = halve(softened)
    attended = halve(jnp.einsum("abhij,abjhe->abihe", softened_half, values))
    grad_attended = halve(jnp.einsum("abnd,kd->abnk", grad_full, output_weight.astype(jnp.float32)))
    grad_heads = grad_attended.reshape(outer_count, inner_count, win_tokens, head_count, head_size)
    grad_values = halve(jnp.einsum("abhij,abihe->abjhe", softened_half, grad_heads))
    grad_softened = jnp.einsum("abihe,abjhe->abhij", grad_heads, values)
    grad_scores = softened * (grad_softened - jnp.sum(softened * grad_softened, axis=-1, keepdims=True))
    grad_scores_half = halve(grad_scores)
    grad_queries = halve(jnp.einsum("abhij,abjhe->abihe", grad_scores_half, key_rows) * scaling)
    grad_keys = halve(jnp.einsum("abhij,abihe->abjhe", grad_scores_half, queries) * scaling)
    grad_projected = jnp.stack([grad_queries, grad_keys, grad_values]).reshape(3, outer_count, inner_count, win_tokens, head_count * head_size)
    attended = attended.reshape(outer_count, inner_count, win_tokens, head_count * head_size)
    return attended, grad_projected, grad_scores


def reference(features, attend_weight, output_weight, bias_table, bias_type, window_shift, grad_out):
    offset = window_shift[0]
    rolled = jnp.roll(features, -offset, axis=2)
    rolled_grad = jnp.roll(grad_out, -offset, axis=2)
    relation = relative_index(WIN_LEVEL, WIN_LAT, WIN_LON)
    lon_wins = LON // WIN_LON
    level_wins = LEVELS // WIN_LEVEL
    win_tokens = WIN_LEVEL * WIN_LAT * WIN_LON
    head_count = bias_table.shape[1]
    rel_total = bias_table.shape[2]
    group_cols = D // N_HEAD

    def to_windows(band):
        shaped = band.reshape(level_wins, WIN_LEVEL, WIN_LAT, lon_wins, WIN_LON, D)
        return shaped.transpose(0, 3, 1, 2, 4, 5).reshape(level_wins, lon_wins, win_tokens, D)

    def from_windows(windows):
        shaped = windows.reshape(level_wins, lon_wins, WIN_LEVEL, WIN_LAT, WIN_LON, D)
        return shaped.transpose(0, 2, 3, 1, 4, 5).reshape(LEVELS, WIN_LAT, LON, D)

    def band_step(totals, band_index):
        grad_attend, grad_output, grad_bias = totals
        band_start = band_index * WIN_LAT
        tokens = to_windows(lax.dynamic_slice_in_dim(rolled, band_start, WIN_LAT, 1))
        grad_rows = to_windows(lax.dynamic_slice_in_dim(rolled_grad, band_start, WIN_LAT, 1))
        window_types = lax.dynamic_slice_in_dim(bias_type, band_index, 1, 1)[:, 0].astype(jnp.int32)
        attended, grad_projected, grad_scores = attend_backward(tokens, grad_rows, window_types, attend_weight, output_weight, bias_table, relation)
        tokens_full = tokens.astype(jnp.float32)
        grad_attend = grad_attend + jnp.einsum("abnd,cabnk->cdk", tokens_full, grad_projected)
        grad_output = grad_output + jnp.einsum("abnk,abnd->kd", attended, grad_rows.astype(jnp.float32))
        summed_scores = jnp.sum(grad_scores, axis=1).reshape(-1)
        segment_ids = (window_types[:, None, None] * head_count * rel_total + jnp.arange(head_count, dtype=jnp.int32)[None, :, None] * rel_total + relation[None, None, :]).reshape(-1)
        grad_bias = grad_bias + jax.ops.segment_sum(summed_scores, segment_ids, num_segments=bias_table.shape[0] * head_count * rel_total).reshape(bias_table.shape)
        grouped = grad_projected.reshape(3, level_wins, lon_wins, win_tokens, N_HEAD, group_cols)
        weight_grouped = attend_weight.astype(jnp.float32).reshape(3, D, N_HEAD, group_cols)
        pieces = halve(jnp.einsum("cabngk,cdgk->gabnd", grouped, weight_grouped))
        band_grad = from_windows(jnp.sum(pieces, axis=0)).astype(jnp.bfloat16)
        return (grad_attend, grad_output, grad_bias), band_grad

    start_totals = (jnp.zeros((3, D, D), jnp.float32), jnp.zeros((D, D), jnp.float32), jnp.zeros(bias_table.shape, jnp.float32))
    totals, bands = lax.scan(band_step, start_totals, jnp.arange(LAT // WIN_LAT, dtype=jnp.int32))
    grid_grad = bands.transpose(1, 0, 2, 3, 4).reshape(LEVELS, LAT, LON, D)
    feature_grad = jnp.roll(grid_grad, offset, axis=2)
    return feature_grad, totals[0], totals[1], totals[2]
```

```python
import jax
import jax.numpy as jnp
from jax import lax
from jax.experimental import pallas as pl
from jax.experimental.pallas import tpu as pltpu
from jax.sharding import PartitionSpec as P

WIN_LEVEL = 2
WIN_LAT = 6
WIN_LON = 12
ROWS = WIN_LEVEL * WIN_LAT
PAD = 16
WIDE = WIN_LON * PAD
TOKENS = WIN_LON * ROWS
OFFSETS = 2 * WIN_LON - 1
LANES = 128
MASKED = -1e30
F32 = jnp.float32
BF16 = jnp.bfloat16


def dot_nn(a, b):
    return lax.dot_general(a, b, (((1,), (0,)), ((), ())), preferred_element_type=F32)


def dot_nt(a, b):
    return lax.dot_general(a, b, (((1,), (1,)), ((), ())), preferred_element_type=F32)


def dot_tn(a, b):
    return lax.dot_general(a, b, (((0,), (0,)), ((), ())), preferred_element_type=F32)


def grid_of(rows, cols):
    shape = (rows, cols)
    return lax.broadcasted_iota(jnp.int32, shape, 0), lax.broadcasted_iota(jnp.int32, shape, 1)


def one_hot(hit):
    return jnp.where(hit, 1.0, 0.0).astype(BF16)


def split16(index):
    return lax.shift_right_logical(index, 4), lax.bitwise_and(index, 15)


def copy_rows(source_ref, rows_ref, slot):
    for level in range(WIN_LEVEL):
        for lat in range(WIN_LAT):
            start = (level * WIN_LAT + lat) * PAD
            rows_ref[start : start + WIN_LON, :] = source_ref[slot * WIN_LEVEL + level, lat]


def pack_kernel(shift_ref, x_ref, g_ref, out_ref, rows_ref):
    half = WIN_LON // 2
    base = jnp.where(shift_ref[0] <= half, 0, WIN_LON - half)
    row, src = grid_of(half * ROWS, ROWS * PAD)
    place, col = split16(src)
    col = col - base
    sel = one_hot((col >= 0) & (col < half) & (row == col * ROWS + place))
    for slot in range(out_ref.shape[1]):
        for array, ref in enumerate((x_ref, g_ref)):
            rows = rows_ref.at[array, slot]
            rows[...] = jnp.zeros(rows.shape, BF16)
            copy_rows(ref, rows, slot)
            out_ref[array, slot] = dot_nn(sel, rows[...]).astype(BF16)


def window_selectors(shift):
    half = WIN_LON // 2
    low = shift <= half
    row, src = grid_of(WIDE, ROWS * PAD)
    lon, place = split16(row)
    src_place, col = split16(src)
    target = lon + shift - jnp.where(low, 0, WIN_LON)
    local = (place == src_place) & (col == target) & (col < WIN_LON) & (place < ROWS)
    row, src = grid_of(WIDE, half * ROWS)
    lon, place = split16(row)
    col = lon + shift - jnp.where(low, WIN_LON, WIN_LON - half)
    taken = (src == col * ROWS + place) & (place < ROWS)
    borrowed = taken & (col >= 0) & (low | (lon + shift < WIN_LON))
    return one_hot(local), one_hot(borrowed)


def main_kernel(
    shift_ref, x_ref, g_ref, far_ref, weight_ref, out_weight_ref, table_ref, *rest
):
    n_head = lax.axis_size("head")
    pieces = rest[:n_head]
    sums_ref, folded_ref, rows_ref, bias_ref = rest[n_head:]
    width = out_weight_ref.shape[0]
    heads = table_ref.shape[1] // PAD
    size = width // heads
    scaling = size ** (-0.5)
    mine = lax.axis_index("head")
    local, borrowed = window_selectors(shift_ref[0])
    row, src = grid_of(TOKENS, WIDE)
    lon, place = split16(src)
    compact = one_hot((row == lon * ROWS + place) & (place < ROWS))
    lane = lax.broadcasted_iota(jnp.int32, (WIDE, width), 1)
    masks = [(lane >= h * size) & (lane < (h + 1) * size) for h in range(heads)]
    span = table_ref.shape[2]
    sums = [jnp.zeros((width, x_ref.shape[3]), F32) for _ in range(4)]
    rows_ref[...] = jnp.zeros(rows_ref.shape, BF16)
    for slot in range(table_ref.shape[0]):
        copy_rows(x_ref, rows_ref.at[0], slot)
        copy_rows(g_ref, rows_ref.at[1], slot)
        tokens = (dot_nn(local, rows_ref[0]) + dot_nn(borrowed, far_ref[0, slot])).astype(BF16)
        grads = (dot_nn(local, rows_ref[1]) + dot_nn(borrowed, far_ref[1, slot])).astype(BF16)
        query = dot_nn(tokens, weight_ref[0]).astype(BF16)
        key = dot_nn(tokens, weight_ref[1]).astype(BF16)
        value = dot_nn(tokens, weight_ref[2]).astype(BF16)
        grad_attended = dot_nt(grads, out_weight_ref[...]).astype(BF16)
        table = table_ref[slot]
        for lon_i in range(WIN_LON):
            by = (WIN_LON - 1 - lon_i) * PAD
            turned = table if by == 0 else pltpu.roll(table, span - by, 1)
            for h in range(heads):
                bias_ref[h, lon_i * PAD : (lon_i + 1) * PAD, :] = turned[
                    h * PAD : (h + 1) * PAD, :WIDE
                ]
        attended = jnp.zeros((WIDE, width), F32)
        grad_query = jnp.zeros((WIDE, width), F32)
        grad_key = jnp.zeros((WIDE, width), F32)
        grad_value = jnp.zeros((WIDE, width), F32)
        for h in range(heads):
            query_h = jnp.where(masks[h], query, jnp.zeros_like(query))
            key_h = jnp.where(masks[h], key, jnp.zeros_like(key))
            value_h = jnp.where(masks[h], value, jnp.zeros_like(value))
            grad_h = jnp.where(masks[h], grad_attended, jnp.zeros_like(grad_attended))
            scores = dot_nt(query_h, key) * scaling + bias_ref[h]
            raised = jnp.exp(scores - jnp.max(scores, axis=1, keepdims=True))
            softened = raised * (1.0 / jnp.sum(raised, axis=1, keepdims=True))
            softened_half = softened.astype(BF16)
            attended = attended + dot_nn(softened_half, value_h)
            grad_value = grad_value + dot_tn(softened_half, grad_h)
            grad_softened = dot_nt(grad_h, value)
            inner = jnp.sum(softened * grad_softened, axis=1, keepdims=True)
            grad_scores = softened * (grad_softened - inner)
            grad_half = grad_scores.astype(BF16)
            grad_query = grad_query + dot_nn(grad_half, key_h)
            grad_key = grad_key + dot_tn(grad_half, query_h)
            padded = jnp.concatenate(
                [grad_scores, jnp.zeros((WIDE, span - WIDE), F32)], axis=1
            )
            total = jnp.zeros((PAD, span), F32)
            for lon_i in range(WIN_LON):
                by = (WIN_LON - 1 - lon_i) * PAD
                part = padded[lon_i * PAD : (lon_i + 1) * PAD, :]
                total = total + (part if by == 0 else pltpu.roll(part, by, 1))
            folded_ref[slot, h * PAD : (h + 1) * PAD, :] = total
        projected = [
            (grad_query * scaling).astype(BF16),
            (grad_key * scaling).astype(BF16),
            grad_value.astype(BF16),
        ]
        for c in range(3):
            sums[c] = sums[c] + dot_tn(projected[c], tokens)
        sums[3] = sums[3] + dot_tn(attended.astype(BF16), grads)
        packed = [dot_nn(compact, part).astype(BF16) for part in projected]
        for step in range(n_head):
            to = lax.rem(mine + step, n_head)
            start = pl.multiple_of(to * width, 16)
            piece = jnp.zeros((TOKENS, width), F32)
            for c in range(3):
                piece = piece + dot_nt(packed[c], weight_ref[c, pl.ds(start, width), :])
            pieces[step][slot * TOKENS : (slot + 1) * TOKENS, :] = piece.astype(BF16)
    for c in range(4):
        sums_ref[c] = sums[c].astype(BF16)


def sum_kernel(shift_ref, *refs):
    parts = refs[:-2]
    summed_ref, back_ref = refs[-2:]
    half = WIN_LON // 2
    shift = shift_ref[0]
    low = shift <= half
    row, src = grid_of(half * ROWS, TOKENS)
    by = (shift - jnp.where(low, WIN_LON, WIN_LON - half)) * ROWS
    back = one_hot((row == src + by) & (low | (src < (WIN_LON - shift) * ROWS)))
    for slot in range(summed_ref.shape[0] // TOKENS):
        at = slice(slot * TOKENS, (slot + 1) * TOKENS)
        total = parts[0][at, :].astype(F32)
        for part in parts[1:]:
            total = total + part[at, :].astype(F32)
        total = total.astype(BF16)
        summed_ref[at, :] = total
        count = half * ROWS
        back_ref[slot * count : (slot + 1) * count, :] = dot_nn(back, total).astype(BF16)


def place_kernel(shift_ref, summed_ref, back_ref, out_ref):
    half = WIN_LON // 2
    shift = shift_ref[0]
    low = shift <= half
    row, src = grid_of(ROWS * PAD, TOKENS)
    place, col = split16(row)
    lon = col - shift + jnp.where(low, 0, WIN_LON)
    own = one_hot(
        (src == lon * ROWS + place) & (lon >= 0) & (col < WIN_LON) & (low | (col < shift))
    )
    row, src = grid_of(ROWS * PAD, half * ROWS)
    place, col = split16(row)
    given = col - jnp.where(low, 0, WIN_LON - half)
    other = one_hot(
        (src == given * ROWS + place)
        & ((low & (col < shift)) | (~low & (col >= shift) & (col < WIN_LON)))
    )
    count = half * ROWS
    for slot in range(summed_ref.shape[0] // TOKENS):
        placed = dot_nn(own, summed_ref[slot * TOKENS : (slot + 1) * TOKENS, :]) + dot_nn(
            other, back_ref[slot * count : (slot + 1) * count, :]
        )
        placed = placed.astype(BF16)
        for level in range(WIN_LEVEL):
            for lat in range(WIN_LAT):
                start = (level * WIN_LAT + lat) * PAD
                out_ref[slot * WIN_LEVEL + level, lat] = placed[start : start + WIN_LON, :]


def finish_kernel(rows_ref, sums_ref, bias_ref, attend_ref, output_ref):
    types, heads, count = bias_ref.shape
    width = output_ref.shape[0]
    for c in range(3):
        attend_ref[c] = sums_ref[c * width : (c + 1) * width, :].astype(F32).T
    output_ref[...] = sums_ref[3 * width :, :].astype(F32)
    kind = rows_ref[:, count : count + 1].astype(F32)
    head = rows_ref[:, count + 1 : count + 2].astype(F32)
    lane = lax.broadcasted_iota(jnp.int32, (rows_ref.shape[0], types), 1).astype(F32)
    for h in range(heads):
        sel = one_hot((kind == lane) & (head == float(h)))
        bias_ref[:, h, :] = dot_tn(sel, rows_ref[:, :count])


SMEM = pl.BlockSpec(memory_space=pltpu.SMEM)
VMEM = pl.BlockSpec(memory_space=pltpu.VMEM)


def exchange(x, axis, shift, sign):
    count = lax.axis_size(axis)
    ahead = lax.ppermute(x, axis, [(i, (i - sign) % count) for i in range(count)])
    if count == 2:
        return ahead
    behind = lax.ppermute(x, axis, [(i, (i + sign) % count) for i in range(count)])
    return jnp.where(shift[0] <= WIN_LON // 2, ahead, behind)


def table_rows(bias_table, kinds):
    slots, heads = kinds.shape[0], bias_table.shape[1]
    chosen = jnp.take(bias_table, kinds, axis=0)
    shaped = chosen.reshape(slots, heads, WIN_LEVEL, WIN_LEVEL, WIN_LAT, WIN_LAT, OFFSETS)
    turned = shaped[..., ::-1].transpose(0, 1, 2, 4, 6, 3, 5)
    turned = turned.reshape(slots, heads, ROWS, OFFSETS, ROWS)
    turned = jnp.pad(turned, ((0, 0),) * 4 + ((0, PAD - ROWS),), constant_values=MASKED)
    turned = turned.reshape(slots, heads, ROWS, OFFSETS * PAD)
    span = -(-OFFSETS * PAD // LANES) * LANES
    edges = ((0, 0), (0, 0), (0, PAD - ROWS), (0, span - OFFSETS * PAD))
    return jnp.pad(turned, edges).reshape(slots, heads * PAD, span)


def natural_rows(folded, kinds, heads):
    slots = folded.shape[0]
    shaped = folded[:, :, : OFFSETS * PAD].reshape(slots, heads, PAD, OFFSETS, PAD)
    shaped = shaped[:, :, :ROWS, ::-1, :ROWS]
    shaped = shaped.reshape(slots, heads, WIN_LEVEL, WIN_LAT, OFFSETS, WIN_LEVEL, WIN_LAT)
    rows = shaped.transpose(0, 1, 2, 5, 3, 6, 4).reshape(slots * heads, -1).astype(BF16)
    kind = jnp.repeat(kinds, heads).astype(BF16)
    head = jnp.tile(jnp.arange(heads), slots).astype(BF16)
    extra = -rows.shape[1] % LANES
    tail = jnp.stack([kind, head] + [jnp.zeros_like(kind)] * (extra - 2), axis=1)
    return jnp.concatenate([rows, tail], axis=1)


def per_device(
    features, attend_weight, output_weight, bias_table, bias_type, window_shift, grad_out
):
    levels, lat_rows, lon_cols, model_width = features.shape
    assert lat_rows == WIN_LAT and lon_cols == WIN_LON and levels % WIN_LEVEL == 0
    slots = levels // WIN_LEVEL
    width, heads = output_weight.shape[0], bias_table.shape[1]
    half_rows = WIN_LON // 2 * ROWS
    n_head = lax.axis_size("head")
    kinds = bias_type[:, 0]
    shape = jax.ShapeDtypeStruct
    slab = pl.pallas_call(
        pack_kernel,
        name="pack",
        out_shape=shape((2, slots, half_rows, model_width), BF16),
        in_specs=[SMEM, VMEM, VMEM],
        out_specs=VMEM,
        scratch_shapes=[pltpu.VMEM((2, slots, ROWS * PAD, model_width), BF16)],
    )(window_shift, features, grad_out)
    far = exchange(slab, "lon", window_shift, 1)
    table = table_rows(bias_table, kinds)
    *pieces, sums, folded = pl.pallas_call(
        main_kernel,
        name="main",
        out_shape=[shape((slots * TOKENS, width), BF16)] * n_head
        + [
            shape((4, width, model_width), BF16),
            shape(table.shape, F32),
        ],
        in_specs=[SMEM] + [VMEM] * 6,
        out_specs=[VMEM] * (n_head + 2),
        scratch_shapes=[
            pltpu.VMEM((2, ROWS * PAD, model_width), BF16),
            pltpu.VMEM((heads, WIDE, WIDE), F32),
        ],
    )(window_shift, features, grad_out, far, attend_weight, output_weight, table)
    parts = [pieces[0]]
    for step in range(1, n_head):
        ring = [(i, (i + step) % n_head) for i in range(n_head)]
        parts.append(lax.ppermute(pieces[step], "head", ring))
    summed, back = pl.pallas_call(
        sum_kernel,
        name="sum_heads",
        out_shape=[
            shape((slots * TOKENS, width), BF16),
            shape((slots * half_rows, width), BF16),
        ],
        in_specs=[SMEM] + [VMEM] * n_head,
        out_specs=[VMEM] * 2,
    )(window_shift, *parts)
    returned = exchange(back, "lon", window_shift, -1)
    feature_grad = pl.pallas_call(
        place_kernel,
        name="place",
        out_shape=shape((levels, lat_rows, lon_cols, width), BF16),
        in_specs=[SMEM, VMEM, VMEM],
        out_specs=VMEM,
    )(window_shift, summed, returned)
    every = ("lon", "lat")
    n_every = lax.axis_size("lon") * lax.axis_size("lat")
    shares = sums.reshape(n_every, 4 * width // n_every, model_width)
    shares = lax.all_to_all(shares, every, 0, 0)
    share = jnp.sum(shares.astype(F32), axis=0).astype(BF16)
    sums = lax.all_gather(share, every, axis=0, tiled=True)
    rows = lax.all_gather(natural_rows(folded, kinds, heads), every, axis=0, tiled=True)
    bias_grad, attend_grad, output_grad = pl.pallas_call(
        finish_kernel,
        name="finish",
        out_shape=[
            shape(bias_table.shape, F32),
            shape(attend_weight.shape, F32),
            shape(output_weight.shape, F32),
        ],
        in_specs=[VMEM] * 2,
        out_specs=[VMEM] * 3,
    )(rows, sums)
    return (feature_grad, attend_grad, output_grad, bias_grad)


def solution(mesh):
    placed = (
        P(None, "lat", "lon", None),
        P(None, None, "head"),
        P("head", None),
        P(None, "head", None),
        P(None, "lat"),
        P(),
        P(None, "lat", "lon", None),
    )
    return jax.shard_map(
        per_device,
        mesh=mesh,
        in_specs=placed,
        out_specs=(
            P(None, "lat", "lon", "head"),
            P(None, None, "head"),
            P("head", None),
            P(None, "head", None),
        ),
        check_vma=False,
    )
```

```python
import jax
import jax.numpy as jnp
from jax import lax
from jax.experimental import pallas as pl
from jax.experimental.pallas import tpu as pltpu
from jax.sharding import PartitionSpec as P

WIN_LEVEL = 2
WIN_LAT = 6
WIN_LON = 12
ROWS = WIN_LEVEL * WIN_LAT
PAD = 16
WIDE = WIN_LON * PAD
HALF = WIN_LON // 2
OFFSETS = 2 * WIN_LON - 1
PIECE = WIN_LAT * OFFSETS
LANES = 128
SPAN = -(-OFFSETS * PAD // LANES) * LANES
MASKED = -1e30
F32 = jnp.float32
BF16 = jnp.bfloat16
SMEM = pl.BlockSpec(memory_space=pltpu.SMEM)
VMEM = pl.BlockSpec(memory_space=pltpu.VMEM)
ANY = pl.BlockSpec(memory_space=pl.ANY)


def dot_nn(a, b):
    return lax.dot_general(a, b, (((1,), (0,)), ((), ())), preferred_element_type=F32)


def dot_nt(a, b):
    return lax.dot_general(a, b, (((1,), (1,)), ((), ())), preferred_element_type=F32)


def dot_tn(a, b):
    return lax.dot_general(a, b, (((0,), (0,)), ((), ())), preferred_element_type=F32)


def grid_of(rows, cols):
    shape = (rows, cols)
    return lax.broadcasted_iota(jnp.int32, shape, 0), lax.broadcasted_iota(jnp.int32, shape, 1)


def one_hot(hit):
    return jnp.where(hit, 1.0, 0.0).astype(BF16)


def window_order(levels):
    row, src = grid_of(levels // WIN_LEVEL * PAD, WIN_LAT * levels)
    bits = levels.bit_length() - 1
    lat = lax.shift_right_logical(src, bits)
    level = lax.bitwise_and(src, levels - 1)
    slot = lax.shift_right_logical(level, 1)
    return one_hot(row == slot * PAD + lax.bitwise_and(level, 1) * WIN_LAT + lat)


def offset_order(level_j):
    src, lane = grid_of(2 * LANES, SPAN)
    back = lax.shift_right_logical(lane, 4)
    lat = lax.bitwise_and(lane, PAD - 1) - level_j * WIN_LAT
    hit = (src == lat * OFFSETS + OFFSETS - 1 - back) & (lat >= 0) & (lat < WIN_LAT)
    return one_hot(hit & (back < OFFSETS))


def table_pieces():
    for level_i in range(WIN_LEVEL):
        for level_j in range(WIN_LEVEL):
            for lat_i in range(WIN_LAT):
                index = (level_i * WIN_LEVEL + level_j) * WIN_LAT + lat_i
                yield level_i * WIN_LAT + lat_i, level_j, index * PIECE


def pack_kernel(shift_ref, x_ref, g_ref, out_ref, sems):
    base = jnp.where(shift_ref[0] <= HALF, 0, WIN_LON - HALF)
    copies = [
        pltpu.make_async_copy(ref.at[:, pl.ds(base, HALF)], out_ref.at[i], sems.at[i])
        for i, ref in enumerate((x_ref, g_ref))
    ]
    for copy in copies:
        copy.start()
    for copy in copies:
        copy.wait()


def project(rows_x, rows_g, weights):
    width = 3 * LANES
    return jnp.concatenate(
        [dot_nt(rows_x, weights[:width]), dot_nt(rows_g, weights[width:])], axis=1
    )


def prepare_kernel(
    kind_ref, x_ref, g_ref, weight_ref, out_weight_ref, table_ref,
    turned_ref, projected_ref, weights_ref, natural_ref, pieces_ref,
):
    lats, cols, levels, depth = x_ref.shape
    heads = table_ref.shape[0]
    slots = kind_ref.shape[0]
    count = table_ref.shape[2]
    width = out_weight_ref.shape[0]
    weights_ref[...] = jnp.zeros(weights_ref.shape, BF16)
    for c in range(3):
        weights_ref[c * LANES : c * LANES + width, :] = weight_ref[c]
    weights_ref[3 * LANES : 3 * LANES + width, :] = out_weight_ref[...]
    flat = (lats * cols * levels, depth)
    projected = project(x_ref[...].reshape(flat), g_ref[...].reshape(flat), weights_ref[...])
    for lat in range(lats):
        for col in range(cols):
            start = (lat * cols + col) * levels
            projected_ref[col, lat * levels : (lat + 1) * levels, :] = projected[
                start : start + levels, :
            ].astype(BF16)
    natural_ref[...] = jnp.zeros(natural_ref.shape, F32)
    pieces_ref[...] = jnp.zeros(pieces_ref.shape, F32)
    for h in range(heads):
        for slot in range(slots):
            row = h * slots + slot
            natural_ref[row : row + 1, :count] = table_ref[h, pl.ds(kind_ref[slot, 0], 1), :]
    number = heads * slots
    for place, level_j, start in table_pieces():
        low = start // LANES * LANES
        block = natural_ref[:, low : low + 3 * LANES]
        if start > low:
            block = pltpu.roll(block, 3 * LANES - (start - low), 1)
        for t in range(2):
            pieces_ref[2 * level_j + t, pl.ds(place, number, stride=PAD), :] = block[
                :number, t * LANES : (t + 1) * LANES
            ]
    turned = jnp.zeros((number * PAD, SPAN), F32)
    for level_j in range(WIN_LEVEL):
        order = offset_order(level_j)
        rest = jnp.concatenate([pieces_ref[2 * level_j], pieces_ref[2 * level_j + 1]], axis=1)
        for _ in range(3):
            part = rest.astype(BF16)
            turned = turned + dot_nn(part, order)
            rest = rest - part.astype(F32)
    lane = lax.broadcasted_iota(jnp.int32, turned.shape, 1)
    turned = jnp.where(lax.bitwise_and(lane, PAD - 1) < ROWS, turned, MASKED)
    for h in range(heads):
        turned_ref[h] = turned[h * slots * PAD : (h + 1) * slots * PAD, :]


def main_kernel(
    shift_ref, x_ref, g_ref, far_ref, near_ref, weights_ref, turned_ref, *rest
):
    n_head = lax.axis_size("head")
    pieces = rest[:n_head]
    sums_ref, folded_ref = rest[n_head : n_head + 2]
    beyond_ref, own_ref, ordered_ref, bias_ref, given_ref, back_ref, chunk_ref = rest[n_head + 2 :]
    lats, cols, levels, depth = x_ref.shape
    width = sums_ref.shape[1]
    heads, slot_rows = turned_ref.shape[0], turned_ref.shape[1]
    slots = slot_rows // PAD
    size = width // heads
    scaling = size ** (-0.5)
    mine = lax.axis_index("head")
    shift = shift_ref[0]
    low = shift <= HALF
    tall = lats * levels
    flat = (lats * HALF * levels, depth)
    projected = project(far_ref[0].reshape(flat), far_ref[1].reshape(flat), weights_ref[...])
    for lat in range(lats):
        for col in range(HALF):
            start = (lat * HALF + col) * levels
            beyond_ref[col, lat * levels : (lat + 1) * levels, :] = projected[
                start : start + levels, :
            ].astype(BF16)
    order = window_order(levels)
    for col in range(cols):
        at = col + shift
        inside = jnp.logical_xor(low, at >= cols)
        local = jnp.where(at >= cols, at - cols, at)
        taken = jnp.where(low, at - cols, at - (cols - HALF))
        taken = jnp.clip(taken, 0, HALF - 1)
        rows = jnp.where(inside, near_ref[local], beyond_ref[taken])
        ordered = dot_nn(order, rows).astype(BF16)
        for slot in range(slots):
            ordered_ref[slot, col * PAD : (col + 1) * PAD, :] = ordered[
                slot * PAD : (slot + 1) * PAD, :
            ]
        for array, ref in enumerate((x_ref, g_ref)):
            for lat in range(lats):
                start = col * tall + lat * levels
                own_ref[array, start : start + levels, :] = jnp.where(
                    inside, ref[lat, local], far_ref[array, lat, taken]
                )
    lane = lax.broadcasted_iota(jnp.int32, (WIDE, LANES), 1)
    masks = [(lane >= h * size) & (lane < (h + 1) * size) for h in range(heads)]
    none = jnp.zeros((WIDE, LANES), BF16)
    for slot in range(slots):
        query = ordered_ref[slot, :, :LANES]
        key = ordered_ref[slot, :, LANES : 2 * LANES]
        value = ordered_ref[slot, :, 2 * LANES : 3 * LANES]
        grad_attended = ordered_ref[slot, :, 3 * LANES :]
        at = slice(slot * PAD, (slot + 1) * PAD)
        attended = jnp.zeros((WIDE, LANES), F32)
        grad_query = jnp.zeros((WIDE, LANES), F32)
        grad_key = jnp.zeros((WIDE, LANES), F32)
        grad_value = jnp.zeros((WIDE, LANES), F32)
        for h in range(heads):
            table = turned_ref[h, at, :]
            for col in range(WIN_LON):
                by = (WIN_LON - 1 - col) * PAD
                moved = table if by == 0 else pltpu.roll(table, SPAN - by, 1)
                bias_ref[h, col * PAD : (col + 1) * PAD, :] = moved[:, :WIDE]
            query_h = jnp.where(masks[h], query, none)
            key_h = jnp.where(masks[h], key, none)
            value_h = jnp.where(masks[h], value, none)
            grad_h = jnp.where(masks[h], grad_attended, none)
            scores = dot_nt(query_h, key) * scaling + bias_ref[h]
            raised = jnp.exp(scores - jnp.max(scores, axis=1, keepdims=True))
            softened = raised * (1.0 / jnp.sum(raised, axis=1, keepdims=True))
            softened_half = softened.astype(BF16)
            attended = attended + dot_nn(softened_half, value_h)
            grad_value = grad_value + dot_tn(softened_half, grad_h)
            grad_softened = dot_nt(grad_h, value)
            inner = jnp.sum(softened * grad_softened, axis=1, keepdims=True)
            grad_scores = softened * (grad_softened - inner)
            grad_half = grad_scores.astype(BF16)
            grad_query = grad_query + dot_nn(grad_half, key_h)
            grad_key = grad_key + dot_tn(grad_half, query_h)
            padded = jnp.concatenate([grad_scores, jnp.zeros((WIDE, SPAN - WIDE), F32)], axis=1)
            total = jnp.zeros((PAD, SPAN), F32)
            for col in range(WIN_LON):
                by = (WIN_LON - 1 - col) * PAD
                part = padded[col * PAD : (col + 1) * PAD, :]
                total = total + (part if by == 0 else pltpu.roll(part, by, 1))
            folded_ref[h, at, :] = total
        results = (grad_query * scaling, grad_key * scaling, grad_value, attended)
        for c, result in enumerate(results):
            rounded = result.astype(BF16)
            for col in range(WIN_LON):
                given_ref[col, at, c * LANES : (c + 1) * LANES] = rounded[
                    col * PAD : (col + 1) * PAD, :
                ]
    for col in range(WIN_LON):
        back_ref[col * tall : (col + 1) * tall, :] = dot_tn(order, given_ref[col]).astype(BF16)
    grads = 3 * LANES
    piece = dot_nn(back_ref[:, :grads], weights_ref[:grads, :])
    group = WIN_LON // 4 * tall
    third = width // 3
    for to in range(n_head):
        lanes = piece[:, to * width : (to + 1) * width]
        for g in range(3):
            tail = lanes[3 * group :, g * third : (g + 1) * third]
            chunk_ref[to, g * group : (g + 1) * group, :] = jnp.concatenate(
                [lanes[g * group : (g + 1) * group, :], tail], axis=1
            ).astype(BF16)
    for step in range(n_head):
        pieces[step][...] = chunk_ref[lax.rem(mine + step, n_head)]
    summed = dot_tn(back_ref[:, :grads], own_ref[0])
    for c in range(3):
        sums_ref[c] = summed[c * LANES : c * LANES + width, :].astype(BF16)
    sums_ref[3] = dot_tn(back_ref[:, grads:], own_ref[1])[:width, :].astype(BF16)


def bias_kernel(kind_ref, folded_ref, out_ref, pieces_ref, natural_ref, dense_ref):
    heads, slot_rows, span = folded_ref.shape
    slots = slot_rows // PAD
    number = heads * slots
    rows = folded_ref[...].reshape(heads * slot_rows, span).astype(BF16)
    for level_j in range(WIN_LEVEL):
        moved = dot_nt(rows, offset_order(level_j))
        for t in range(2):
            pieces_ref[2 * level_j + t] = moved[:, t * LANES : (t + 1) * LANES]
    natural_ref[...] = jnp.zeros(natural_ref.shape, F32)
    for place, level_j, start in table_pieces():
        low = start // LANES * LANES
        parts = [
            pieces_ref[2 * level_j + t, pl.ds(place, number, stride=PAD), :] for t in range(2)
        ]
        part = jnp.concatenate(parts + [jnp.zeros((number, LANES), F32)], axis=1)
        if start > low:
            part = pltpu.roll(part, start - low, 1)
        at = (slice(0, number), slice(low, low + 3 * LANES))
        natural_ref[at] = natural_ref[at] + part
    count = WIN_LEVEL * WIN_LEVEL * WIN_LAT * PIECE
    low = count // LANES * LANES
    row, lane = grid_of(number, LANES)
    kind = jnp.zeros((number, LANES), F32)
    for slot in range(slots):
        kind = jnp.where(lax.rem(row, slots) == slot, kind_ref[slot, 0].astype(F32), kind)
    at = (slice(0, number), slice(low, low + LANES))
    natural_ref[at] = natural_ref[at] + jnp.where(lane == count - low, kind, 0.0)
    full = low + LANES
    middle = full // 2
    dense_ref[:, :full] = natural_ref[0:8, :full]
    dense_ref[0:4, full:] = natural_ref[8:12, :middle]
    dense_ref[4:8, full:] = natural_ref[8:12, middle:full]
    wide = out_ref.shape[1]
    for j in range(out_ref.shape[0] // 8):
        out_ref[j * 8 : (j + 1) * 8, :] = dense_ref[:, j * wide : (j + 1) * wide].astype(BF16)


def sum_kernel(shift_ref, *refs):
    parts = refs[:-2]
    summed_ref, back_ref = refs[-2:]
    shift = shift_ref[0]
    total = parts[0][...].astype(F32)
    for part in parts[1:]:
        total = total + part[...].astype(F32)
    cols, tall, width = summed_ref.shape
    group = cols // 4
    for g in range(3):
        for i in range(group):
            start = (g * group + i) * tall
            summed_ref[g * group + i] = total[start : start + tall, :width].astype(BF16)
    for i in range(group):
        tails = [
            total[(g * group + i) * tall : (g * group + i + 1) * tall, width:] for g in range(3)
        ]
        summed_ref[3 * group + i] = jnp.concatenate(tails, axis=1).astype(BF16)
    for col in range(HALF):
        source = col - shift + jnp.where(shift <= HALF, WIN_LON, WIN_LON - HALF)
        back_ref[col] = summed_ref[jnp.clip(source, 0, WIN_LON - 1)]


def share_kernel(shares_ref, rows_ref, out_ref):
    total = shares_ref[0].astype(F32)
    for i in range(1, shares_ref.shape[0]):
        total = total + shares_ref[i].astype(F32)
    count = rows_ref.shape[0]
    out_ref[:count, :] = rows_ref[...]
    out_ref[count:, :] = total.astype(BF16)


def finish_kernel(
    shift_ref, gathered_ref, summed_ref, returned_ref,
    feature_ref, attend_ref, output_ref, bias_ref, dense_ref,
):
    shift = shift_ref[0]
    low = shift <= HALF
    lats, cols, levels, width = feature_ref.shape
    for col in range(cols):
        own = jnp.logical_xor(low, col < shift)
        source = jnp.where(low, col - shift, col + cols - shift)
        given = jnp.where(low, col, col - (cols - HALF))
        rows = jnp.where(
            own,
            summed_ref[jnp.clip(source, 0, cols - 1)],
            returned_ref[jnp.clip(given, 0, HALF - 1)],
        )
        for lat in range(lats):
            feature_ref[lat, col] = rows[lat * levels : (lat + 1) * levels, :]
    heads, types, count = bias_ref.shape
    devices, height, wide = gathered_ref.shape
    dense = dense_ref.shape[1] // wide
    share = height - 8 * dense
    for i in range(devices):
        start = i * share
        block = gathered_ref[i, 8 * dense :, :].astype(F32)
        if start < 3 * width:
            attend_ref[start // width, start % width : start % width + share, :] = block
        else:
            output_ref[start - 3 * width : start - 3 * width + share, :] = block
        for j in range(dense):
            dense_ref[i * 8 : (i + 1) * 8, j * wide : (j + 1) * wide] = gathered_ref[
                i, j * 8 : (j + 1) * 8, :
            ]
    full = -(-count // LANES) * LANES
    middle = full // 2
    row, lane = grid_of(devices * 8, types)
    row = lax.bitwise_and(row, 7)
    tag = count - (full - LANES)
    lane = lane.astype(F32)
    kind = dense_ref[:, full - LANES : full].astype(F32)[:, tag : tag + 1]
    for h in range(2):
        mine = (row >= 4 * h) & (row < 4 * h + 4)
        sel = one_hot((kind == lane) & mine)
        bias_ref[h] = dot_tn(sel, dense_ref[:, :full])[:, :count]
    block = dense_ref[:, full + middle - LANES : full + middle].astype(F32)
    below = block[:, tag : tag + 1]
    above = pltpu.roll(block, devices * 8 - 4, 0)[:, tag : tag + 1]
    tail = dense_ref[:, full:]
    bias_ref[2, :, :middle] = dot_tn(one_hot((above == lane) & (row < 4)), tail)
    bias_ref[2, :, middle:] = dot_tn(one_hot((below == lane) & (row >= 4)), tail)[
        :, : count - middle
    ]


def exchange(x, axis, shift, sign):
    count = lax.axis_size(axis)
    ahead = lax.ppermute(x, axis, [(i, (i - sign) % count) for i in range(count)])
    if count == 2:
        return ahead
    behind = lax.ppermute(x, axis, [(i, (i + sign) % count) for i in range(count)])
    return jnp.where(shift[0] <= HALF, ahead, behind)


def per_device(
    features, attend_weight, output_weight, bias_table, bias_type, window_shift, grad_out
):
    levels, lats, cols, depth = features.shape
    slots = levels // WIN_LEVEL
    width, heads = output_weight.shape[0], bias_table.shape[1]
    types, count = bias_table.shape[0], bias_table.shape[2]
    assert lats == WIN_LAT and cols == WIN_LON and levels == 8 and heads * slots == 12
    assert count == WIN_LEVEL * WIN_LEVEL * WIN_LAT * PIECE
    n_head = lax.axis_size("head")
    tall = lats * levels
    number = heads * slots
    shape = jax.ShapeDtypeStruct
    x = features.transpose(1, 2, 0, 3)
    g = grad_out.transpose(1, 2, 0, 3)
    weight = attend_weight.transpose(0, 2, 1)
    table = bias_table.transpose(1, 0, 2)
    slab = pl.pallas_call(
        pack_kernel,
        name="pack",
        out_shape=shape((2, lats, HALF, levels, depth), BF16),
        in_specs=[SMEM, ANY, ANY],
        out_specs=ANY,
        scratch_shapes=[pltpu.SemaphoreType.DMA((2,))],
    )(window_shift, x, g)
    far = exchange(slab, "lon", window_shift, 1)
    natural = -(-count // LANES) * LANES + LANES
    turned, near, weights = pl.pallas_call(
        prepare_kernel,
        name="prepare",
        out_shape=[
            shape((heads, slots * PAD, SPAN), F32),
            shape((cols, tall, 4 * LANES), BF16),
            shape((4 * LANES, depth), BF16),
        ],
        in_specs=[SMEM] + [VMEM] * 5,
        out_specs=[VMEM] * 3,
        scratch_shapes=[
            pltpu.VMEM((PAD, natural), F32),
            pltpu.VMEM((2 * WIN_LEVEL, number * PAD, LANES), F32),
        ],
    )(bias_type, x, g, weight, output_weight, table)
    packed = 3 * (cols // 4) * tall
    *pieces, sums, folded = pl.pallas_call(
        main_kernel,
        name="main",
        out_shape=[shape((packed, LANES), BF16)] * n_head
        + [
            shape((4, width, depth), BF16),
            shape((heads, slots * PAD, SPAN), F32),
        ],
        in_specs=[SMEM] + [VMEM] * 6,
        out_specs=[VMEM] * (n_head + 2),
        scratch_shapes=[
            pltpu.VMEM((HALF, tall, 4 * LANES), BF16),
            pltpu.VMEM((2, cols * tall, depth), BF16),
            pltpu.VMEM((slots, WIDE, 4 * LANES), BF16),
            pltpu.VMEM((heads, WIDE, WIDE), F32),
            pltpu.VMEM((cols, slots * PAD, 4 * LANES), BF16),
            pltpu.VMEM((cols * tall, 4 * LANES), BF16),
            pltpu.VMEM((n_head, packed, LANES), BF16),
        ],
    )(window_shift, x, g, far, near, weights, turned)
    parts = [pieces[0]]
    for step in range(1, n_head):
        ring = [(i, (i + step) % n_head) for i in range(n_head)]
        parts.append(lax.ppermute(pieces[step], "head", ring))
    every = ("lon", "lat")
    n_every = lax.axis_size("lon") * lax.axis_size("lat")
    shares = sums.reshape(n_every, 4 * width // n_every, depth)
    shares = lax.all_to_all(shares, every, 0, 0)
    full = natural - LANES
    dense = full + full // 2
    rows = pl.pallas_call(
        bias_kernel,
        name="bias_rows",
        out_shape=shape((8 * dense // depth, depth), BF16),
        in_specs=[SMEM, VMEM],
        out_specs=VMEM,
        scratch_shapes=[
            pltpu.VMEM((2 * WIN_LEVEL, number * PAD, LANES), F32),
            pltpu.VMEM((PAD, natural), F32),
            pltpu.VMEM((8, dense), F32),
        ],
    )(bias_type, folded)
    summed, back = pl.pallas_call(
        sum_kernel,
        name="sum_heads",
        out_shape=[shape((cols, tall, width), BF16), shape((HALF, tall, width), BF16)],
        in_specs=[SMEM] + [VMEM] * n_head,
        out_specs=[VMEM] * 2,
    )(window_shift, *parts)
    returned = exchange(back, "lon", window_shift, -1)
    share = pl.pallas_call(
        share_kernel,
        name="share",
        out_shape=shape((rows.shape[0] + shares.shape[1], depth), BF16),
        in_specs=[VMEM] * 2,
        out_specs=VMEM,
    )(shares, rows)
    gathered = lax.all_gather(share, every, axis=0)
    feature_grad, attend_grad, output_grad, bias_grad = pl.pallas_call(
        finish_kernel,
        name="finish",
        out_shape=[
            shape((lats, cols, levels, width), BF16),
            shape((3, width, depth), F32),
            shape((width, depth), F32),
            shape((heads, types, count), F32),
        ],
        in_specs=[SMEM] + [VMEM] * 3,
        out_specs=[VMEM] * 4,
        scratch_shapes=[pltpu.VMEM((8 * n_every, dense), BF16)],
    )(window_shift, gathered, summed, returned)
    return (
        feature_grad.transpose(2, 0, 1, 3),
        attend_grad.transpose(0, 2, 1),
        output_grad,
        bias_grad.transpose(1, 0, 2),
    )


def solution(mesh):
    placed = (
        P(None, "lat", "lon", None),
        P(None, None, "head"),
        P("head", None),
        P(None, "head", None),
        P(None, "lat"),
        P(),
        P(None, "lat", "lon", None),
    )
    return jax.shard_map(
        per_device,
        mesh=mesh,
        in_specs=placed,
        out_specs=(
            P(None, "lat", "lon", "head"),
            P(None, None, "head"),
            P("head", None),
            P(None, "head", None),
        ),
        check_vma=False,
    )
```

```python
import jax
import jax.numpy as jnp
from jax import lax
from jax.experimental import pallas as pl
from jax.experimental.pallas import tpu as pltpu
from jax.sharding import PartitionSpec as P

WIN_LEVEL = 2
WIN_LAT = 6
WIN_LON = 12
ROWS = WIN_LEVEL * WIN_LAT
PAD = 16
WIDE = WIN_LON * PAD
HALF = WIN_LON // 2
OFFSETS = 2 * WIN_LON - 1
PIECE = WIN_LAT * OFFSETS
LANES = 128
SPAN = -(-OFFSETS * PAD // LANES) * LANES
MASKED = -1e30
F32 = jnp.float32
BF16 = jnp.bfloat16
SMEM = pl.BlockSpec(memory_space=pltpu.SMEM)
VMEM = pl.BlockSpec(memory_space=pltpu.VMEM)
HBM = pl.BlockSpec(memory_space=pltpu.HBM)


def dot_nn(a, b):
    return lax.dot_general(a, b, (((1,), (0,)), ((), ())), preferred_element_type=F32)


def dot_nt(a, b):
    return lax.dot_general(a, b, (((1,), (1,)), ((), ())), preferred_element_type=F32)


def dot_tn(a, b):
    return lax.dot_general(a, b, (((0,), (0,)), ((), ())), preferred_element_type=F32)


def grid_of(rows, cols):
    shape = (rows, cols)
    return lax.broadcasted_iota(jnp.int32, shape, 0), lax.broadcasted_iota(jnp.int32, shape, 1)


def one_hot(hit):
    return jnp.where(hit, 1.0, 0.0).astype(BF16)


def window_order(levels):
    row, src = grid_of(levels // WIN_LEVEL * PAD, WIN_LAT * levels)
    bits = levels.bit_length() - 1
    lat = lax.shift_right_logical(src, bits)
    level = lax.bitwise_and(src, levels - 1)
    slot = lax.shift_right_logical(level, 1)
    return one_hot(row == slot * PAD + lax.bitwise_and(level, 1) * WIN_LAT + lat)


def offset_order(level_j):
    src, lane = grid_of(2 * LANES, SPAN)
    back = lax.shift_right_logical(lane, 4)
    lat = lax.bitwise_and(lane, PAD - 1) - level_j * WIN_LAT
    hit = (src == lat * OFFSETS + OFFSETS - 1 - back) & (lat >= 0) & (lat < WIN_LAT)
    return one_hot(hit & (back < OFFSETS))


def table_pieces():
    for level_i in range(WIN_LEVEL):
        for level_j in range(WIN_LEVEL):
            for lat_i in range(WIN_LAT):
                index = (level_i * WIN_LEVEL + level_j) * WIN_LAT + lat_i
                yield level_i * WIN_LAT + lat_i, level_j, index * PIECE


def pack_kernel(shift_ref, x_ref, g_ref, out_ref, sems):
    base = jnp.where(shift_ref[0] <= HALF, 0, WIN_LON - HALF)
    copies = [
        pltpu.make_async_copy(ref.at[:, pl.ds(base, HALF)], out_ref.at[i], sems.at[i])
        for i, ref in enumerate((x_ref, g_ref))
    ]
    for copy in copies:
        copy.start()
    for copy in copies:
        copy.wait()


def project(rows_x, rows_g, weights):
    width = 3 * LANES
    return jnp.concatenate(
        [dot_nt(rows_x, weights[:width]), dot_nt(rows_g, weights[width:])], axis=1
    )


def prepare_kernel(
    kind_ref, x_ref, g_ref, weight_ref, out_weight_ref, table_ref,
    turned_ref, projected_ref, weights_ref, natural_ref, pieces_ref,
):
    lats, cols, levels, depth = x_ref.shape
    heads = table_ref.shape[0]
    slots = kind_ref.shape[0]
    count = table_ref.shape[2]
    width = out_weight_ref.shape[0]
    weights_ref[...] = jnp.zeros(weights_ref.shape, BF16)
    for c in range(3):
        weights_ref[c * LANES : c * LANES + width, :] = weight_ref[c]
    weights_ref[3 * LANES : 3 * LANES + width, :] = out_weight_ref[...]
    flat = (lats * cols * levels, depth)
    projected = project(x_ref[...].reshape(flat), g_ref[...].reshape(flat), weights_ref[...])
    for lat in range(lats):
        for col in range(cols):
            start = (lat * cols + col) * levels
            projected_ref[col, lat * levels : (lat + 1) * levels, :] = projected[
                start : start + levels, :
            ].astype(BF16)
    natural_ref[...] = jnp.zeros(natural_ref.shape, F32)
    pieces_ref[...] = jnp.zeros(pieces_ref.shape, F32)
    for h in range(heads):
        for slot in range(slots):
            row = h * slots + slot
            natural_ref[row : row + 1, :count] = table_ref[h, pl.ds(kind_ref[slot, 0], 1), :]
    number = heads * slots
    for place, level_j, start in table_pieces():
        low = start // LANES * LANES
        block = natural_ref[:, low : low + 3 * LANES]
        if start > low:
            block = pltpu.roll(block, 3 * LANES - (start - low), 1)
        for t in range(2):
            pieces_ref[2 * level_j + t, pl.ds(place, number, stride=PAD), :] = block[
                :number, t * LANES : (t + 1) * LANES
            ]
    turned = jnp.zeros((number * PAD, SPAN), F32)
    for level_j in range(WIN_LEVEL):
        order = offset_order(level_j)
        rest = jnp.concatenate([pieces_ref[2 * level_j], pieces_ref[2 * level_j + 1]], axis=1)
        for _ in range(3):
            part = rest.astype(BF16)
            turned = turned + dot_nn(part, order)
            rest = rest - part.astype(F32)
    lane = lax.broadcasted_iota(jnp.int32, turned.shape, 1)
    turned = jnp.where(lax.bitwise_and(lane, PAD - 1) < ROWS, turned, MASKED)
    for h in range(heads):
        turned_ref[h] = turned[h * slots * PAD : (h + 1) * slots * PAD, :]


def main_kernel(
    shift_ref, x_ref, g_ref, far_ref, near_ref, weights_ref, turned_ref, *rest
):
    n_head = lax.axis_size("head")
    pieces = rest[:n_head]
    sums_ref, folded_ref = rest[n_head : n_head + 2]
    beyond_ref, own_ref, ordered_ref, bias_ref, given_ref, back_ref, chunk_ref = rest[n_head + 2 :]
    lats, cols, levels, depth = x_ref.shape
    width = sums_ref.shape[1]
    heads, slot_rows = turned_ref.shape[0], turned_ref.shape[1]
    slots = slot_rows // PAD
    size = width // heads
    scaling = size ** (-0.5)
    mine = lax.axis_index("head")
    shift = shift_ref[0]
    low = shift <= HALF
    tall = lats * levels
    flat = (lats * HALF * levels, depth)
    projected = project(far_ref[0].reshape(flat), far_ref[1].reshape(flat), weights_ref[...])
    for lat in range(lats):
        for col in range(HALF):
            start = (lat * HALF + col) * levels
            beyond_ref[col, lat * levels : (lat + 1) * levels, :] = projected[
                start : start + levels, :
            ].astype(BF16)
    order = window_order(levels)
    for col in range(cols):
        at = col + shift
        inside = jnp.logical_xor(low, at >= cols)
        local = jnp.where(at >= cols, at - cols, at)
        taken = jnp.where(low, at - cols, at - (cols - HALF))
        taken = jnp.clip(taken, 0, HALF - 1)
        rows = jnp.where(inside, near_ref[local], beyond_ref[taken])
        ordered = dot_nn(order, rows).astype(BF16)
        for slot in range(slots):
            ordered_ref[slot, col * PAD : (col + 1) * PAD, :] = ordered[
                slot * PAD : (slot + 1) * PAD, :
            ]
        for array, ref in enumerate((x_ref, g_ref)):
            for lat in range(lats):
                start = col * tall + lat * levels
                own_ref[array, start : start + levels, :] = jnp.where(
                    inside, ref[lat, local], far_ref[array, lat, taken]
                )
    lane = lax.broadcasted_iota(jnp.int32, (WIDE, LANES), 1)
    masks = [(lane >= h * size) & (lane < (h + 1) * size) for h in range(heads)]
    none = jnp.zeros((WIDE, LANES), BF16)
    for slot in range(slots):
        query = ordered_ref[slot, :, :LANES]
        key = ordered_ref[slot, :, LANES : 2 * LANES]
        value = ordered_ref[slot, :, 2 * LANES : 3 * LANES]
        grad_attended = ordered_ref[slot, :, 3 * LANES :]
        at = slice(slot * PAD, (slot + 1) * PAD)
        attended = jnp.zeros((WIDE, LANES), F32)
        grad_query = jnp.zeros((WIDE, LANES), F32)
        grad_key = jnp.zeros((WIDE, LANES), F32)
        grad_value = jnp.zeros((WIDE, LANES), F32)
        for h in range(heads):
            table = turned_ref[h, at, :]
            for col in range(WIN_LON):
                by = (WIN_LON - 1 - col) * PAD
                moved = table if by == 0 else pltpu.roll(table, SPAN - by, 1)
                bias_ref[h, col * PAD : (col + 1) * PAD, :] = moved[:, :WIDE]
            query_h = jnp.where(masks[h], query, none)
            key_h = jnp.where(masks[h], key, none)
            value_h = jnp.where(masks[h], value, none)
            grad_h = jnp.where(masks[h], grad_attended, none)
            scores = dot_nt(query_h, key) * scaling + bias_ref[h]
            raised = jnp.exp(scores - jnp.max(scores, axis=1, keepdims=True))
            softened = raised * (1.0 / jnp.sum(raised, axis=1, keepdims=True))
            softened_half = softened.astype(BF16)
            attended = attended + dot_nn(softened_half, value_h)
            grad_value = grad_value + dot_tn(softened_half, grad_h)
            grad_softened = dot_nt(grad_h, value)
            inner = jnp.sum(softened * grad_softened, axis=1, keepdims=True)
            grad_scores = softened * (grad_softened - inner)
            grad_half = grad_scores.astype(BF16)
            grad_query = grad_query + dot_nn(grad_half, key_h)
            grad_key = grad_key + dot_tn(grad_half, query_h)
            padded = jnp.concatenate([grad_scores, jnp.zeros((WIDE, SPAN - WIDE), F32)], axis=1)
            total = jnp.zeros((PAD, SPAN), F32)
            for col in range(WIN_LON):
                by = (WIN_LON - 1 - col) * PAD
                part = padded[col * PAD : (col + 1) * PAD, :]
                total = total + (part if by == 0 else pltpu.roll(part, by, 1))
            folded_ref[h, at, :] = total
        results = (grad_query * scaling, grad_key * scaling, grad_value, attended)
        for c, result in enumerate(results):
            rounded = result.astype(BF16)
            for col in range(WIN_LON):
                given_ref[col, at, c * LANES : (c + 1) * LANES] = rounded[
                    col * PAD : (col + 1) * PAD, :
                ]
    for col in range(WIN_LON):
        back_ref[col * tall : (col + 1) * tall, :] = dot_tn(order, given_ref[col]).astype(BF16)
    grads = 3 * LANES
    piece = dot_nn(back_ref[:, :grads], weights_ref[:grads, :])
    group = WIN_LON // 4 * tall
    third = width // 3
    for to in range(n_head):
        lanes = piece[:, to * width : (to + 1) * width]
        for g in range(3):
            tail = lanes[3 * group :, g * third : (g + 1) * third]
            chunk_ref[to, g * group : (g + 1) * group, :] = jnp.concatenate(
                [lanes[g * group : (g + 1) * group, :], tail], axis=1
            ).astype(BF16)
    for step in range(n_head):
        pieces[step][...] = chunk_ref[lax.rem(mine + step, n_head)]
    summed = dot_tn(back_ref[:, :grads], own_ref[0])
    for c in range(3):
        sums_ref[c] = summed[c * LANES : c * LANES + width, :].astype(BF16)
    sums_ref[3] = dot_tn(back_ref[:, grads:], own_ref[1])[:width, :].astype(BF16)


def bias_kernel(kind_ref, folded_ref, out_ref, pieces_ref, natural_ref, dense_ref):
    heads, slot_rows, span = folded_ref.shape
    slots = slot_rows // PAD
    number = heads * slots
    rows = folded_ref[...].reshape(heads * slot_rows, span).astype(BF16)
    for level_j in range(WIN_LEVEL):
        moved = dot_nt(rows, offset_order(level_j))
        for t in range(2):
            pieces_ref[2 * level_j + t] = moved[:, t * LANES : (t + 1) * LANES]
    natural_ref[...] = jnp.zeros(natural_ref.shape, F32)
    for place, level_j, start in table_pieces():
        low = start // LANES * LANES
        parts = [
            pieces_ref[2 * level_j + t, pl.ds(place, number, stride=PAD), :] for t in range(2)
        ]
        part = jnp.concatenate(parts + [jnp.zeros((number, LANES), F32)], axis=1)
        if start > low:
            part = pltpu.roll(part, start - low, 1)
        at = (slice(0, number), slice(low, low + 3 * LANES))
        natural_ref[at] = natural_ref[at] + part
    count = WIN_LEVEL * WIN_LEVEL * WIN_LAT * PIECE
    low = count // LANES * LANES
    row, lane = grid_of(number, LANES)
    kind = jnp.zeros((number, LANES), F32)
    for slot in range(slots):
        kind = jnp.where(lax.rem(row, slots) == slot, kind_ref[slot, 0].astype(F32), kind)
    at = (slice(0, number), slice(low, low + LANES))
    natural_ref[at] = natural_ref[at] + jnp.where(lane == count - low, kind, 0.0)
    full = low + LANES
    middle = full // 2
    dense_ref[:, :full] = natural_ref[0:8, :full]
    dense_ref[0:4, full:] = natural_ref[8:12, :middle]
    dense_ref[4:8, full:] = natural_ref[8:12, middle:full]
    wide = out_ref.shape[1]
    for j in range(out_ref.shape[0] // 8):
        out_ref[j * 8 : (j + 1) * 8, :] = dense_ref[:, j * wide : (j + 1) * wide].astype(BF16)


def sum_kernel(shift_ref, *refs):
    parts = refs[:-2]
    summed_ref, back_ref = refs[-2:]
    shift = shift_ref[0]
    total = parts[0][...].astype(F32)
    for part in parts[1:]:
        total = total + part[...].astype(F32)
    cols, tall, width = summed_ref.shape
    group = cols // 4
    for g in range(3):
        for i in range(group):
            start = (g * group + i) * tall
            summed_ref[g * group + i] = total[start : start + tall, :width].astype(BF16)
    for i in range(group):
        tails = [
            total[(g * group + i) * tall : (g * group + i + 1) * tall, width:] for g in range(3)
        ]
        summed_ref[3 * group + i] = jnp.concatenate(tails, axis=1).astype(BF16)
    for col in range(HALF):
        source = col - shift + jnp.where(shift <= HALF, WIN_LON, WIN_LON - HALF)
        back_ref[col] = summed_ref[jnp.clip(source, 0, WIN_LON - 1)]


def share_kernel(shares_ref, rows_ref, out_ref):
    total = shares_ref[0].astype(F32)
    for i in range(1, shares_ref.shape[0]):
        total = total + shares_ref[i].astype(F32)
    count = rows_ref.shape[0]
    out_ref[:count, :] = rows_ref[...]
    out_ref[count:, :] = total.astype(BF16)


def finish_kernel(
    shift_ref, gathered_ref, summed_ref, returned_ref,
    feature_ref, attend_ref, output_ref, bias_ref, dense_ref,
):
    shift = shift_ref[0]
    low = shift <= HALF
    lats, cols, levels, width = feature_ref.shape
    for col in range(cols):
        own = jnp.logical_xor(low, col < shift)
        source = jnp.where(low, col - shift, col + cols - shift)
        given = jnp.where(low, col, col - (cols - HALF))
        rows = jnp.where(
            own,
            summed_ref[jnp.clip(source, 0, cols - 1)],
            returned_ref[jnp.clip(given, 0, HALF - 1)],
        )
        for lat in range(lats):
            feature_ref[lat, col] = rows[lat * levels : (lat + 1) * levels, :]
    heads, types, count = bias_ref.shape
    devices, height, wide = gathered_ref.shape
    dense = dense_ref.shape[1] // wide
    share = height - 8 * dense
    for i in range(devices):
        start = i * share
        block = gathered_ref[i, 8 * dense :, :].astype(F32)
        if start < 3 * width:
            attend_ref[start // width, start % width : start % width + share, :] = block
        else:
            output_ref[start - 3 * width : start - 3 * width + share, :] = block
        for j in range(dense):
            dense_ref[i * 8 : (i + 1) * 8, j * wide : (j + 1) * wide] = gathered_ref[
                i, j * 8 : (j + 1) * 8, :
            ]
    full = -(-count // LANES) * LANES
    middle = full // 2
    row, lane = grid_of(devices * 8, types)
    row = lax.bitwise_and(row, 7)
    tag = count - (full - LANES)
    lane = lane.astype(F32)
    kind = dense_ref[:, full - LANES : full].astype(F32)[:, tag : tag + 1]
    for h in range(2):
        mine = (row >= 4 * h) & (row < 4 * h + 4)
        sel = one_hot((kind == lane) & mine)
        bias_ref[h] = dot_tn(sel, dense_ref[:, :full])[:, :count]
    block = dense_ref[:, full + middle - LANES : full + middle].astype(F32)
    below = block[:, tag : tag + 1]
    above = pltpu.roll(block, devices * 8 - 4, 0)[:, tag : tag + 1]
    tail = dense_ref[:, full:]
    bias_ref[2, :, :middle] = dot_tn(one_hot((above == lane) & (row < 4)), tail)
    bias_ref[2, :, middle:] = dot_tn(one_hot((below == lane) & (row >= 4)), tail)[
        :, : count - middle
    ]


def small(mebibytes):
    return pltpu.CompilerParams(vmem_limit_bytes=mebibytes << 20)


def exchange(x, axis, shift, sign):
    count = lax.axis_size(axis)
    ahead = lax.ppermute(x, axis, [(i, (i - sign) % count) for i in range(count)])
    if count == 2:
        return ahead
    behind = lax.ppermute(x, axis, [(i, (i + sign) % count) for i in range(count)])
    return jnp.where(shift[0] <= HALF, ahead, behind)


def per_device(
    features, attend_weight, output_weight, bias_table, bias_type, window_shift, grad_out
):
    levels, lats, cols, depth = features.shape
    slots = levels // WIN_LEVEL
    width, heads = output_weight.shape[0], bias_table.shape[1]
    types, count = bias_table.shape[0], bias_table.shape[2]
    assert lats == WIN_LAT and cols == WIN_LON and levels == 8 and heads * slots == 12
    assert count == WIN_LEVEL * WIN_LEVEL * WIN_LAT * PIECE
    n_head = lax.axis_size("head")
    tall = lats * levels
    number = heads * slots
    shape = jax.ShapeDtypeStruct
    x = features.transpose(1, 2, 0, 3)
    g = grad_out.transpose(1, 2, 0, 3)
    weight = attend_weight.transpose(0, 2, 1)
    table = bias_table.transpose(1, 0, 2)
    slab = pl.pallas_call(
        pack_kernel,
        name="pack",
        out_shape=shape((2, lats, HALF, levels, depth), BF16),
        in_specs=[SMEM, HBM, HBM],
        out_specs=VMEM,
        scratch_shapes=[pltpu.SemaphoreType.DMA((2,))],
        compiler_params=small(4),
    )(window_shift, x, g)
    far = exchange(slab, "lon", window_shift, 1)
    natural = -(-count // LANES) * LANES + LANES
    turned, near, weights = pl.pallas_call(
        prepare_kernel,
        name="prepare",
        out_shape=[
            shape((heads, slots * PAD, SPAN), F32),
            shape((cols, tall, 4 * LANES), BF16),
            shape((4 * LANES, depth), BF16),
        ],
        in_specs=[SMEM] + [VMEM] * 5,
        out_specs=[VMEM] * 3,
        scratch_shapes=[
            pltpu.VMEM((PAD, natural), F32),
            pltpu.VMEM((2 * WIN_LEVEL, number * PAD, LANES), F32),
        ],
        compiler_params=small(16),
    )(bias_type, x, g, weight, output_weight, table)
    packed = 3 * (cols // 4) * tall
    *pieces, sums, folded = pl.pallas_call(
        main_kernel,
        name="main",
        out_shape=[shape((packed, LANES), BF16)] * n_head
        + [
            shape((4, width, depth), BF16),
            shape((heads, slots * PAD, SPAN), F32),
        ],
        in_specs=[SMEM] + [VMEM] * 6,
        out_specs=[VMEM] * (n_head + 2),
        scratch_shapes=[
            pltpu.VMEM((HALF, tall, 4 * LANES), BF16),
            pltpu.VMEM((2, cols * tall, depth), BF16),
            pltpu.VMEM((slots, WIDE, 4 * LANES), BF16),
            pltpu.VMEM((heads, WIDE, WIDE), F32),
            pltpu.VMEM((cols, slots * PAD, 4 * LANES), BF16),
            pltpu.VMEM((cols * tall, 4 * LANES), BF16),
            pltpu.VMEM((n_head, packed, LANES), BF16),
        ],
        compiler_params=small(24),
    )(window_shift, x, g, far, near, weights, turned)
    parts = [pieces[0]]
    for step in range(1, n_head):
        ring = [(i, (i + step) % n_head) for i in range(n_head)]
        parts.append(lax.ppermute(pieces[step], "head", ring))
    every = ("lon", "lat")
    n_every = lax.axis_size("lon") * lax.axis_size("lat")
    shares = sums.reshape(n_every, 4 * width // n_every, depth)
    shares = lax.all_to_all(shares, every, 0, 0)
    full = natural - LANES
    dense = full + full // 2
    rows = pl.pallas_call(
        bias_kernel,
        name="bias_rows",
        out_shape=shape((8 * dense // depth, depth), BF16),
        in_specs=[SMEM, VMEM],
        out_specs=VMEM,
        scratch_shapes=[
            pltpu.VMEM((2 * WIN_LEVEL, number * PAD, LANES), F32),
            pltpu.VMEM((PAD, natural), F32),
            pltpu.VMEM((8, dense), F32),
        ],
        compiler_params=small(8),
    )(bias_type, folded)
    summed, back = pl.pallas_call(
        sum_kernel,
        name="sum_heads",
        out_shape=[shape((cols, tall, width), BF16), shape((HALF, tall, width), BF16)],
        in_specs=[SMEM] + [VMEM] * n_head,
        out_specs=[VMEM] * 2,
        compiler_params=small(6),
    )(window_shift, *parts)
    returned = exchange(back, "lon", window_shift, -1)
    share = pl.pallas_call(
        share_kernel,
        name="share",
        out_shape=shape((rows.shape[0] + shares.shape[1], depth), BF16),
        in_specs=[VMEM] * 2,
        out_specs=VMEM,
        compiler_params=small(4),
    )(shares, rows)
    gathered = lax.all_gather(share, every, axis=0)
    feature_grad, attend_grad, output_grad, bias_grad = pl.pallas_call(
        finish_kernel,
        name="finish",
        out_shape=[
            shape((lats, cols, levels, width), BF16),
            shape((3, width, depth), F32),
            shape((width, depth), F32),
            shape((heads, types, count), F32),
        ],
        in_specs=[SMEM] + [VMEM] * 3,
        out_specs=[VMEM] * 4,
        scratch_shapes=[pltpu.VMEM((8 * n_every, dense), BF16)],
        compiler_params=small(16),
    )(window_shift, gathered, summed, returned)
    return (
        feature_grad.transpose(2, 0, 1, 3),
        attend_grad.transpose(0, 2, 1),
        output_grad,
        bias_grad.transpose(1, 0, 2),
    )


def solution(mesh):
    placed = (
        P(None, "lat", "lon", None),
        P(None, None, "head"),
        P("head", None),
        P(None, "head", None),
        P(None, "lat"),
        P(),
        P(None, "lat", "lon", None),
    )
    return jax.shard_map(
        per_device,
        mesh=mesh,
        in_specs=placed,
        out_specs=(
            P(None, "lat", "lon", "head"),
            P(None, None, "head"),
            P("head", None),
            P(None, "head", None),
        ),
        check_vma=False,
    )
```

```python
import jax
import jax.numpy as jnp
from jax import lax
from jax.experimental import pallas as pl
from jax.experimental.pallas import tpu as pltpu
from jax.sharding import PartitionSpec as P

WIN_LEVEL = 2
WIN_LAT = 6
WIN_LON = 12
ROWS = WIN_LEVEL * WIN_LAT
PAD = 16
WIDE = WIN_LON * PAD
HALF = WIN_LON // 2
OFFSETS = 2 * WIN_LON - 1
PIECE = WIN_LAT * OFFSETS
LANES = 128
SPAN = -(-OFFSETS * PAD // LANES) * LANES
MASKED = -1e30
F32 = jnp.float32
BF16 = jnp.bfloat16
SMEM = pl.BlockSpec(memory_space=pltpu.SMEM)
VMEM = pl.BlockSpec(memory_space=pltpu.VMEM)
HBM = pl.BlockSpec(memory_space=pltpu.HBM)


def dot_nn(a, b):
    return lax.dot_general(a, b, (((1,), (0,)), ((), ())), preferred_element_type=F32)


def dot_nt(a, b):
    return lax.dot_general(a, b, (((1,), (1,)), ((), ())), preferred_element_type=F32)


def dot_tn(a, b):
    return lax.dot_general(a, b, (((0,), (0,)), ((), ())), preferred_element_type=F32)


def grid_of(rows, cols):
    shape = (rows, cols)
    return lax.broadcasted_iota(jnp.int32, shape, 0), lax.broadcasted_iota(jnp.int32, shape, 1)


def one_hot(hit):
    return jnp.where(hit, 1.0, 0.0).astype(BF16)


def window_order(levels):
    row, src = grid_of(levels // WIN_LEVEL * PAD, WIN_LAT * levels)
    bits = levels.bit_length() - 1
    lat = lax.shift_right_logical(src, bits)
    level = lax.bitwise_and(src, levels - 1)
    slot = lax.shift_right_logical(level, 1)
    return one_hot(row == slot * PAD + lax.bitwise_and(level, 1) * WIN_LAT + lat)


def offset_order(level_j):
    src, lane = grid_of(2 * LANES, SPAN)
    back = lax.shift_right_logical(lane, 4)
    lat = lax.bitwise_and(lane, PAD - 1) - level_j * WIN_LAT
    hit = (src == lat * OFFSETS + OFFSETS - 1 - back) & (lat >= 0) & (lat < WIN_LAT)
    return one_hot(hit & (back < OFFSETS))


def table_pieces():
    for level_i in range(WIN_LEVEL):
        for level_j in range(WIN_LEVEL):
            for lat_i in range(WIN_LAT):
                index = (level_i * WIN_LEVEL + level_j) * WIN_LAT + lat_i
                yield level_i * WIN_LAT + lat_i, level_j, index * PIECE


def run_all(copies):
    for copy in copies:
        copy.start()
    for copy in copies:
        copy.wait()


def start_kernel(
    shift_ref, x_ref, g_ref, weight_ref, out_weight_ref, raw_ref, projected_ref, rows_ref, sems
):
    base = jnp.where(shift_ref[0] <= HALF, 0, WIN_LON - HALF)
    lats, _, levels, depth = x_ref.shape
    width = out_weight_ref.shape[0]
    moves = [(ref.at[:, pl.ds(base, HALF)], raw_ref.at[i]) for i, ref in enumerate((x_ref, g_ref))]
    moves += [(weight_ref.at[c], rows_ref.at[pl.ds(c * width, width)]) for c in range(3)]
    moves.append((out_weight_ref, rows_ref.at[pl.ds(3 * width, width)]))
    run_all([pltpu.make_async_copy(a, b, sems.at[i]) for i, (a, b) in enumerate(moves)])
    flat = (lats * HALF * levels, depth)
    projected = jnp.concatenate(
        [
            dot_nt(raw_ref[0].reshape(flat), rows_ref[: 3 * width, :]),
            dot_nt(raw_ref[1].reshape(flat), rows_ref[3 * width :, :]),
        ],
        axis=1,
    ).astype(BF16)
    for lat in range(lats):
        for col in range(HALF):
            start = (lat * HALF + col) * levels
            projected_ref[col, lat * levels : (lat + 1) * levels, :] = projected[
                start : start + levels, :
            ]


def prepare_kernel(
    kind_ref, x_ref, g_ref, weight_ref, out_weight_ref, table_ref,
    bias_ref, near_ref, weights_ref,
    own_ref, given_ref, chosen_ref, natural_ref, pieces_ref, sems,
):
    lats, cols, levels, depth = x_ref.shape
    heads = table_ref.shape[0]
    slots = kind_ref.shape[0]
    count = table_ref.shape[2]
    width = out_weight_ref.shape[0]
    number = heads * slots
    moves = []
    for slot in range(slots):
        for h in range(heads):
            source = table_ref.at[h, pl.ds(kind_ref[slot, 0], 1), :]
            moves.append((source, chosen_ref.at[pl.ds(h * slots + slot, 1), :]))
    moves += [(x_ref, own_ref), (g_ref, given_ref)]
    moves += [(weight_ref.at[c], weights_ref.at[pl.ds(c * LANES, width)]) for c in range(3)]
    moves.append((out_weight_ref, weights_ref.at[pl.ds(3 * LANES, width)]))
    copies = [pltpu.make_async_copy(a, b, sems.at[i]) for i, (a, b) in enumerate(moves)]
    for copy in copies:
        copy.start()
    for c in range(4):
        weights_ref[c * LANES + width : (c + 1) * LANES, :] = jnp.zeros(
            (LANES - width, depth), BF16
        )
    natural_ref[...] = jnp.zeros(natural_ref.shape, F32)
    pieces_ref[...] = jnp.zeros(pieces_ref.shape, F32)
    for copy in copies[:number]:
        copy.wait()
    natural_ref[:number, :count] = chosen_ref[...]
    for place, level_j, start in table_pieces():
        low = start // LANES * LANES
        block = natural_ref[:, low : low + 3 * LANES]
        if start > low:
            block = pltpu.roll(block, 3 * LANES - (start - low), 1)
        for t in range(2):
            pieces_ref[2 * level_j + t, pl.ds(place, number, stride=PAD), :] = block[
                :number, t * LANES : (t + 1) * LANES
            ]
    turned = jnp.zeros((number * PAD, SPAN), F32)
    for level_j in range(WIN_LEVEL):
        order = offset_order(level_j)
        rest = jnp.concatenate([pieces_ref[2 * level_j], pieces_ref[2 * level_j + 1]], axis=1)
        for _ in range(3):
            part = rest.astype(BF16)
            turned = turned + dot_nn(part, order)
            rest = rest - part.astype(F32)
    lane = lax.broadcasted_iota(jnp.int32, turned.shape, 1)
    turned = jnp.where(lax.bitwise_and(lane, PAD - 1) < ROWS, turned, MASKED)
    for h in range(heads):
        for slot in range(slots):
            row = (h * slots + slot) * PAD
            table = turned[row : row + PAD, :]
            for col in range(WIN_LON):
                by = (WIN_LON - 1 - col) * PAD
                moved = table if by == 0 else pltpu.roll(table, SPAN - by, 1)
                start = h * WIDE + col * PAD
                bias_ref[slot, start : start + PAD, :] = moved[:, :WIDE]
    for copy in copies[number:]:
        copy.wait()
    flat = (lats * cols * levels, depth)
    projected = project(own_ref[...].reshape(flat), given_ref[...].reshape(flat), weights_ref[...])
    for lat in range(lats):
        for col in range(cols):
            start = (lat * cols + col) * levels
            near_ref[col, lat * levels : (lat + 1) * levels, :] = projected[
                start : start + levels, :
            ].astype(BF16)


def project(rows_x, rows_g, weights):
    width = 3 * LANES
    return jnp.concatenate(
        [dot_nt(rows_x, weights[:width]), dot_nt(rows_g, weights[width:])], axis=1
    )


def column_source(shift, col, cols):
    low = shift <= HALF
    at = col + shift
    inside = jnp.logical_xor(low, at >= cols)
    local = jnp.where(at >= cols, at - cols, at)
    taken = jnp.where(low, at - cols, at - (cols - HALF))
    return inside, local, jnp.clip(taken, 0, HALF - 1)


def main_kernel(shift_ref, far_ref, near_ref, weights_ref, bias_ref, *rest):
    n_head = lax.axis_size("head")
    pieces = rest[:n_head]
    back_ref, folded_ref = rest[n_head : n_head + 2]
    (
        beyond_ref, ordered_ref, score_ref, slope_ref, soft_ref, grad_ref, exact_ref, given_ref,
        chunk_ref,
    ) = rest[n_head + 2 :]
    cols, tall, _ = near_ref.shape
    levels = tall // WIN_LAT
    slots = bias_ref.shape[0]
    heads = bias_ref.shape[1] // WIDE
    width = far_ref.shape[2] // 4
    size = width // heads
    scaling = size ** (-0.5)
    mine = lax.axis_index("head")
    shift = shift_ref[0]
    for c in range(4):
        beyond_ref[:, :, c * LANES : c * LANES + width] = far_ref[
            :, :, c * width : (c + 1) * width
        ]
        beyond_ref[:, :, c * LANES + width : (c + 1) * LANES] = jnp.zeros(
            (HALF, tall, LANES - width), BF16
        )
    order = window_order(levels)
    for col in range(cols):
        inside, local, taken = column_source(shift, col, cols)
        rows = jnp.where(inside, near_ref[local], beyond_ref[taken])
        ordered = dot_nn(order, rows).astype(BF16)
        for slot in range(slots):
            ordered_ref[slot, col * PAD : (col + 1) * PAD, :] = ordered[
                slot * PAD : (slot + 1) * PAD, :
            ]
    lane = lax.broadcasted_iota(jnp.int32, (WIDE, LANES), 1)
    masks = [(lane >= h * size) & (lane < (h + 1) * size) for h in range(heads)]
    none = jnp.zeros((WIDE, LANES), BF16)

    def by_head(array):
        return jnp.concatenate([jnp.where(mask, array, none) for mask in masks], axis=0)

    def own_lanes(array):
        total = jnp.where(masks[0], array[:WIDE, :], 0.0)
        for h in range(1, heads):
            total = jnp.where(masks[h], array[h * WIDE : (h + 1) * WIDE, :], total)
        return total

    block = 3 * PAD
    for slot in range(slots):
        half = slot % 2
        query = ordered_ref[slot, :, :LANES]
        key = ordered_ref[slot, :, LANES : 2 * LANES]
        value = ordered_ref[slot, :, 2 * LANES : 3 * LANES]
        queries = by_head(query)
        grads = by_head(ordered_ref[slot, :, 3 * LANES :])
        score_ref[half] = dot_nt(queries, key)
        slope_ref[half] = dot_nt(grads, value)
        for start in range(0, heads * WIDE, block):
            at = slice(start, start + block)
            scores = score_ref[half, at, :] * scaling + bias_ref[slot, at, :]
            raised = jnp.exp(scores - jnp.max(scores, axis=1, keepdims=True))
            softened = raised * (1.0 / jnp.sum(raised, axis=1, keepdims=True))
            soft_ref[half, at, :] = softened.astype(BF16)
            slope = slope_ref[half, at, :]
            inner = jnp.sum(softened * slope, axis=1, keepdims=True)
            grad_scores = softened * (slope - inner)
            grad_ref[half, at, :] = grad_scores.astype(BF16)
            exact_ref[half, at, :WIDE] = grad_scores
        for h in range(heads):
            total = jnp.zeros((PAD, SPAN), F32)
            for col in range(WIN_LON):
                by = (WIN_LON - 1 - col) * PAD
                start = h * WIDE + col * PAD
                part = jnp.concatenate(
                    [
                        exact_ref[half, start : start + PAD, :WIDE],
                        jnp.zeros((PAD, SPAN - WIDE), F32),
                    ],
                    axis=1,
                )
                total = total + (part if by == 0 else pltpu.roll(part, by, 1))
            folded_ref[h, slot * PAD : (slot + 1) * PAD, :] = total
        results = (
            own_lanes(dot_nn(grad_ref[half], key)) * scaling,
            dot_tn(grad_ref[half], queries) * scaling,
            dot_tn(soft_ref[half], grads),
            own_lanes(dot_nn(soft_ref[half], value)),
        )
        rows = slice(slot * PAD, (slot + 1) * PAD)
        for c, result in enumerate(results):
            rounded = result.astype(BF16)
            for col in range(WIN_LON):
                given_ref[col, rows, c * LANES : (c + 1) * LANES] = rounded[
                    col * PAD : (col + 1) * PAD, :
                ]
    for col in range(WIN_LON):
        back_ref[col * tall : (col + 1) * tall, :] = dot_tn(order, given_ref[col]).astype(BF16)
    piece = dot_nn(back_ref[:, : 3 * LANES], weights_ref[: 3 * LANES, :])
    group = WIN_LON // 4 * tall
    third = width // 3
    for to in range(n_head):
        lanes = piece[:, to * width : (to + 1) * width]
        for g in range(3):
            tail = lanes[3 * group :, g * third : (g + 1) * third]
            chunk_ref[to, g * group : (g + 1) * group, :] = jnp.concatenate(
                [lanes[g * group : (g + 1) * group, :], tail], axis=1
            ).astype(BF16)
    for step in range(n_head):
        pieces[step][...] = chunk_ref[lax.rem(mine + step, n_head)]


def sums_kernel(shift_ref, x_ref, g_ref, far_ref, back_ref, sums_ref, own_ref):
    lats, cols, levels, _ = x_ref.shape
    width = sums_ref.shape[1]
    for col in range(cols):
        inside, local, taken = column_source(shift_ref[0], col, cols)
        for array, ref in enumerate((x_ref, g_ref)):
            for lat in range(lats):
                start = (col * lats + lat) * levels
                own_ref[array, start : start + levels, :] = jnp.where(
                    inside, ref[lat, local], far_ref[array, lat, taken]
                )
    grads = 3 * LANES
    summed = dot_tn(back_ref[:, :grads], own_ref[0])
    for c in range(3):
        sums_ref[c] = summed[c * LANES : c * LANES + width, :].astype(BF16)
    sums_ref[3] = dot_tn(back_ref[:, grads:], own_ref[1])[:width, :].astype(BF16)


def bias_kernel(kind_ref, folded_ref, out_ref, pieces_ref, natural_ref, dense_ref):
    heads, slot_rows, span = folded_ref.shape
    slots = slot_rows // PAD
    number = heads * slots
    rows = folded_ref[...].reshape(heads * slot_rows, span).astype(BF16)
    for level_j in range(WIN_LEVEL):
        moved = dot_nt(rows, offset_order(level_j))
        for t in range(2):
            pieces_ref[2 * level_j + t] = moved[:, t * LANES : (t + 1) * LANES]
    natural_ref[...] = jnp.zeros(natural_ref.shape, F32)
    for place, level_j, start in table_pieces():
        low = start // LANES * LANES
        parts = [
            pieces_ref[2 * level_j + t, pl.ds(place, number, stride=PAD), :] for t in range(2)
        ]
        part = jnp.concatenate(parts + [jnp.zeros((number, LANES), F32)], axis=1)
        if start > low:
            part = pltpu.roll(part, start - low, 1)
        at = (slice(0, number), slice(low, low + 3 * LANES))
        natural_ref[at] = natural_ref[at] + part
    count = WIN_LEVEL * WIN_LEVEL * WIN_LAT * PIECE
    low = count // LANES * LANES
    row, lane = grid_of(number, LANES)
    kind = jnp.zeros((number, LANES), F32)
    for slot in range(slots):
        kind = jnp.where(lax.rem(row, slots) == slot, kind_ref[slot, 0].astype(F32), kind)
    at = (slice(0, number), slice(low, low + LANES))
    natural_ref[at] = natural_ref[at] + jnp.where(lane == count - low, kind, 0.0)
    full = low + LANES
    middle = full // 2
    dense_ref[:, :full] = natural_ref[0:8, :full]
    dense_ref[0:4, full:] = natural_ref[8:12, :middle]
    dense_ref[4:8, full:] = natural_ref[8:12, middle:full]
    wide = out_ref.shape[1]
    for j in range(out_ref.shape[0] // 8):
        out_ref[j * 8 : (j + 1) * 8, :] = dense_ref[:, j * wide : (j + 1) * wide].astype(BF16)


def sum_kernel(shift_ref, *refs):
    parts = refs[:-2]
    summed_ref, back_ref = refs[-2:]
    shift = shift_ref[0]
    total = parts[0][...].astype(F32)
    for part in parts[1:]:
        total = total + part[...].astype(F32)
    cols, tall, width = summed_ref.shape
    group = cols // 4
    for g in range(3):
        for i in range(group):
            start = (g * group + i) * tall
            summed_ref[g * group + i] = total[start : start + tall, :width].astype(BF16)
    for i in range(group):
        tails = [
            total[(g * group + i) * tall : (g * group + i + 1) * tall, width:] for g in range(3)
        ]
        summed_ref[3 * group + i] = jnp.concatenate(tails, axis=1).astype(BF16)
    for col in range(HALF):
        source = col - shift + jnp.where(shift <= HALF, WIN_LON, WIN_LON - HALF)
        back_ref[col] = summed_ref[jnp.clip(source, 0, WIN_LON - 1)]


def share_kernel(shares_ref, rows_ref, out_ref):
    total = shares_ref[0].astype(F32)
    for i in range(1, shares_ref.shape[0]):
        total = total + shares_ref[i].astype(F32)
    count = rows_ref.shape[0]
    out_ref[:count, :] = rows_ref[...]
    out_ref[count:, :] = total.astype(BF16)


def finish_kernel(
    shift_ref, gathered_ref, summed_ref, returned_ref,
    feature_ref, attend_ref, output_ref, bias_ref, dense_ref,
):
    shift = shift_ref[0]
    low = shift <= HALF
    lats, cols, levels, width = feature_ref.shape
    for col in range(cols):
        own = jnp.logical_xor(low, col < shift)
        source = jnp.where(low, col - shift, col + cols - shift)
        given = jnp.where(low, col, col - (cols - HALF))
        rows = jnp.where(
            own,
            summed_ref[jnp.clip(source, 0, cols - 1)],
            returned_ref[jnp.clip(given, 0, HALF - 1)],
        )
        for lat in range(lats):
            feature_ref[lat, col] = rows[lat * levels : (lat + 1) * levels, :]
    heads, types, count = bias_ref.shape
    devices, height, wide = gathered_ref.shape
    dense = dense_ref.shape[1] // wide
    share = height - 8 * dense
    for i in range(devices):
        start = i * share
        block = gathered_ref[i, 8 * dense :, :].astype(F32)
        if start < 3 * width:
            attend_ref[start // width, start % width : start % width + share, :] = block
        else:
            output_ref[start - 3 * width : start - 3 * width + share, :] = block
        for j in range(dense):
            dense_ref[i * 8 : (i + 1) * 8, j * wide : (j + 1) * wide] = gathered_ref[
                i, j * 8 : (j + 1) * 8, :
            ]
    full = -(-count // LANES) * LANES
    middle = full // 2
    row, lane = grid_of(devices * 8, types)
    row = lax.bitwise_and(row, 7)
    tag = count - (full - LANES)
    lane = lane.astype(F32)
    kind = dense_ref[:, full - LANES : full].astype(F32)[:, tag : tag + 1]
    for h in range(2):
        mine = (row >= 4 * h) & (row < 4 * h + 4)
        sel = one_hot((kind == lane) & mine)
        bias_ref[h] = dot_tn(sel, dense_ref[:, :full])[:, :count]
    block = dense_ref[:, full + middle - LANES : full + middle].astype(F32)
    below = block[:, tag : tag + 1]
    above = pltpu.roll(block, devices * 8 - 4, 0)[:, tag : tag + 1]
    tail = dense_ref[:, full:]
    bias_ref[2, :, :middle] = dot_tn(one_hot((above == lane) & (row < 4)), tail)
    bias_ref[2, :, middle:] = dot_tn(one_hot((below == lane) & (row >= 4)), tail)[
        :, : count - middle
    ]


def small(mebibytes):
    return pltpu.CompilerParams(vmem_limit_bytes=mebibytes << 20)


def exchange(x, axis, shift, sign):
    count = lax.axis_size(axis)
    ahead = lax.ppermute(x, axis, [(i, (i - sign) % count) for i in range(count)])
    if count == 2:
        return ahead
    behind = lax.ppermute(x, axis, [(i, (i + sign) % count) for i in range(count)])
    return jnp.where(shift[0] <= HALF, ahead, behind)


def per_device(
    features, attend_weight, output_weight, bias_table, bias_type, window_shift, grad_out
):
    levels, lats, cols, depth = features.shape
    slots = levels // WIN_LEVEL
    width, heads = output_weight.shape[0], bias_table.shape[1]
    types, count = bias_table.shape[0], bias_table.shape[2]
    assert lats == WIN_LAT and cols == WIN_LON and levels == 8 and heads * slots == 12
    assert count == WIN_LEVEL * WIN_LEVEL * WIN_LAT * PIECE
    n_head = lax.axis_size("head")
    tall = lats * levels
    number = heads * slots
    shape = jax.ShapeDtypeStruct
    x = features.transpose(1, 2, 0, 3)
    g = grad_out.transpose(1, 2, 0, 3)
    weight = attend_weight.transpose(0, 2, 1)
    table = bias_table.transpose(1, 0, 2)
    stored = [
        pltpu.with_memory_space_constraint(array, pltpu.HBM)
        for array in (x, g, weight, output_weight, table)
    ]
    raw, projected = pl.pallas_call(
        start_kernel,
        name="start",
        out_shape=[
            shape((2, lats, HALF, levels, depth), BF16),
            shape((HALF, tall, 4 * width), BF16),
        ],
        in_specs=[SMEM] + [HBM] * 4,
        out_specs=[VMEM] * 2,
        scratch_shapes=[pltpu.VMEM((4 * width, depth), BF16), pltpu.SemaphoreType.DMA((6,))],
        compiler_params=small(8),
    )(window_shift, *stored[:4])
    far = exchange(projected, "lon", window_shift, 1)
    far_raw = exchange(raw, "lon", window_shift, 1)
    natural = -(-count // LANES) * LANES + LANES
    bias, near, weights = pl.pallas_call(
        prepare_kernel,
        name="prepare",
        out_shape=[
            shape((slots, heads * WIDE, WIDE), F32),
            shape((cols, tall, 4 * LANES), BF16),
            shape((4 * LANES, depth), BF16),
        ],
        in_specs=[SMEM] + [HBM] * 5,
        out_specs=[VMEM] * 3,
        scratch_shapes=[
            pltpu.VMEM((lats, cols, levels, depth), BF16),
            pltpu.VMEM((lats, cols, levels, depth), BF16),
            pltpu.VMEM((number, count), F32),
            pltpu.VMEM((PAD, natural), F32),
            pltpu.VMEM((2 * WIN_LEVEL, number * PAD, LANES), F32),
            pltpu.SemaphoreType.DMA((number + 6,)),
        ],
        compiler_params=small(16),
    )(bias_type, *stored)
    packed = 3 * (cols // 4) * tall
    *pieces, own_back, folded = pl.pallas_call(
        main_kernel,
        name="main",
        out_shape=[shape((packed, LANES), BF16)] * n_head
        + [
            shape((cols * tall, 4 * LANES), BF16),
            shape((heads, slots * PAD, SPAN), F32),
        ],
        in_specs=[SMEM] + [VMEM] * 4,
        out_specs=[VMEM] * (n_head + 2),
        scratch_shapes=[
            pltpu.VMEM((HALF, tall, 4 * LANES), BF16),
            pltpu.VMEM((slots, WIDE, 4 * LANES), BF16),
            pltpu.VMEM((2, heads * WIDE, WIDE), F32),
            pltpu.VMEM((2, heads * WIDE, WIDE), F32),
            pltpu.VMEM((2, heads * WIDE, WIDE), BF16),
            pltpu.VMEM((2, heads * WIDE, WIDE), BF16),
            pltpu.VMEM((2, heads * WIDE, WIDE), F32),
            pltpu.VMEM((cols, slots * PAD, 4 * LANES), BF16),
            pltpu.VMEM((n_head, packed, LANES), BF16),
        ],
        compiler_params=small(24),
    )(window_shift, far, near, weights, bias)
    sums = pl.pallas_call(
        sums_kernel,
        name="weight_sums",
        out_shape=shape((4, width, depth), BF16),
        in_specs=[SMEM] + [VMEM] * 4,
        out_specs=VMEM,
        scratch_shapes=[pltpu.VMEM((2, cols * tall, depth), BF16)],
        compiler_params=small(8),
    )(window_shift, x, g, far_raw, own_back)
    parts = [pieces[0]]
    for step in range(1, n_head):
        ring = [(i, (i + step) % n_head) for i in range(n_head)]
        parts.append(lax.ppermute(pieces[step], "head", ring))
    every = ("lon", "lat")
    n_every = lax.axis_size("lon") * lax.axis_size("lat")
    shares = sums.reshape(n_every, 4 * width // n_every, depth)
    shares = lax.all_to_all(shares, every, 0, 0)
    full = natural - LANES
    dense = full + full // 2
    rows = pl.pallas_call(
        bias_kernel,
        name="bias_rows",
        out_shape=shape((8 * dense // depth, depth), BF16),
        in_specs=[SMEM, VMEM],
        out_specs=VMEM,
        scratch_shapes=[
            pltpu.VMEM((2 * WIN_LEVEL, number * PAD, LANES), F32),
            pltpu.VMEM((PAD, natural), F32),
            pltpu.VMEM((8, dense), F32),
        ],
        compiler_params=small(8),
    )(bias_type, folded)
    summed, back = pl.pallas_call(
        sum_kernel,
        name="sum_heads",
        out_shape=[shape((cols, tall, width), BF16), shape((HALF, tall, width), BF16)],
        in_specs=[SMEM] + [VMEM] * n_head,
        out_specs=[VMEM] * 2,
        compiler_params=small(6),
    )(window_shift, *parts)
    returned = exchange(back, "lon", window_shift, -1)
    share = pl.pallas_call(
        share_kernel,
        name="share",
        out_shape=shape((rows.shape[0] + shares.shape[1], depth), BF16),
        in_specs=[VMEM] * 2,
        out_specs=VMEM,
        compiler_params=small(4),
    )(shares, rows)
    gathered = lax.all_gather(share, every, axis=0)
    feature_grad, attend_grad, output_grad, bias_grad = pl.pallas_call(
        finish_kernel,
        name="finish",
        out_shape=[
            shape((lats, cols, levels, width), BF16),
            shape((3, width, depth), F32),
            shape((width, depth), F32),
            shape((heads, types, count), F32),
        ],
        in_specs=[SMEM] + [VMEM] * 3,
        out_specs=[VMEM] * 4,
        scratch_shapes=[pltpu.VMEM((8 * n_every, dense), BF16)],
        compiler_params=small(16),
    )(window_shift, gathered, summed, returned)
    return (
        feature_grad.transpose(2, 0, 1, 3),
        attend_grad.transpose(0, 2, 1),
        output_grad,
        bias_grad.transpose(1, 0, 2),
    )


def solution(mesh):
    placed = (
        P(None, "lat", "lon", None),
        P(None, None, "head"),
        P("head", None),
        P(None, "head", None),
        P(None, "lat"),
        P(),
        P(None, "lat", "lon", None),
    )
    return jax.shard_map(
        per_device,
        mesh=mesh,
        in_specs=placed,
        out_specs=(
            P(None, "lat", "lon", "head"),
            P(None, None, "head"),
            P("head", None),
            P(None, "head", None),
        ),
        check_vma=False,
    )
```

```python
import jax
import jax.numpy as jnp
from jax import lax
from jax.experimental import pallas as pl
from jax.experimental.pallas import tpu as pltpu
from jax.sharding import PartitionSpec as P


WIN_LEVEL = 2
WIN_LAT = 6
WIN_LON = 12
ROWS = WIN_LEVEL * WIN_LAT
PAD = 16
WIDE = WIN_LON * PAD
HALF = WIN_LON // 2
OFFSETS = 2 * WIN_LON - 1
PIECE = WIN_LAT * OFFSETS
LANES = 128
SPAN = -(-OFFSETS * PAD // LANES) * LANES
MASKED = -1e30
F32 = jnp.float32
BF16 = jnp.bfloat16
SMEM = pl.BlockSpec(memory_space=pltpu.SMEM)
VMEM = pl.BlockSpec(memory_space=pltpu.VMEM)
HBM = pl.BlockSpec(memory_space=pltpu.HBM)


def dot_nn(a, b):
    return lax.dot_general(a, b, (((1,), (0,)), ((), ())), preferred_element_type=F32)


def dot_nt(a, b):
    return lax.dot_general(a, b, (((1,), (1,)), ((), ())), preferred_element_type=F32)


def dot_tn(a, b):
    return lax.dot_general(a, b, (((0,), (0,)), ((), ())), preferred_element_type=F32)


def grid_of(rows, cols):
    shape = (rows, cols)
    return lax.broadcasted_iota(jnp.int32, shape, 0), lax.broadcasted_iota(jnp.int32, shape, 1)


def one_hot(hit):
    return jnp.where(hit, 1.0, 0.0).astype(BF16)


def window_order(levels):
    row, src = grid_of(levels // WIN_LEVEL * PAD, WIN_LAT * levels)
    bits = levels.bit_length() - 1
    lat = lax.shift_right_logical(src, bits)
    level = lax.bitwise_and(src, levels - 1)
    slot = lax.shift_right_logical(level, 1)
    return one_hot(row == slot * PAD + lax.bitwise_and(level, 1) * WIN_LAT + lat)


def offset_order(level_j):
    src, lane = grid_of(2 * LANES, SPAN)
    back = lax.shift_right_logical(lane, 4)
    lat = lax.bitwise_and(lane, PAD - 1) - level_j * WIN_LAT
    hit = (src == lat * OFFSETS + OFFSETS - 1 - back) & (lat >= 0) & (lat < WIN_LAT)
    return one_hot(hit & (back < OFFSETS))


def table_pieces():
    for level_i in range(WIN_LEVEL):
        for level_j in range(WIN_LEVEL):
            for lat_i in range(WIN_LAT):
                index = (level_i * WIN_LEVEL + level_j) * WIN_LAT + lat_i
                yield level_i * WIN_LAT + lat_i, level_j, index * PIECE


def run_all(copies):
    for copy in copies:
        copy.start()
    for copy in copies:
        copy.wait()


def start_kernel(
    shift_ref, x_ref, g_ref, weight_ref, out_weight_ref,
    moved_ref, own_x_ref, own_g_ref, projected_ref, rows_ref, sems,
):
    lats, _, levels, depth = x_ref.shape
    width = out_weight_ref.shape[0]
    moves = [(shift_ref, moved_ref), (x_ref, own_x_ref), (g_ref, own_g_ref)]
    moves += [(weight_ref.at[c], rows_ref.at[pl.ds(c * width, width)]) for c in range(3)]
    moves.append((out_weight_ref, rows_ref.at[pl.ds(3 * width, width)]))
    run_all([pltpu.make_async_copy(a, b, sems.at[i]) for i, (a, b) in enumerate(moves)])
    base = jnp.where(moved_ref[0] <= HALF, 0, WIN_LON - HALF)
    flat = (lats * HALF * levels, depth)
    projected = jnp.concatenate(
        [
            dot_nt(own_x_ref[:, pl.ds(base, HALF)].reshape(flat), rows_ref[: 3 * width, :]),
            dot_nt(own_g_ref[:, pl.ds(base, HALF)].reshape(flat), rows_ref[3 * width :, :]),
        ],
        axis=1,
    ).astype(BF16)
    for lat in range(lats):
        for col in range(HALF):
            start = (lat * HALF + col) * levels
            projected_ref[col, lat * levels : (lat + 1) * levels, :] = projected[
                start : start + levels, :
            ]


def prepare_kernel(
    shift_ref, x_ref, g_ref, rows_ref, kind_ref, table_ref,
    kinds_ref, raw_ref, bias_ref, near_ref, weights_ref,
    chosen_ref, natural_ref, pieces_ref, sems,
):
    lats, cols, levels, depth = x_ref.shape
    heads = table_ref.shape[0]
    slots = kind_ref.shape[1]
    count = table_ref.shape[2]
    width = rows_ref.shape[0] // 4
    number = heads * slots
    run_all([pltpu.make_async_copy(kind_ref, kinds_ref, sems.at[number])])
    copies = []
    for slot in range(slots):
        for h in range(heads):
            row = h * slots + slot
            source = table_ref.at[h, pl.ds(kinds_ref[0, slot], 1), :]
            target = chosen_ref.at[pl.ds(row, 1), :]
            copies.append(pltpu.make_async_copy(source, target, sems.at[row]))
            copies[-1].start()
    base = jnp.where(shift_ref[0] <= HALF, 0, WIN_LON - HALF)
    raw_ref[0] = x_ref[:, pl.ds(base, HALF)]
    raw_ref[1] = g_ref[:, pl.ds(base, HALF)]
    for c in range(4):
        weights_ref[c * LANES : c * LANES + width, :] = rows_ref[c * width : (c + 1) * width, :]
        weights_ref[c * LANES + width : (c + 1) * LANES, :] = jnp.zeros(
            (LANES - width, depth), BF16
        )
    flat = (lats * cols * levels, depth)
    projected = project(x_ref[...].reshape(flat), g_ref[...].reshape(flat), weights_ref[...])
    for lat in range(lats):
        for col in range(cols):
            start = (lat * cols + col) * levels
            near_ref[col, lat * levels : (lat + 1) * levels, :] = projected[
                start : start + levels, :
            ].astype(BF16)
    natural_ref[...] = jnp.zeros(natural_ref.shape, F32)
    pieces_ref[...] = jnp.zeros(pieces_ref.shape, F32)
    for copy in copies:
        copy.wait()
    natural_ref[:number, :count] = chosen_ref[...]
    for place, level_j, start in table_pieces():
        low = start // LANES * LANES
        block = natural_ref[:, low : low + 3 * LANES]
        if start > low:
            block = pltpu.roll(block, 3 * LANES - (start - low), 1)
        for t in range(2):
            pieces_ref[2 * level_j + t, pl.ds(place, number, stride=PAD), :] = block[
                :number, t * LANES : (t + 1) * LANES
            ]
    turned = jnp.zeros((number * PAD, SPAN), F32)
    for level_j in range(WIN_LEVEL):
        order = offset_order(level_j)
        rest = jnp.concatenate([pieces_ref[2 * level_j], pieces_ref[2 * level_j + 1]], axis=1)
        for _ in range(3):
            part = rest.astype(BF16)
            turned = turned + dot_nn(part, order)
            rest = rest - part.astype(F32)
    lane = lax.broadcasted_iota(jnp.int32, turned.shape, 1)
    turned = jnp.where(lax.bitwise_and(lane, PAD - 1) < ROWS, turned, MASKED)
    for h in range(heads):
        for slot in range(slots):
            row = (h * slots + slot) * PAD
            table = turned[row : row + PAD, :]
            for col in range(WIN_LON):
                by = (WIN_LON - 1 - col) * PAD
                moved = table if by == 0 else pltpu.roll(table, SPAN - by, 1)
                start = h * WIDE + col * PAD
                bias_ref[slot, start : start + PAD, :] = moved[:, :WIDE]


def project(rows_x, rows_g, weights):
    width = 3 * LANES
    return jnp.concatenate(
        [dot_nt(rows_x, weights[:width]), dot_nt(rows_g, weights[width:])], axis=1
    )


def column_source(shift, col, cols):
    low = shift <= HALF
    at = col + shift
    inside = jnp.logical_xor(low, at >= cols)
    local = jnp.where(at >= cols, at - cols, at)
    taken = jnp.where(low, at - cols, at - (cols - HALF))
    return inside, local, jnp.clip(taken, 0, HALF - 1)


def main_kernel(shift_ref, far_ref, near_ref, weights_ref, bias_ref, *rest):
    n_head = lax.axis_size("head")
    pieces = rest[:n_head]
    back_ref, folded_ref = rest[n_head : n_head + 2]
    (
        beyond_ref, ordered_ref, score_ref, slope_ref, soft_ref, grad_ref, exact_ref, given_ref,
        chunk_ref,
    ) = rest[n_head + 2 :]
    cols, tall, _ = near_ref.shape
    levels = tall // WIN_LAT
    slots = bias_ref.shape[0]
    heads = bias_ref.shape[1] // WIDE
    width = far_ref.shape[2] // 4
    size = width // heads
    scaling = size ** (-0.5)
    mine = lax.axis_index("head")
    shift = shift_ref[0]
    for c in range(4):
        beyond_ref[:, :, c * LANES : c * LANES + width] = far_ref[
            :, :, c * width : (c + 1) * width
        ]
        beyond_ref[:, :, c * LANES + width : (c + 1) * LANES] = jnp.zeros(
            (HALF, tall, LANES - width), BF16
        )
    order = window_order(levels)
    for col in range(cols):
        inside, local, taken = column_source(shift, col, cols)
        rows = jnp.where(inside, near_ref[local], beyond_ref[taken])
        ordered = dot_nn(order, rows).astype(BF16)
        for slot in range(slots):
            ordered_ref[slot, col * PAD : (col + 1) * PAD, :] = ordered[
                slot * PAD : (slot + 1) * PAD, :
            ]
    lane = lax.broadcasted_iota(jnp.int32, (WIDE, LANES), 1)
    masks = [(lane >= h * size) & (lane < (h + 1) * size) for h in range(heads)]
    none = jnp.zeros((WIDE, LANES), BF16)

    def by_head(array):
        return jnp.concatenate([jnp.where(mask, array, none) for mask in masks], axis=0)

    def own_lanes(array):
        total = jnp.where(masks[0], array[:WIDE, :], 0.0)
        for h in range(1, heads):
            total = jnp.where(masks[h], array[h * WIDE : (h + 1) * WIDE, :], total)
        return total

    block = 3 * PAD
    for slot in range(slots):
        half = slot % 2
        query = ordered_ref[slot, :, :LANES]
        key = ordered_ref[slot, :, LANES : 2 * LANES]
        value = ordered_ref[slot, :, 2 * LANES : 3 * LANES]
        queries = by_head(query)
        grads = by_head(ordered_ref[slot, :, 3 * LANES :])
        score_ref[half] = dot_nt(queries, key)
        slope_ref[half] = dot_nt(grads, value)
        for start in range(0, heads * WIDE, block):
            at = slice(start, start + block)
            scores = score_ref[half, at, :] * scaling + bias_ref[slot, at, :]
            raised = jnp.exp(scores - jnp.max(scores, axis=1, keepdims=True))
            softened = raised * (1.0 / jnp.sum(raised, axis=1, keepdims=True))
            soft_ref[half, at, :] = softened.astype(BF16)
            slope = slope_ref[half, at, :]
            inner = jnp.sum(softened * slope, axis=1, keepdims=True)
            grad_scores = softened * (slope - inner)
            grad_ref[half, at, :] = grad_scores.astype(BF16)
            exact_ref[half, at, :WIDE] = grad_scores
        for h in range(heads):
            total = jnp.zeros((PAD, SPAN), F32)
            for col in range(WIN_LON):
                by = (WIN_LON - 1 - col) * PAD
                start = h * WIDE + col * PAD
                part = jnp.concatenate(
                    [
                        exact_ref[half, start : start + PAD, :WIDE],
                        jnp.zeros((PAD, SPAN - WIDE), F32),
                    ],
                    axis=1,
                )
                total = total + (part if by == 0 else pltpu.roll(part, by, 1))
            folded_ref[h, slot * PAD : (slot + 1) * PAD, :] = total
        results = (
            own_lanes(dot_nn(grad_ref[half], key)) * scaling,
            dot_tn(grad_ref[half], queries) * scaling,
            dot_tn(soft_ref[half], grads),
            own_lanes(dot_nn(soft_ref[half], value)),
        )
        rows = slice(slot * PAD, (slot + 1) * PAD)
        for c, result in enumerate(results):
            rounded = result.astype(BF16)
            for col in range(WIN_LON):
                given_ref[col, rows, c * LANES : (c + 1) * LANES] = rounded[
                    col * PAD : (col + 1) * PAD, :
                ]
    for col in range(WIN_LON):
        back_ref[col * tall : (col + 1) * tall, :] = dot_tn(order, given_ref[col]).astype(BF16)
    piece = dot_nn(back_ref[:, : 3 * LANES], weights_ref[: 3 * LANES, :])
    group = WIN_LON // 4 * tall
    third = width // 3
    for to in range(n_head):
        lanes = piece[:, to * width : (to + 1) * width]
        for g in range(3):
            tail = lanes[3 * group :, g * third : (g + 1) * third]
            chunk_ref[to, g * group : (g + 1) * group, :] = jnp.concatenate(
                [lanes[g * group : (g + 1) * group, :], tail], axis=1
            ).astype(BF16)
    for step in range(n_head):
        pieces[step][...] = chunk_ref[lax.rem(mine + step, n_head)]


def sums_kernel(shift_ref, x_ref, g_ref, far_ref, back_ref, sums_ref, own_ref):
    lats, cols, levels, _ = x_ref.shape
    width = sums_ref.shape[1]
    for col in range(cols):
        inside, local, taken = column_source(shift_ref[0], col, cols)
        for array, ref in enumerate((x_ref, g_ref)):
            for lat in range(lats):
                start = (col * lats + lat) * levels
                own_ref[array, start : start + levels, :] = jnp.where(
                    inside, ref[lat, local], far_ref[array, lat, taken]
                )
    grads = 3 * LANES
    summed = dot_tn(back_ref[:, :grads], own_ref[0])
    for c in range(3):
        sums_ref[c] = summed[c * LANES : c * LANES + width, :].astype(BF16)
    sums_ref[3] = dot_tn(back_ref[:, grads:], own_ref[1])[:width, :].astype(BF16)


def bias_kernel(kind_ref, folded_ref, out_ref, pieces_ref, natural_ref, dense_ref):
    heads, slot_rows, span = folded_ref.shape
    slots = slot_rows // PAD
    number = heads * slots
    rows = folded_ref[...].reshape(heads * slot_rows, span).astype(BF16)
    for level_j in range(WIN_LEVEL):
        moved = dot_nt(rows, offset_order(level_j))
        for t in range(2):
            pieces_ref[2 * level_j + t] = moved[:, t * LANES : (t + 1) * LANES]
    natural_ref[...] = jnp.zeros(natural_ref.shape, F32)
    for place, level_j, start in table_pieces():
        low = start // LANES * LANES
        parts = [
            pieces_ref[2 * level_j + t, pl.ds(place, number, stride=PAD), :] for t in range(2)
        ]
        part = jnp.concatenate(parts + [jnp.zeros((number, LANES), F32)], axis=1)
        if start > low:
            part = pltpu.roll(part, start - low, 1)
        at = (slice(0, number), slice(low, low + 3 * LANES))
        natural_ref[at] = natural_ref[at] + part
    count = WIN_LEVEL * WIN_LEVEL * WIN_LAT * PIECE
    low = count // LANES * LANES
    row, lane = grid_of(number, LANES)
    kind = jnp.zeros((number, LANES), F32)
    for slot in range(slots):
        kind = jnp.where(lax.rem(row, slots) == slot, kind_ref[0, slot].astype(F32), kind)
    at = (slice(0, number), slice(low, low + LANES))
    natural_ref[at] = natural_ref[at] + jnp.where(lane == count - low, kind, 0.0)
    full = low + LANES
    middle = full // 2
    dense_ref[:, :full] = natural_ref[0:8, :full]
    dense_ref[0:4, full:] = natural_ref[8:12, :middle]
    dense_ref[4:8, full:] = natural_ref[8:12, middle:full]
    wide = out_ref.shape[1]
    for j in range(out_ref.shape[0] // 8):
        out_ref[j * 8 : (j + 1) * 8, :] = dense_ref[:, j * wide : (j + 1) * wide].astype(BF16)


def sum_kernel(shift_ref, *refs):
    parts = refs[:-2]
    summed_ref, back_ref = refs[-2:]
    shift = shift_ref[0]
    total = parts[0][...].astype(F32)
    for part in parts[1:]:
        total = total + part[...].astype(F32)
    cols, tall, width = summed_ref.shape
    group = cols // 4
    for g in range(3):
        for i in range(group):
            start = (g * group + i) * tall
            summed_ref[g * group + i] = total[start : start + tall, :width].astype(BF16)
    for i in range(group):
        tails = [
            total[(g * group + i) * tall : (g * group + i + 1) * tall, width:] for g in range(3)
        ]
        summed_ref[3 * group + i] = jnp.concatenate(tails, axis=1).astype(BF16)
    for col in range(HALF):
        source = col - shift + jnp.where(shift <= HALF, WIN_LON, WIN_LON - HALF)
        back_ref[col] = summed_ref[jnp.clip(source, 0, WIN_LON - 1)]


def share_kernel(shares_ref, rows_ref, out_ref):
    total = shares_ref[0].astype(F32)
    for i in range(1, shares_ref.shape[0]):
        total = total + shares_ref[i].astype(F32)
    count = rows_ref.shape[0]
    out_ref[:count, :] = rows_ref[...]
    out_ref[count:, :] = total.astype(BF16)


def finish_kernel(
    shift_ref, gathered_ref, summed_ref, returned_ref,
    feature_ref, attend_ref, output_ref, bias_ref, dense_ref,
):
    shift = shift_ref[0]
    low = shift <= HALF
    lats, cols, levels, width = feature_ref.shape
    for col in range(cols):
        own = jnp.logical_xor(low, col < shift)
        source = jnp.where(low, col - shift, col + cols - shift)
        given = jnp.where(low, col, col - (cols - HALF))
        rows = jnp.where(
            own,
            summed_ref[jnp.clip(source, 0, cols - 1)],
            returned_ref[jnp.clip(given, 0, HALF - 1)],
        )
        for lat in range(lats):
            feature_ref[lat, col] = rows[lat * levels : (lat + 1) * levels, :]
    _, types, count = bias_ref.shape
    devices, height, wide = gathered_ref.shape
    dense = dense_ref.shape[1] // wide
    share = height - 8 * dense
    for i in range(devices):
        start = i * share
        block = gathered_ref[i, 8 * dense :, :].astype(F32)
        if start < 3 * width:
            attend_ref[start // width, start % width : start % width + share, :] = block
        else:
            output_ref[start - 3 * width : start - 3 * width + share, :] = block
        for j in range(dense):
            dense_ref[i * 8 : (i + 1) * 8, j * wide : (j + 1) * wide] = gathered_ref[
                i, j * 8 : (j + 1) * 8, :
            ]
    full = -(-count // LANES) * LANES
    middle = full // 2
    row, lane = grid_of(devices * 8, types)
    row = lax.bitwise_and(row, 7)
    tag = count - (full - LANES)
    lane = lane.astype(F32)
    kind = dense_ref[:, full - LANES : full].astype(F32)[:, tag : tag + 1]
    for h in range(2):
        mine = (row >= 4 * h) & (row < 4 * h + 4)
        sel = one_hot((kind == lane) & mine)
        bias_ref[h] = dot_tn(sel, dense_ref[:, :full])[:, :count]
    block = dense_ref[:, full + middle - LANES : full + middle].astype(F32)
    below = block[:, tag : tag + 1]
    above = pltpu.roll(block, devices * 8 - 4, 0)[:, tag : tag + 1]
    tail = dense_ref[:, full:]
    bias_ref[2, :, :middle] = dot_tn(one_hot((above == lane) & (row < 4)), tail)
    bias_ref[2, :, middle:] = dot_tn(one_hot((below == lane) & (row >= 4)), tail)[
        :, : count - middle
    ]


def small(mebibytes):
    return pltpu.CompilerParams(vmem_limit_bytes=mebibytes << 20)


def exchange(x, axis, shift, sign):
    count = lax.axis_size(axis)
    ahead = lax.ppermute(x, axis, [(i, (i - sign) % count) for i in range(count)])
    if count == 2:
        return ahead
    behind = lax.ppermute(x, axis, [(i, (i + sign) % count) for i in range(count)])
    return jnp.where(shift[0] <= HALF, ahead, behind)


def per_device(
    features, attend_weight, output_weight, bias_table, bias_type, window_shift, grad_out
):
    levels, lats, cols, depth = features.shape
    slots = levels // WIN_LEVEL
    width, heads = output_weight.shape[0], bias_table.shape[1]
    types, count = bias_table.shape[0], bias_table.shape[2]
    assert lats == WIN_LAT and cols == WIN_LON and levels == 8 and heads * slots == 12
    assert count == WIN_LEVEL * WIN_LEVEL * WIN_LAT * PIECE
    n_head = lax.axis_size("head")
    tall = lats * levels
    number = heads * slots
    shape = jax.ShapeDtypeStruct
    x = features.transpose(1, 2, 0, 3)
    g = grad_out.transpose(1, 2, 0, 3)
    weight = attend_weight.transpose(0, 2, 1)
    table = bias_table.transpose(1, 0, 2)

    def stored(array):
        return pltpu.with_memory_space_constraint(array, pltpu.HBM)

    grid = shape(x.shape, BF16)
    shift, own_x, own_g, projected, rows = pl.pallas_call(
        start_kernel,
        name="start",
        out_shape=[
            shape((1,), jnp.int32),
            grid,
            grid,
            shape((HALF, tall, 4 * width), BF16),
            shape((4 * width, depth), BF16),
        ],
        in_specs=[HBM] * 5,
        out_specs=[SMEM] + [VMEM] * 4,
        scratch_shapes=[pltpu.SemaphoreType.DMA((7,))],
        compiler_params=small(8),
    )(window_shift, stored(x), stored(g), stored(weight), stored(output_weight))
    far = exchange(projected, "lon", shift, 1)
    natural = -(-count // LANES) * LANES + LANES
    kinds, raw, bias, near, weights = pl.pallas_call(
        prepare_kernel,
        name="prepare",
        out_shape=[
            shape((1, slots), jnp.int32),
            shape((2, lats, HALF, levels, depth), BF16),
            shape((slots, heads * WIDE, WIDE), F32),
            shape((cols, tall, 4 * LANES), BF16),
            shape((4 * LANES, depth), BF16),
        ],
        in_specs=[SMEM] + [VMEM] * 3 + [HBM] * 2,
        out_specs=[SMEM] + [VMEM] * 4,
        scratch_shapes=[
            pltpu.VMEM((number, count), F32),
            pltpu.VMEM((PAD, natural), F32),
            pltpu.VMEM((2 * WIN_LEVEL, number * PAD, LANES), F32),
            pltpu.SemaphoreType.DMA((number + 1,)),
        ],
        compiler_params=small(16),
    )(shift, own_x, own_g, rows, bias_type.reshape(1, slots), stored(table))
    far_raw = exchange(raw, "lon", shift, 1)
    packed = 3 * (cols // 4) * tall
    *pieces, own_back, folded = pl.pallas_call(
        main_kernel,
        name="main",
        out_shape=[shape((packed, LANES), BF16)] * n_head
        + [
            shape((cols * tall, 4 * LANES), BF16),
            shape((heads, slots * PAD, SPAN), F32),
        ],
        in_specs=[SMEM] + [VMEM] * 4,
        out_specs=[VMEM] * (n_head + 2),
        scratch_shapes=[
            pltpu.VMEM((HALF, tall, 4 * LANES), BF16),
            pltpu.VMEM((slots, WIDE, 4 * LANES), BF16),
            pltpu.VMEM((2, heads * WIDE, WIDE), F32),
            pltpu.VMEM((2, heads * WIDE, WIDE), F32),
            pltpu.VMEM((2, heads * WIDE, WIDE), BF16),
            pltpu.VMEM((2, heads * WIDE, WIDE), BF16),
            pltpu.VMEM((2, heads * WIDE, WIDE), F32),
            pltpu.VMEM((cols, slots * PAD, 4 * LANES), BF16),
            pltpu.VMEM((n_head, packed, LANES), BF16),
        ],
        compiler_params=small(24),
    )(shift, far, near, weights, bias)
    parts = [pieces[0]]
    for step in range(1, n_head):
        ring = [(i, (i + step) % n_head) for i in range(n_head)]
        parts.append(lax.ppermute(pieces[step], "head", ring))
    sums = pl.pallas_call(
        sums_kernel,
        name="weight_sums",
        out_shape=shape((4, width, depth), BF16),
        in_specs=[SMEM] + [VMEM] * 4,
        out_specs=VMEM,
        scratch_shapes=[pltpu.VMEM((2, cols * tall, depth), BF16)],
        compiler_params=small(8),
    )(shift, own_x, own_g, far_raw, own_back)
    every = ("lon", "lat")
    n_every = lax.axis_size("lon") * lax.axis_size("lat")
    shares = sums.reshape(n_every, 4 * width // n_every, depth)
    shares = lax.all_to_all(shares, every, 0, 0)
    full = natural - LANES
    dense = full + full // 2
    rows = pl.pallas_call(
        bias_kernel,
        name="bias_rows",
        out_shape=shape((8 * dense // depth, depth), BF16),
        in_specs=[SMEM, VMEM],
        out_specs=VMEM,
        scratch_shapes=[
            pltpu.VMEM((2 * WIN_LEVEL, number * PAD, LANES), F32),
            pltpu.VMEM((PAD, natural), F32),
            pltpu.VMEM((8, dense), F32),
        ],
        compiler_params=small(8),
    )(kinds, folded)
    summed, back = pl.pallas_call(
        sum_kernel,
        name="sum_heads",
        out_shape=[shape((cols, tall, width), BF16), shape((HALF, tall, width), BF16)],
        in_specs=[SMEM] + [VMEM] * n_head,
        out_specs=[VMEM] * 2,
        compiler_params=small(6),
    )(shift, *parts)
    returned = exchange(back, "lon", shift, -1)
    share = pl.pallas_call(
        share_kernel,
        name="share",
        out_shape=shape((rows.shape[0] + shares.shape[1], depth), BF16),
        in_specs=[VMEM] * 2,
        out_specs=VMEM,
        compiler_params=small(4),
    )(shares, rows)
    gathered = lax.all_gather(share, every, axis=0)
    feature_grad, attend_grad, output_grad, bias_grad = pl.pallas_call(
        finish_kernel,
        name="finish",
        out_shape=[
            shape((lats, cols, levels, width), BF16),
            shape((3, width, depth), F32),
            shape((width, depth), F32),
            shape((heads, types, count), F32),
        ],
        in_specs=[SMEM] + [VMEM] * 3,
        out_specs=[VMEM] * 4,
        scratch_shapes=[pltpu.VMEM((8 * n_every, dense), BF16)],
        compiler_params=small(16),
    )(shift, gathered, summed, returned)
    return (
        feature_grad.transpose(2, 0, 1, 3),
        attend_grad.transpose(0, 2, 1),
        output_grad,
        bias_grad.transpose(1, 0, 2),
    )


def solution(mesh):
    placed = (
        P(None, "lat", "lon", None),
        P(None, None, "head"),
        P("head", None),
        P(None, "head", None),
        P(None, "lat"),
        P(),
        P(None, "lat", "lon", None),
    )
    return jax.shard_map(
        per_device,
        mesh=mesh,
        in_specs=placed,
        out_specs=(
            P(None, "lat", "lon", "head"),
            P(None, None, "head"),
            P("head", None),
            P(None, "head", None),
        ),
        check_vma=False,
    )
```

```python
import jax
import jax.numpy as jnp
from jax import lax
from jax.experimental import pallas as pl
from jax.experimental.pallas import tpu as pltpu
from jax.sharding import PartitionSpec as P


WIN_LEVEL = 2
WIN_LAT = 6
WIN_LON = 12
ROWS = WIN_LEVEL * WIN_LAT
PAD = 16
WIDE = WIN_LON * PAD
HALF = WIN_LON // 2
OFFSETS = 2 * WIN_LON - 1
PIECE = WIN_LAT * OFFSETS
LANES = 128
SPAN = -(-OFFSETS * PAD // LANES) * LANES
MASKED = -1e30
F32 = jnp.float32
BF16 = jnp.bfloat16
SMEM = pl.BlockSpec(memory_space=pltpu.SMEM)
VMEM = pl.BlockSpec(memory_space=pltpu.VMEM)
HBM = pl.BlockSpec(memory_space=pltpu.HBM)


def dot_nn(a, b):
    return lax.dot_general(a, b, (((1,), (0,)), ((), ())), preferred_element_type=F32)


def dot_nt(a, b):
    return lax.dot_general(a, b, (((1,), (1,)), ((), ())), preferred_element_type=F32)


def dot_tn(a, b):
    return lax.dot_general(a, b, (((0,), (0,)), ((), ())), preferred_element_type=F32)


def grid_of(rows, cols):
    shape = (rows, cols)
    return lax.broadcasted_iota(jnp.int32, shape, 0), lax.broadcasted_iota(jnp.int32, shape, 1)


def one_hot(hit):
    return jnp.where(hit, 1.0, 0.0).astype(BF16)


def window_order(levels):
    row, src = grid_of(levels // WIN_LEVEL * PAD, WIN_LAT * levels)
    bits = levels.bit_length() - 1
    lat = lax.shift_right_logical(src, bits)
    level = lax.bitwise_and(src, levels - 1)
    slot = lax.shift_right_logical(level, 1)
    return one_hot(row == slot * PAD + lax.bitwise_and(level, 1) * WIN_LAT + lat)


def offset_order(level_j):
    src, lane = grid_of(2 * LANES, SPAN)
    back = lax.shift_right_logical(lane, 4)
    lat = lax.bitwise_and(lane, PAD - 1) - level_j * WIN_LAT
    hit = (src == lat * OFFSETS + OFFSETS - 1 - back) & (lat >= 0) & (lat < WIN_LAT)
    return one_hot(hit & (back < OFFSETS))


def table_pieces():
    for level_i in range(WIN_LEVEL):
        for level_j in range(WIN_LEVEL):
            for lat_i in range(WIN_LAT):
                index = (level_i * WIN_LEVEL + level_j) * WIN_LAT + lat_i
                yield level_i * WIN_LAT + lat_i, level_j, index * PIECE


def run_all(copies):
    for copy in copies:
        copy.start()
    for copy in copies:
        copy.wait()


def start_kernel(
    shift_ref, x_ref, g_ref, weight_ref, out_weight_ref,
    moved_ref, own_x_ref, own_g_ref, projected_ref, rows_ref, sems,
):
    lats, _, levels, depth = x_ref.shape
    width = out_weight_ref.shape[0]
    moves = [(shift_ref, moved_ref), (x_ref, own_x_ref), (g_ref, own_g_ref)]
    moves += [(weight_ref.at[c], rows_ref.at[pl.ds(c * width, width)]) for c in range(3)]
    moves.append((out_weight_ref, rows_ref.at[pl.ds(3 * width, width)]))
    run_all([pltpu.make_async_copy(a, b, sems.at[i]) for i, (a, b) in enumerate(moves)])
    base = jnp.where(moved_ref[0] <= HALF, 0, WIN_LON - HALF)
    flat = (lats * HALF * levels, depth)
    projected = jnp.concatenate(
        [
            dot_nt(own_x_ref[:, pl.ds(base, HALF)].reshape(flat), rows_ref[: 3 * width, :]),
            dot_nt(own_g_ref[:, pl.ds(base, HALF)].reshape(flat), rows_ref[3 * width :, :]),
        ],
        axis=1,
    ).astype(BF16)
    for lat in range(lats):
        for col in range(HALF):
            start = (lat * HALF + col) * levels
            projected_ref[col, lat * levels : (lat + 1) * levels, :] = projected[
                start : start + levels, :
            ]


def prepare_kernel(
    shift_ref, x_ref, g_ref, rows_ref, kind_ref, table_ref,
    kinds_ref, raw_ref, bias_ref, near_ref, weights_ref,
    chosen_ref, natural_ref, pieces_ref, sems,
):
    lats, cols, levels, depth = x_ref.shape
    heads = table_ref.shape[0]
    slots = kind_ref.shape[1]
    count = table_ref.shape[2]
    width = rows_ref.shape[0] // 4
    number = heads * slots
    run_all([pltpu.make_async_copy(kind_ref, kinds_ref, sems.at[number])])
    copies = []
    for slot in range(slots):
        for h in range(heads):
            row = h * slots + slot
            source = table_ref.at[h, pl.ds(kinds_ref[0, slot], 1), :]
            target = chosen_ref.at[pl.ds(row, 1), :]
            copies.append(pltpu.make_async_copy(source, target, sems.at[row]))
            copies[-1].start()
    base = jnp.where(shift_ref[0] <= HALF, 0, WIN_LON - HALF)
    raw_ref[0] = x_ref[:, pl.ds(base, HALF)]
    raw_ref[1] = g_ref[:, pl.ds(base, HALF)]
    for c in range(4):
        weights_ref[c * LANES : c * LANES + width, :] = rows_ref[c * width : (c + 1) * width, :]
        weights_ref[c * LANES + width : (c + 1) * LANES, :] = jnp.zeros(
            (LANES - width, depth), BF16
        )
    flat = (lats * cols * levels, depth)
    projected = project(x_ref[...].reshape(flat), g_ref[...].reshape(flat), weights_ref[...])
    for lat in range(lats):
        for col in range(cols):
            start = (lat * cols + col) * levels
            near_ref[col, lat * levels : (lat + 1) * levels, :] = projected[
                start : start + levels, :
            ].astype(BF16)
    natural_ref[...] = jnp.zeros(natural_ref.shape, F32)
    pieces_ref[...] = jnp.zeros(pieces_ref.shape, F32)
    for copy in copies:
        copy.wait()
    natural_ref[:number, :count] = chosen_ref[...]
    for place, level_j, start in table_pieces():
        low = start // LANES * LANES
        block = natural_ref[:, low : low + 3 * LANES]
        if start > low:
            block = pltpu.roll(block, 3 * LANES - (start - low), 1)
        for t in range(2):
            pieces_ref[2 * level_j + t, pl.ds(place, number, stride=PAD), :] = block[
                :number, t * LANES : (t + 1) * LANES
            ]
    turned = jnp.zeros((number * PAD, SPAN), F32)
    for level_j in range(WIN_LEVEL):
        order = offset_order(level_j)
        rest = jnp.concatenate([pieces_ref[2 * level_j], pieces_ref[2 * level_j + 1]], axis=1)
        for _ in range(3):
            part = rest.astype(BF16)
            turned = turned + dot_nn(part, order)
            rest = rest - part.astype(F32)
    lane = lax.broadcasted_iota(jnp.int32, turned.shape, 1)
    turned = jnp.where(lax.bitwise_and(lane, PAD - 1) < ROWS, turned, MASKED)
    for h in range(heads):
        for slot in range(slots):
            row = (h * slots + slot) * PAD
            table = turned[row : row + PAD, :]
            for col in range(WIN_LON):
                by = (WIN_LON - 1 - col) * PAD
                moved = table if by == 0 else pltpu.roll(table, SPAN - by, 1)
                start = h * WIDE + col * PAD
                bias_ref[slot, start : start + PAD, :] = moved[:, :WIDE]


def project(rows_x, rows_g, weights):
    width = 3 * LANES
    return jnp.concatenate(
        [dot_nt(rows_x, weights[:width]), dot_nt(rows_g, weights[width:])], axis=1
    )


def column_source(shift, col, cols):
    low = shift <= HALF
    at = col + shift
    inside = jnp.logical_xor(low, at >= cols)
    local = jnp.where(at >= cols, at - cols, at)
    taken = jnp.where(low, at - cols, at - (cols - HALF))
    return inside, local, jnp.clip(taken, 0, HALF - 1)


def main_kernel(shift_ref, far_ref, near_ref, weights_ref, bias_ref, *rest):
    n_head = lax.axis_size("head")
    pieces = rest[:n_head]
    back_ref, folded_ref = rest[n_head : n_head + 2]
    (
        beyond_ref, ordered_ref, score_ref, slope_ref, soft_ref, grad_ref, exact_ref, given_ref,
        chunk_ref,
    ) = rest[n_head + 2 :]
    cols, tall, _ = near_ref.shape
    levels = tall // WIN_LAT
    slots = bias_ref.shape[0]
    heads = bias_ref.shape[1] // WIDE
    width = far_ref.shape[2] // 4
    size = width // heads
    scaling = size ** (-0.5)
    mine = lax.axis_index("head")
    shift = shift_ref[0]
    for c in range(4):
        beyond_ref[:, :, c * LANES : c * LANES + width] = far_ref[
            :, :, c * width : (c + 1) * width
        ]
        beyond_ref[:, :, c * LANES + width : (c + 1) * LANES] = jnp.zeros(
            (HALF, tall, LANES - width), BF16
        )
    order = window_order(levels)
    for col in range(cols):
        inside, local, taken = column_source(shift, col, cols)
        rows = jnp.where(inside, near_ref[local], beyond_ref[taken])
        ordered = dot_nn(order, rows).astype(BF16)
        for slot in range(slots):
            ordered_ref[slot, col * PAD : (col + 1) * PAD, :] = ordered[
                slot * PAD : (slot + 1) * PAD, :
            ]
    lane = lax.broadcasted_iota(jnp.int32, (WIDE, LANES), 1)
    masks = [(lane >= h * size) & (lane < (h + 1) * size) for h in range(heads)]
    none = jnp.zeros((WIDE, LANES), BF16)

    def by_head(array):
        return jnp.concatenate([jnp.where(mask, array, none) for mask in masks], axis=0)

    def own_lanes(array):
        total = jnp.where(masks[0], array[:WIDE, :], 0.0)
        for h in range(1, heads):
            total = jnp.where(masks[h], array[h * WIDE : (h + 1) * WIDE, :], total)
        return total

    block = 3 * PAD
    for slot in range(slots):
        half = slot % 2
        query = ordered_ref[slot, :, :LANES]
        key = ordered_ref[slot, :, LANES : 2 * LANES]
        value = ordered_ref[slot, :, 2 * LANES : 3 * LANES]
        queries = by_head(query)
        grads = by_head(ordered_ref[slot, :, 3 * LANES :])
        score_ref[half] = dot_nt(queries, key)
        slope_ref[half] = dot_nt(grads, value)
        for start in range(0, heads * WIDE, block):
            at = slice(start, start + block)
            scores = score_ref[half, at, :] * scaling + bias_ref[slot, at, :]
            raised = jnp.exp(scores - jnp.max(scores, axis=1, keepdims=True))
            softened = raised * (1.0 / jnp.sum(raised, axis=1, keepdims=True))
            soft_ref[half, at, :] = softened.astype(BF16)
            slope = slope_ref[half, at, :]
            inner = jnp.sum(softened * slope, axis=1, keepdims=True)
            grad_scores = softened * (slope - inner)
            grad_ref[half, at, :] = grad_scores.astype(BF16)
            exact_ref[half, at, :WIDE] = grad_scores
        for h in range(heads):
            total = jnp.zeros((PAD, SPAN), F32)
            for col in range(WIN_LON):
                by = (WIN_LON - 1 - col) * PAD
                start = h * WIDE + col * PAD
                part = jnp.concatenate(
                    [
                        exact_ref[half, start : start + PAD, :WIDE],
                        jnp.zeros((PAD, SPAN - WIDE), F32),
                    ],
                    axis=1,
                )
                total = total + (part if by == 0 else pltpu.roll(part, by, 1))
            folded_ref[h, slot * PAD : (slot + 1) * PAD, :] = total
        results = (
            own_lanes(dot_nn(grad_ref[half], key)) * scaling,
            dot_tn(grad_ref[half], queries) * scaling,
            dot_tn(soft_ref[half], grads),
            own_lanes(dot_nn(soft_ref[half], value)),
        )
        rows = slice(slot * PAD, (slot + 1) * PAD)
        for c, result in enumerate(results):
            rounded = result.astype(BF16)
            for col in range(WIN_LON):
                given_ref[col, rows, c * LANES : (c + 1) * LANES] = rounded[
                    col * PAD : (col + 1) * PAD, :
                ]
    for col in range(WIN_LON):
        back_ref[col * tall : (col + 1) * tall, :] = dot_tn(order, given_ref[col]).astype(BF16)
    piece = dot_nn(back_ref[:, : 3 * LANES], weights_ref[: 3 * LANES, :])
    group = WIN_LON // 4 * tall
    third = width // 3
    for to in range(n_head):
        lanes = piece[:, to * width : (to + 1) * width]
        for g in range(3):
            tail = lanes[3 * group :, g * third : (g + 1) * third]
            chunk_ref[to, g * group : (g + 1) * group, :] = jnp.concatenate(
                [lanes[g * group : (g + 1) * group, :], tail], axis=1
            ).astype(BF16)
    for step in range(n_head):
        pieces[step][...] = chunk_ref[lax.rem(mine + step, n_head)]


def sums_kernel(shift_ref, x_ref, g_ref, far_ref, back_ref, sums_ref, own_ref):
    lats, cols, levels, _ = x_ref.shape
    width = sums_ref.shape[1]
    for col in range(cols):
        inside, local, taken = column_source(shift_ref[0], col, cols)
        for array, ref in enumerate((x_ref, g_ref)):
            for lat in range(lats):
                start = (col * lats + lat) * levels
                own_ref[array, start : start + levels, :] = jnp.where(
                    inside, ref[lat, local], far_ref[array, lat, taken]
                )
    grads = 3 * LANES
    summed = dot_tn(back_ref[:, :grads], own_ref[0])
    for c in range(3):
        sums_ref[c] = summed[c * LANES : c * LANES + width, :].astype(BF16)
    sums_ref[3] = dot_tn(back_ref[:, grads:], own_ref[1])[:width, :].astype(BF16)


def bias_kernel(kind_ref, folded_ref, out_ref, pieces_ref, natural_ref, dense_ref):
    heads, slot_rows, span = folded_ref.shape
    slots = slot_rows // PAD
    number = heads * slots
    rows = folded_ref[...].reshape(heads * slot_rows, span).astype(BF16)
    for level_j in range(WIN_LEVEL):
        moved = dot_nt(rows, offset_order(level_j))
        for t in range(2):
            pieces_ref[2 * level_j + t] = moved[:, t * LANES : (t + 1) * LANES]
    natural_ref[...] = jnp.zeros(natural_ref.shape, F32)
    for place, level_j, start in table_pieces():
        low = start // LANES * LANES
        parts = [
            pieces_ref[2 * level_j + t, pl.ds(place, number, stride=PAD), :] for t in range(2)
        ]
        part = jnp.concatenate(parts + [jnp.zeros((number, LANES), F32)], axis=1)
        if start > low:
            part = pltpu.roll(part, start - low, 1)
        at = (slice(0, number), slice(low, low + 3 * LANES))
        natural_ref[at] = natural_ref[at] + part
    count = WIN_LEVEL * WIN_LEVEL * WIN_LAT * PIECE
    low = count // LANES * LANES
    row, lane = grid_of(number, LANES)
    kind = jnp.zeros((number, LANES), F32)
    for slot in range(slots):
        kind = jnp.where(lax.rem(row, slots) == slot, kind_ref[0, slot].astype(F32), kind)
    at = (slice(0, number), slice(low, low + LANES))
    natural_ref[at] = natural_ref[at] + jnp.where(lane == count - low, kind, 0.0)
    full = low + LANES
    middle = full // 2
    dense_ref[:, :full] = natural_ref[0:8, :full]
    dense_ref[0:4, full:] = natural_ref[8:12, :middle]
    dense_ref[4:8, full:] = natural_ref[8:12, middle:full]
    wide = out_ref.shape[1]
    for j in range(out_ref.shape[0] // 8):
        out_ref[j * 8 : (j + 1) * 8, :] = dense_ref[:, j * wide : (j + 1) * wide].astype(BF16)


def sum_kernel(shift_ref, *refs):
    parts = refs[:-2]
    summed_ref, back_ref = refs[-2:]
    shift = shift_ref[0]
    total = parts[0][...].astype(F32)
    for part in parts[1:]:
        total = total + part[...].astype(F32)
    cols, tall, width = summed_ref.shape
    group = cols // 4
    for g in range(3):
        for i in range(group):
            start = (g * group + i) * tall
            summed_ref[g * group + i] = total[start : start + tall, :width].astype(BF16)
    for i in range(group):
        tails = [
            total[(g * group + i) * tall : (g * group + i + 1) * tall, width:] for g in range(3)
        ]
        summed_ref[3 * group + i] = jnp.concatenate(tails, axis=1).astype(BF16)
    for col in range(HALF):
        source = col - shift + jnp.where(shift <= HALF, WIN_LON, WIN_LON - HALF)
        back_ref[col] = summed_ref[jnp.clip(source, 0, WIN_LON - 1)]


def share_kernel(shares_ref, rows_ref, out_ref):
    total = shares_ref[0].astype(F32)
    for i in range(1, shares_ref.shape[0]):
        total = total + shares_ref[i].astype(F32)
    count = rows_ref.shape[0]
    out_ref[:count, :] = rows_ref[...]
    out_ref[count:, :] = total.astype(BF16)


def finish_kernel(
    shift_ref, gathered_ref, summed_ref, returned_ref,
    feature_ref, attend_ref, output_ref, bias_ref, dense_ref,
):
    shift = shift_ref[0]
    low = shift <= HALF
    lats, cols, levels, width = feature_ref.shape
    for col in range(cols):
        own = jnp.logical_xor(low, col < shift)
        source = jnp.where(low, col - shift, col + cols - shift)
        given = jnp.where(low, col, col - (cols - HALF))
        rows = jnp.where(
            own,
            summed_ref[jnp.clip(source, 0, cols - 1)],
            returned_ref[jnp.clip(given, 0, HALF - 1)],
        )
        for lat in range(lats):
            feature_ref[lat, col] = rows[lat * levels : (lat + 1) * levels, :]
    _, types, count = bias_ref.shape
    devices, height, wide = gathered_ref.shape
    dense = dense_ref.shape[1] // wide
    share = height - 8 * dense
    for i in range(devices):
        start = i * share
        block = gathered_ref[i, 8 * dense :, :].astype(F32)
        if start < 3 * width:
            attend_ref[start // width, start % width : start % width + share, :] = block
        else:
            output_ref[start - 3 * width : start - 3 * width + share, :] = block
        for j in range(dense):
            dense_ref[i * 8 : (i + 1) * 8, j * wide : (j + 1) * wide] = gathered_ref[
                i, j * 8 : (j + 1) * 8, :
            ]
    full = -(-count // LANES) * LANES
    middle = full // 2
    row, lane = grid_of(devices * 8, types)
    row = lax.bitwise_and(row, 7)
    tag = count - (full - LANES)
    lane = lane.astype(F32)
    kind = dense_ref[:, full - LANES : full].astype(F32)[:, tag : tag + 1]
    for h in range(2):
        mine = (row >= 4 * h) & (row < 4 * h + 4)
        sel = one_hot((kind == lane) & mine)
        bias_ref[h] = dot_tn(sel, dense_ref[:, :full])[:, :count]
    block = dense_ref[:, full + middle - LANES : full + middle].astype(F32)
    below = block[:, tag : tag + 1]
    above = pltpu.roll(block, devices * 8 - 4, 0)[:, tag : tag + 1]
    tail = dense_ref[:, full:]
    bias_ref[2, :, :middle] = dot_tn(one_hot((above == lane) & (row < 4)), tail)
    bias_ref[2, :, middle:] = dot_tn(one_hot((below == lane) & (row >= 4)), tail)[
        :, : count - middle
    ]


def small(mebibytes):
    return pltpu.CompilerParams(vmem_limit_bytes=mebibytes << 20)


def exchange(x, axis, shift, sign):
    count = lax.axis_size(axis)
    ahead = lax.ppermute(x, axis, [(i, (i - sign) % count) for i in range(count)])
    if count == 2:
        return ahead
    behind = lax.ppermute(x, axis, [(i, (i + sign) % count) for i in range(count)])
    return jnp.where(shift[0] <= HALF, ahead, behind)


def per_device(
    features, attend_weight, output_weight, bias_table, bias_type, window_shift, grad_out
):
    levels, lats, cols, depth = features.shape
    slots = levels // WIN_LEVEL
    width, heads = output_weight.shape[0], bias_table.shape[1]
    types, count = bias_table.shape[0], bias_table.shape[2]
    assert lats == WIN_LAT and cols == WIN_LON and levels == 8 and heads * slots == 12
    assert count == WIN_LEVEL * WIN_LEVEL * WIN_LAT * PIECE
    n_head = lax.axis_size("head")
    tall = lats * levels
    number = heads * slots
    shape = jax.ShapeDtypeStruct
    x = features.transpose(1, 2, 0, 3)
    g = grad_out.transpose(1, 2, 0, 3)
    weight = attend_weight.transpose(0, 2, 1)
    table = bias_table.transpose(1, 0, 2)

    def stored(array):
        return pltpu.with_memory_space_constraint(array, pltpu.HBM)

    grid = shape(x.shape, BF16)
    shift, own_x, own_g, projected, rows = pl.pallas_call(
        start_kernel,
        name="start",
        out_shape=[
            shape((1,), jnp.int32),
            grid,
            grid,
            shape((HALF, tall, 4 * width), BF16),
            shape((4 * width, depth), BF16),
        ],
        in_specs=[HBM] * 5,
        out_specs=[SMEM] + [VMEM] * 4,
        scratch_shapes=[pltpu.SemaphoreType.DMA((7,))],
        compiler_params=small(8),
    )(window_shift, stored(x), stored(g), stored(weight), stored(output_weight))
    far = exchange(projected, "lon", shift, 1)
    natural = -(-count // LANES) * LANES + LANES
    prepare = pl.pallas_call(
        prepare_kernel,
        name="prepare",
        out_shape=[
            shape((1, slots), jnp.int32),
            shape((2, lats, HALF, levels, depth), BF16),
            shape((slots, heads * WIDE, WIDE), F32),
            shape((cols, tall, 4 * LANES), BF16),
            shape((4 * LANES, depth), BF16),
        ],
        in_specs=[SMEM] + [VMEM] * 3 + [HBM] * 2,
        out_specs=[SMEM] + [VMEM] * 4,
        scratch_shapes=[
            pltpu.VMEM((number, count), F32),
            pltpu.VMEM((PAD, natural), F32),
            pltpu.VMEM((2 * WIN_LEVEL, number * PAD, LANES), F32),
            pltpu.SemaphoreType.DMA((number + 1,)),
        ],
        compiler_params=small(16),
    )
    kinds, raw, bias, near, weights = prepare(
        shift, own_x, own_g, rows, bias_type.reshape(1, slots), stored(table)
    )
    far_raw = exchange(raw, "lon", shift, 1)
    packed = 3 * (cols // 4) * tall
    *pieces, own_back, folded = pl.pallas_call(
        main_kernel,
        name="main",
        out_shape=[shape((packed, LANES), BF16)] * n_head
        + [
            shape((cols * tall, 4 * LANES), BF16),
            shape((heads, slots * PAD, SPAN), F32),
        ],
        in_specs=[SMEM] + [VMEM] * 4,
        out_specs=[VMEM] * (n_head + 2),
        scratch_shapes=[
            pltpu.VMEM((HALF, tall, 4 * LANES), BF16),
            pltpu.VMEM((slots, WIDE, 4 * LANES), BF16),
            pltpu.VMEM((2, heads * WIDE, WIDE), F32),
            pltpu.VMEM((2, heads * WIDE, WIDE), F32),
            pltpu.VMEM((2, heads * WIDE, WIDE), BF16),
            pltpu.VMEM((2, heads * WIDE, WIDE), BF16),
            pltpu.VMEM((2, heads * WIDE, WIDE), F32),
            pltpu.VMEM((cols, slots * PAD, 4 * LANES), BF16),
            pltpu.VMEM((n_head, packed, LANES), BF16),
        ],
        compiler_params=small(24),
    )(shift, far, near, weights, bias)
    parts = [pieces[0]]
    for step in range(1, n_head):
        ring = [(i, (i + step) % n_head) for i in range(n_head)]
        parts.append(lax.ppermute(pieces[step], "head", ring))
    sums = pl.pallas_call(
        sums_kernel,
        name="weight_sums",
        out_shape=shape((4, width, depth), BF16),
        in_specs=[SMEM] + [VMEM] * 4,
        out_specs=VMEM,
        scratch_shapes=[pltpu.VMEM((2, cols * tall, depth), BF16)],
        compiler_params=small(8),
    )(shift, own_x, own_g, far_raw, own_back)
    every = ("lon", "lat")
    n_every = lax.axis_size("lon") * lax.axis_size("lat")
    shares = sums.reshape(n_every, 4 * width // n_every, depth)
    shares = lax.all_to_all(shares, every, 0, 0)
    full = natural - LANES
    dense = full + full // 2
    rows = pl.pallas_call(
        bias_kernel,
        name="bias_rows",
        out_shape=shape((8 * dense // depth, depth), BF16),
        in_specs=[SMEM, VMEM],
        out_specs=VMEM,
        scratch_shapes=[
            pltpu.VMEM((2 * WIN_LEVEL, number * PAD, LANES), F32),
            pltpu.VMEM((PAD, natural), F32),
            pltpu.VMEM((8, dense), F32),
        ],
        compiler_params=small(8),
    )(kinds, folded)
    summed, back = pl.pallas_call(
        sum_kernel,
        name="sum_heads",
        out_shape=[shape((cols, tall, width), BF16), shape((HALF, tall, width), BF16)],
        in_specs=[SMEM] + [VMEM] * n_head,
        out_specs=[VMEM] * 2,
        compiler_params=small(6),
    )(shift, *parts)
    returned = exchange(back, "lon", shift, -1)
    share = pl.pallas_call(
        share_kernel,
        name="share",
        out_shape=shape((rows.shape[0] + shares.shape[1], depth), BF16),
        in_specs=[VMEM] * 2,
        out_specs=VMEM,
        compiler_params=small(4),
    )(shares, rows)
    gathered = lax.all_gather(share, every, axis=0)
    feature_grad, attend_grad, output_grad, bias_grad = pl.pallas_call(
        finish_kernel,
        name="finish",
        out_shape=[
            shape((lats, cols, levels, width), BF16),
            shape((3, width, depth), F32),
            shape((width, depth), F32),
            shape((heads, types, count), F32),
        ],
        in_specs=[SMEM] + [VMEM] * 3,
        out_specs=[VMEM] * 4,
        scratch_shapes=[pltpu.VMEM((8 * n_every, dense), BF16)],
        compiler_params=small(16),
    )(shift, gathered, summed, returned)
    return (
        feature_grad.transpose(2, 0, 1, 3),
        attend_grad.transpose(0, 2, 1),
        output_grad,
        bias_grad.transpose(1, 0, 2),
    )


def solution(mesh):
    placed = (
        P(None, "lat", "lon", None),
        P(None, None, "head"),
        P("head", None),
        P(None, "head", None),
        P(None, "lat"),
        P(),
        P(None, "lat", "lon", None),
    )
    return jax.shard_map(
        per_device,
        mesh=mesh,
        in_specs=placed,
        out_specs=(
            P(None, "lat", "lon", "head"),
            P(None, None, "head"),
            P("head", None),
            P(None, "head", None),
        ),
        check_vma=False,
    )
```

```python
import jax
import jax.numpy as jnp
from jax import lax
from jax.experimental import pallas as pl
from jax.experimental.pallas import tpu as pltpu
from jax.sharding import PartitionSpec as P


WIN_LEVEL = 2
WIN_LAT = 6
WIN_LON = 12
ROWS = WIN_LEVEL * WIN_LAT
PAD = 16
WIDE = WIN_LON * PAD
HALF = WIN_LON // 2
OFFSETS = 2 * WIN_LON - 1
PIECE = WIN_LAT * OFFSETS
LANES = 128
SPAN = -(-OFFSETS * PAD // LANES) * LANES
BIAS_ROWS = 104
MASKED = -1e30
F32 = jnp.float32
BF16 = jnp.bfloat16
SMEM = pl.BlockSpec(memory_space=pltpu.SMEM)
VMEM = pl.BlockSpec(memory_space=pltpu.VMEM)
HBM = pl.BlockSpec(memory_space=pltpu.HBM)


def dot_nn(a, b):
    return lax.dot_general(a, b, (((1,), (0,)), ((), ())), preferred_element_type=F32)


def dot_nt(a, b):
    return lax.dot_general(a, b, (((1,), (1,)), ((), ())), preferred_element_type=F32)


def dot_tn(a, b):
    return lax.dot_general(a, b, (((0,), (0,)), ((), ())), preferred_element_type=F32)


def grid_of(rows, cols):
    shape = (rows, cols)
    return lax.broadcasted_iota(jnp.int32, shape, 0), lax.broadcasted_iota(jnp.int32, shape, 1)


def one_hot(hit):
    return jnp.where(hit, 1.0, 0.0).astype(BF16)


def window_order(levels):
    row, src = grid_of(levels // WIN_LEVEL * PAD, WIN_LAT * levels)
    bits = levels.bit_length() - 1
    lat = lax.shift_right_logical(src, bits)
    level = lax.bitwise_and(src, levels - 1)
    slot = lax.shift_right_logical(level, 1)
    return one_hot(row == slot * PAD + lax.bitwise_and(level, 1) * WIN_LAT + lat)


def offset_order(level_j):
    src, lane = grid_of(2 * LANES, SPAN)
    back = lax.shift_right_logical(lane, 4)
    lat = lax.bitwise_and(lane, PAD - 1) - level_j * WIN_LAT
    hit = (src == lat * OFFSETS + OFFSETS - 1 - back) & (lat >= 0) & (lat < WIN_LAT)
    return one_hot(hit & (back < OFFSETS))


def table_pieces():
    for level_i in range(WIN_LEVEL):
        for level_j in range(WIN_LEVEL):
            for lat_i in range(WIN_LAT):
                index = (level_i * WIN_LEVEL + level_j) * WIN_LAT + lat_i
                yield level_i * WIN_LAT + lat_i, level_j, index * PIECE


def run_all(copies):
    for copy in copies:
        copy.start()
    for copy in copies:
        copy.wait()


def start_kernel(
    shift_ref, x_ref, g_ref, weight_ref, out_weight_ref,
    moved_ref, own_x_ref, own_g_ref, projected_ref, rows_ref, sems,
):
    lats, _, levels, depth = x_ref.shape
    width = out_weight_ref.shape[0]
    moves = [(shift_ref, moved_ref), (x_ref, own_x_ref), (g_ref, own_g_ref)]
    moves += [(weight_ref.at[c], rows_ref.at[pl.ds(c * width, width)]) for c in range(3)]
    moves.append((out_weight_ref, rows_ref.at[pl.ds(3 * width, width)]))
    run_all([pltpu.make_async_copy(a, b, sems.at[i]) for i, (a, b) in enumerate(moves)])
    base = jnp.where(moved_ref[0] <= HALF, 0, WIN_LON - HALF)
    flat = (lats * HALF * levels, depth)
    projected = jnp.concatenate(
        [
            dot_nt(own_x_ref[:, pl.ds(base, HALF)].reshape(flat), rows_ref[: 3 * width, :]),
            dot_nt(own_g_ref[:, pl.ds(base, HALF)].reshape(flat), rows_ref[3 * width :, :]),
        ],
        axis=1,
    ).astype(BF16)
    for lat in range(lats):
        for col in range(HALF):
            start = (lat * HALF + col) * levels
            projected_ref[col, lat * levels : (lat + 1) * levels, :] = projected[
                start : start + levels, :
            ]


def prepare_kernel(
    shift_ref, x_ref, g_ref, rows_ref, kind_ref, table_ref,
    kinds_ref, raw_ref, bias_ref, near_ref, weights_ref,
    chosen_ref, natural_ref, pieces_ref, sems,
):
    lats, cols, levels, depth = x_ref.shape
    heads = table_ref.shape[0]
    slots = kind_ref.shape[1]
    count = table_ref.shape[2]
    width = rows_ref.shape[0] // 4
    number = heads * slots
    run_all([pltpu.make_async_copy(kind_ref, kinds_ref, sems.at[number])])
    copies = []
    for slot in range(slots):
        for h in range(heads):
            row = h * slots + slot
            source = table_ref.at[h, pl.ds(kinds_ref[0, slot], 1), :]
            target = chosen_ref.at[pl.ds(row, 1), :]
            copies.append(pltpu.make_async_copy(source, target, sems.at[row]))
            copies[-1].start()
    base = jnp.where(shift_ref[0] <= HALF, 0, WIN_LON - HALF)
    raw_ref[0] = x_ref[:, pl.ds(base, HALF)]
    raw_ref[1] = g_ref[:, pl.ds(base, HALF)]
    for c in range(4):
        weights_ref[c * LANES : c * LANES + width, :] = rows_ref[c * width : (c + 1) * width, :]
        weights_ref[c * LANES + width : (c + 1) * LANES, :] = jnp.zeros(
            (LANES - width, depth), BF16
        )
    flat = (lats * cols * levels, depth)
    projected = project(x_ref[...].reshape(flat), g_ref[...].reshape(flat), weights_ref[...])
    for lat in range(lats):
        for col in range(cols):
            start = (lat * cols + col) * levels
            near_ref[col, lat * levels : (lat + 1) * levels, :] = projected[
                start : start + levels, :
            ].astype(BF16)
    natural_ref[...] = jnp.zeros(natural_ref.shape, F32)
    pieces_ref[...] = jnp.zeros(pieces_ref.shape, F32)
    for copy in copies:
        copy.wait()
    natural_ref[:number, :count] = chosen_ref[...]
    for place, level_j, start in table_pieces():
        low = start // LANES * LANES
        block = natural_ref[:, low : low + 3 * LANES]
        if start > low:
            block = pltpu.roll(block, 3 * LANES - (start - low), 1)
        for t in range(2):
            pieces_ref[2 * level_j + t, pl.ds(place, number, stride=PAD), :] = block[
                :number, t * LANES : (t + 1) * LANES
            ]
    turned = jnp.zeros((number * PAD, SPAN), F32)
    for level_j in range(WIN_LEVEL):
        order = offset_order(level_j)
        rest = jnp.concatenate([pieces_ref[2 * level_j], pieces_ref[2 * level_j + 1]], axis=1)
        for _ in range(3):
            part = rest.astype(BF16)
            turned = turned + dot_nn(part, order)
            rest = rest - part.astype(F32)
    lane = lax.broadcasted_iota(jnp.int32, turned.shape, 1)
    turned = jnp.where(lax.bitwise_and(lane, PAD - 1) < ROWS, turned, MASKED)
    for h in range(heads):
        for slot in range(slots):
            row = (h * slots + slot) * PAD
            table = turned[row : row + PAD, :]
            for col in range(WIN_LON):
                by = (WIN_LON - 1 - col) * PAD
                moved = table if by == 0 else pltpu.roll(table, SPAN - by, 1)
                start = h * WIDE + col * PAD
                bias_ref[slot, start : start + PAD, :] = moved[:, :WIDE]


def project(rows_x, rows_g, weights):
    width = 3 * LANES
    return jnp.concatenate(
        [dot_nt(rows_x, weights[:width]), dot_nt(rows_g, weights[width:])], axis=1
    )


def column_source(shift, col, cols):
    low = shift <= HALF
    at = col + shift
    inside = jnp.logical_xor(low, at >= cols)
    local = jnp.where(at >= cols, at - cols, at)
    taken = jnp.where(low, at - cols, at - (cols - HALF))
    return inside, local, jnp.clip(taken, 0, HALF - 1)


def main_kernel(shift_ref, far_ref, near_ref, weights_ref, bias_ref, *rest):
    n_head = lax.axis_size("head")
    pieces = rest[:n_head]
    back_ref, folded_ref = rest[n_head : n_head + 2]
    (
        beyond_ref, ordered_ref, score_ref, slope_ref, soft_ref, grad_ref, exact_ref, given_ref,
        chunk_ref,
    ) = rest[n_head + 2 :]
    cols, tall, _ = near_ref.shape
    levels = tall // WIN_LAT
    slots = bias_ref.shape[0]
    heads = bias_ref.shape[1] // WIDE
    width = far_ref.shape[2] // 4
    size = width // heads
    scaling = size ** (-0.5)
    mine = lax.axis_index("head")
    shift = shift_ref[0]
    for c in range(4):
        beyond_ref[:, :, c * LANES : c * LANES + width] = far_ref[
            :, :, c * width : (c + 1) * width
        ]
        beyond_ref[:, :, c * LANES + width : (c + 1) * LANES] = jnp.zeros(
            (HALF, tall, LANES - width), BF16
        )
    order = window_order(levels)
    for col in range(cols):
        inside, local, taken = column_source(shift, col, cols)
        rows = jnp.where(inside, near_ref[local], beyond_ref[taken])
        ordered = dot_nn(order, rows).astype(BF16)
        for slot in range(slots):
            ordered_ref[slot, col * PAD : (col + 1) * PAD, :] = ordered[
                slot * PAD : (slot + 1) * PAD, :
            ]
    lane = lax.broadcasted_iota(jnp.int32, (WIDE, LANES), 1)
    masks = [(lane >= h * size) & (lane < (h + 1) * size) for h in range(heads)]
    none = jnp.zeros((WIDE, LANES), BF16)

    def by_head(array):
        return jnp.concatenate([jnp.where(mask, array, none) for mask in masks], axis=0)

    def own_lanes(array):
        total = jnp.where(masks[0], array[:WIDE, :], 0.0)
        for h in range(1, heads):
            total = jnp.where(masks[h], array[h * WIDE : (h + 1) * WIDE, :], total)
        return total

    block = 3 * PAD
    for slot in range(slots):
        half = slot % 2
        query = ordered_ref[slot, :, :LANES]
        key = ordered_ref[slot, :, LANES : 2 * LANES]
        value = ordered_ref[slot, :, 2 * LANES : 3 * LANES]
        queries = by_head(query)
        grads = by_head(ordered_ref[slot, :, 3 * LANES :])
        score_ref[half] = dot_nt(queries, key)
        slope_ref[half] = dot_nt(grads, value)
        for start in range(0, heads * WIDE, block):
            at = slice(start, start + block)
            scores = score_ref[half, at, :] * scaling + bias_ref[slot, at, :]
            raised = jnp.exp(scores - jnp.max(scores, axis=1, keepdims=True))
            softened = raised * (1.0 / jnp.sum(raised, axis=1, keepdims=True))
            soft_ref[half, at, :] = softened.astype(BF16)
            slope = slope_ref[half, at, :]
            inner = jnp.sum(softened * slope, axis=1, keepdims=True)
            grad_scores = softened * (slope - inner)
            grad_ref[half, at, :] = grad_scores.astype(BF16)
            exact_ref[half, at, :WIDE] = grad_scores
        for h in range(heads):
            total = jnp.zeros((PAD, SPAN), F32)
            for col in range(WIN_LON):
                by = (WIN_LON - 1 - col) * PAD
                start = h * WIDE + col * PAD
                part = jnp.concatenate(
                    [
                        exact_ref[half, start : start + PAD, :WIDE],
                        jnp.zeros((PAD, SPAN - WIDE), F32),
                    ],
                    axis=1,
                )
                total = total + (part if by == 0 else pltpu.roll(part, by, 1))
            folded_ref[h, slot * PAD : (slot + 1) * PAD, :] = total
        results = (
            own_lanes(dot_nn(grad_ref[half], key)) * scaling,
            dot_tn(grad_ref[half], queries) * scaling,
            dot_tn(soft_ref[half], grads),
            own_lanes(dot_nn(soft_ref[half], value)),
        )
        rows = slice(slot * PAD, (slot + 1) * PAD)
        for c, result in enumerate(results):
            rounded = result.astype(BF16)
            for col in range(WIN_LON):
                given_ref[col, rows, c * LANES : (c + 1) * LANES] = rounded[
                    col * PAD : (col + 1) * PAD, :
                ]
    for col in range(WIN_LON):
        back_ref[col * tall : (col + 1) * tall, :] = dot_tn(order, given_ref[col]).astype(BF16)
    piece = dot_nn(back_ref[:, : 3 * LANES], weights_ref[: 3 * LANES, :])
    group = WIN_LON // 4 * tall
    third = width // 3
    for to in range(n_head):
        lanes = piece[:, to * width : (to + 1) * width]
        for g in range(3):
            tail = lanes[3 * group :, g * third : (g + 1) * third]
            chunk_ref[to, g * group : (g + 1) * group, :] = jnp.concatenate(
                [lanes[g * group : (g + 1) * group, :], tail], axis=1
            ).astype(BF16)
    for step in range(n_head):
        pieces[step][...] = chunk_ref[lax.rem(mine + step, n_head)]


def sums_kernel(shift_ref, x_ref, g_ref, far_ref, back_ref, *refs):
    *halves, sums_ref, own_ref = refs
    lats, cols, levels, _ = x_ref.shape
    width = sums_ref.shape[1]
    for col in range(cols):
        inside, local, taken = column_source(shift_ref[0], col, cols)
        for array, ref in enumerate((x_ref, g_ref)):
            for lat in range(lats):
                start = (col * lats + lat) * levels
                own_ref[array, start : start + levels, :] = jnp.where(
                    inside, ref[lat, local], far_ref[array, lat, taken]
                )
    grads = 3 * LANES
    summed = dot_tn(back_ref[:, :grads], own_ref[0])
    for c in range(3):
        sums_ref[c] = summed[c * LANES : c * LANES + width, :].astype(BF16)
    sums_ref[3] = dot_tn(back_ref[:, grads:], own_ref[1])[:width, :].astype(BF16)
    if halves:
        core = lax.rem(lax.axis_index("lat"), 2)
        for ref, side in zip(halves, (core, 1 - core)):
            for i in range(2):
                ref[i * width : (i + 1) * width, :] = sums_ref[2 * side + i]


def pair_kernel(kept_ref, got_ref, rows_ref, out_ref):
    count = rows_ref.shape[0]
    out_ref[:count, :] = rows_ref[...]
    out_ref[count:, :] = (kept_ref[...].astype(F32) + got_ref[...].astype(F32)).astype(BF16)


def merge_kernel(*refs):
    *parts, out_ref, all_ref = refs
    chip = lax.axis_index("lon") * 2 + lax.div(lax.axis_index("lat"), 2)
    for i, part in enumerate(parts):
        all_ref[lax.bitwise_xor(chip, i)] = part[...]
    share = (parts[0].shape[0] - BIAS_ROWS) // 2
    for j in range(2):
        low = all_ref[j, :BIAS_ROWS, :].astype(F32)
        high = all_ref[2 + j, :BIAS_ROWS, :].astype(F32)
        out_ref[j, :BIAS_ROWS, :] = (low + high).astype(BF16)
        start = BIAS_ROWS + j * share
        total = all_ref[0, start : start + share, :].astype(F32)
        for i in range(1, 4):
            total = total + all_ref[i, start : start + share, :].astype(F32)
        out_ref[j, BIAS_ROWS:, :] = total.astype(BF16)


def bias_kernel(kind_ref, folded_ref, out_ref, pieces_ref, natural_ref, dense_ref):
    heads, slot_rows, span = folded_ref.shape
    slots = slot_rows // PAD
    number = heads * slots
    rows = folded_ref[...].reshape(heads * slot_rows, span).astype(BF16)
    for level_j in range(WIN_LEVEL):
        moved = dot_nt(rows, offset_order(level_j))
        for t in range(2):
            pieces_ref[2 * level_j + t] = moved[:, t * LANES : (t + 1) * LANES]
    natural_ref[...] = jnp.zeros(natural_ref.shape, F32)
    for place, level_j, start in table_pieces():
        low = start // LANES * LANES
        parts = [
            pieces_ref[2 * level_j + t, pl.ds(place, number, stride=PAD), :] for t in range(2)
        ]
        part = jnp.concatenate(parts + [jnp.zeros((number, LANES), F32)], axis=1)
        if start > low:
            part = pltpu.roll(part, start - low, 1)
        at = (slice(0, number), slice(low, low + 3 * LANES))
        natural_ref[at] = natural_ref[at] + part
    count = WIN_LEVEL * WIN_LEVEL * WIN_LAT * PIECE
    low = count // LANES * LANES
    row, lane = grid_of(number, LANES)
    kind = jnp.zeros((number, LANES), F32)
    for slot in range(slots):
        kind = jnp.where(lax.rem(row, slots) == slot, kind_ref[0, slot].astype(F32), kind)
    at = (slice(0, number), slice(low, low + LANES))
    natural_ref[at] = natural_ref[at] + jnp.where(lane == count - low, kind, 0.0)
    full = low + LANES
    middle = full // 2
    dense_ref[:, :full] = natural_ref[0:8, :full]
    dense_ref[0:4, full:] = natural_ref[8:12, :middle]
    dense_ref[4:8, full:] = natural_ref[8:12, middle:full]
    wide = out_ref.shape[1]
    for j in range(out_ref.shape[0] // 8):
        out_ref[j * 8 : (j + 1) * 8, :] = dense_ref[:, j * wide : (j + 1) * wide].astype(BF16)


def sum_kernel(shift_ref, *refs):
    parts = refs[:-2]
    summed_ref, back_ref = refs[-2:]
    shift = shift_ref[0]
    total = parts[0][...].astype(F32)
    for part in parts[1:]:
        total = total + part[...].astype(F32)
    cols, tall, width = summed_ref.shape
    group = cols // 4
    for g in range(3):
        for i in range(group):
            start = (g * group + i) * tall
            summed_ref[g * group + i] = total[start : start + tall, :width].astype(BF16)
    for i in range(group):
        tails = [
            total[(g * group + i) * tall : (g * group + i + 1) * tall, width:] for g in range(3)
        ]
        summed_ref[3 * group + i] = jnp.concatenate(tails, axis=1).astype(BF16)
    for col in range(HALF):
        source = col - shift + jnp.where(shift <= HALF, WIN_LON, WIN_LON - HALF)
        back_ref[col] = summed_ref[jnp.clip(source, 0, WIN_LON - 1)]


def share_kernel(shares_ref, rows_ref, out_ref):
    total = shares_ref[0].astype(F32)
    for i in range(1, shares_ref.shape[0]):
        total = total + shares_ref[i].astype(F32)
    count = rows_ref.shape[0]
    out_ref[:count, :] = rows_ref[...]
    out_ref[count:, :] = total.astype(BF16)


def finish_kernel(shift_ref, *refs):
    *gathered, summed_ref, returned_ref, feature_ref, attend_ref, output_ref, bias_ref, dense_ref = refs
    if len(gathered) == 1:
        devices, height, wide = gathered[0].shape
        copies = 1

        def entry(i, rows):
            return gathered[0][i, rows, :]
    else:
        devices, height, wide = 4, *gathered[0].shape[1:]
        copies = 2
        core = lax.rem(lax.axis_index("lat"), 2)

        def entry(i, rows):
            mine, other = (ref[i % 2, rows, :] for ref in gathered)
            return jnp.where(core == i // 2, mine, other)

    shift = shift_ref[0]
    low = shift <= HALF
    lats, cols, levels, width = feature_ref.shape
    for col in range(cols):
        own = jnp.logical_xor(low, col < shift)
        source = jnp.where(low, col - shift, col + cols - shift)
        given = jnp.where(low, col, col - (cols - HALF))
        rows = jnp.where(
            own,
            summed_ref[jnp.clip(source, 0, cols - 1)],
            returned_ref[jnp.clip(given, 0, HALF - 1)],
        )
        for lat in range(lats):
            feature_ref[lat, col] = rows[lat * levels : (lat + 1) * levels, :]
    _, types, count = bias_ref.shape
    dense = dense_ref.shape[1] // wide
    share = height - 8 * dense
    for i in range(devices):
        start = i * share
        block = entry(i, slice(8 * dense, height)).astype(F32)
        if start < 3 * width:
            attend_ref[start // width, start % width : start % width + share, :] = block
        else:
            output_ref[start - 3 * width : start - 3 * width + share, :] = block
        for j in range(dense):
            dense_ref[i * 8 : (i + 1) * 8, j * wide : (j + 1) * wide] = entry(
                i, slice(j * 8, (j + 1) * 8)
            )
    full = -(-count // LANES) * LANES
    middle = full // 2
    row, lane = grid_of(devices * 8, types)
    row = lax.bitwise_and(row, 7)
    tag = count - (full - LANES)
    lane = lane.astype(F32) * copies
    kind = dense_ref[:, full - LANES : full].astype(F32)[:, tag : tag + 1]
    for h in range(2):
        mine = (row >= 4 * h) & (row < 4 * h + 4)
        sel = one_hot((kind == lane) & mine)
        bias_ref[h] = dot_tn(sel, dense_ref[:, :full])[:, :count]
    block = dense_ref[:, full + middle - LANES : full + middle].astype(F32)
    below = block[:, tag : tag + 1]
    above = pltpu.roll(block, devices * 8 - 4, 0)[:, tag : tag + 1]
    tail = dense_ref[:, full:]
    bias_ref[2, :, :middle] = dot_tn(one_hot((above == lane) & (row < 4)), tail)
    bias_ref[2, :, middle:] = dot_tn(one_hot((below == lane) & (row >= 4)), tail)[
        :, : count - middle
    ]


def small(mebibytes):
    return pltpu.CompilerParams(vmem_limit_bytes=mebibytes << 20)


def exchange(x, axis, shift, sign):
    count = lax.axis_size(axis)
    ahead = lax.ppermute(x, axis, [(i, (i - sign) % count) for i in range(count)])
    if count == 2:
        return ahead
    behind = lax.ppermute(x, axis, [(i, (i + sign) % count) for i in range(count)])
    return jnp.where(shift[0] <= HALF, ahead, behind)


def per_device(
    features, attend_weight, output_weight, bias_table, bias_type, window_shift, grad_out
):
    levels, lats, cols, depth = features.shape
    slots = levels // WIN_LEVEL
    width, heads = output_weight.shape[0], bias_table.shape[1]
    types, count = bias_table.shape[0], bias_table.shape[2]
    assert lats == WIN_LAT and cols == WIN_LON and levels == 8 and heads * slots == 12
    assert count == WIN_LEVEL * WIN_LEVEL * WIN_LAT * PIECE
    n_head = lax.axis_size("head")
    tall = lats * levels
    number = heads * slots
    shape = jax.ShapeDtypeStruct
    x = features.transpose(1, 2, 0, 3)
    g = grad_out.transpose(1, 2, 0, 3)
    weight = attend_weight.transpose(0, 2, 1)
    table = bias_table.transpose(1, 0, 2)

    def stored(array):
        return pltpu.with_memory_space_constraint(array, pltpu.HBM)

    grid = shape(x.shape, BF16)
    shift, own_x, own_g, projected, rows = pl.pallas_call(
        start_kernel,
        name="start",
        out_shape=[
            shape((1,), jnp.int32),
            grid,
            grid,
            shape((HALF, tall, 4 * width), BF16),
            shape((4 * width, depth), BF16),
        ],
        in_specs=[HBM] * 5,
        out_specs=[SMEM] + [VMEM] * 4,
        scratch_shapes=[pltpu.SemaphoreType.DMA((7,))],
        compiler_params=small(8),
    )(window_shift, stored(x), stored(g), stored(weight), stored(output_weight))
    far = exchange(projected, "lon", shift, 1)
    natural = -(-count // LANES) * LANES + LANES
    prepare = pl.pallas_call(
        prepare_kernel,
        name="prepare",
        out_shape=[
            shape((1, slots), jnp.int32),
            shape((2, lats, HALF, levels, depth), BF16),
            shape((slots, heads * WIDE, WIDE), F32),
            shape((cols, tall, 4 * LANES), BF16),
            shape((4 * LANES, depth), BF16),
        ],
        in_specs=[SMEM] + [VMEM] * 3 + [HBM] * 2,
        out_specs=[SMEM] + [VMEM] * 4,
        scratch_shapes=[
            pltpu.VMEM((number, count), F32),
            pltpu.VMEM((PAD, natural), F32),
            pltpu.VMEM((2 * WIN_LEVEL, number * PAD, LANES), F32),
            pltpu.SemaphoreType.DMA((number + 1,)),
        ],
        compiler_params=small(16),
    )
    kinds, raw, bias, near, weights = prepare(
        shift, own_x, own_g, rows, bias_type.reshape(1, slots), stored(table)
    )
    far_raw = exchange(raw, "lon", shift, 1)
    packed = 3 * (cols // 4) * tall
    *pieces, own_back, folded = pl.pallas_call(
        main_kernel,
        name="main",
        out_shape=[shape((packed, LANES), BF16)] * n_head
        + [
            shape((cols * tall, 4 * LANES), BF16),
            shape((heads, slots * PAD, SPAN), F32),
        ],
        in_specs=[SMEM] + [VMEM] * 4,
        out_specs=[VMEM] * (n_head + 2),
        scratch_shapes=[
            pltpu.VMEM((HALF, tall, 4 * LANES), BF16),
            pltpu.VMEM((slots, WIDE, 4 * LANES), BF16),
            pltpu.VMEM((2, heads * WIDE, WIDE), F32),
            pltpu.VMEM((2, heads * WIDE, WIDE), F32),
            pltpu.VMEM((2, heads * WIDE, WIDE), BF16),
            pltpu.VMEM((2, heads * WIDE, WIDE), BF16),
            pltpu.VMEM((2, heads * WIDE, WIDE), F32),
            pltpu.VMEM((cols, slots * PAD, 4 * LANES), BF16),
            pltpu.VMEM((n_head, packed, LANES), BF16),
        ],
        compiler_params=small(24),
    )(shift, far, near, weights, bias)
    parts = [pieces[0]]
    for step in range(1, n_head):
        ring = [(i, (i + step) % n_head) for i in range(n_head)]
        parts.append(lax.ppermute(pieces[step], "head", ring))
    every = ("lon", "lat")
    n_lon, n_lat = lax.axis_size("lon"), lax.axis_size("lat")
    n_every = n_lon * n_lat
    paired = n_lon == 2 and n_lat == 4
    halves = [shape((2 * width, depth), BF16)] * 2 if paired else []
    *halves, sums = pl.pallas_call(
        sums_kernel,
        name="weight_sums",
        out_shape=halves + [shape((4, width, depth), BF16)],
        in_specs=[SMEM] + [VMEM] * 4,
        out_specs=[VMEM] * (len(halves) + 1),
        scratch_shapes=[pltpu.VMEM((2, cols * tall, depth), BF16)],
        compiler_params=small(8),
    )(shift, own_x, own_g, far_raw, own_back)
    if paired:
        got = lax.ppermute(halves[1], "lat", [(i, i ^ 1) for i in range(n_lat)])
    else:
        shares = sums.reshape(n_every, 4 * width // n_every, depth)
        shares = lax.all_to_all(shares, every, 0, 0)
    full = natural - LANES
    dense = full + full // 2
    assert 8 * dense == BIAS_ROWS * depth
    rows = pl.pallas_call(
        bias_kernel,
        name="bias_rows",
        out_shape=shape((8 * dense // depth, depth), BF16),
        in_specs=[SMEM, VMEM],
        out_specs=VMEM,
        scratch_shapes=[
            pltpu.VMEM((2 * WIN_LEVEL, number * PAD, LANES), F32),
            pltpu.VMEM((PAD, natural), F32),
            pltpu.VMEM((8, dense), F32),
        ],
        compiler_params=small(8),
    )(kinds, folded)
    summed, back = pl.pallas_call(
        sum_kernel,
        name="sum_heads",
        out_shape=[shape((cols, tall, width), BF16), shape((HALF, tall, width), BF16)],
        in_specs=[SMEM] + [VMEM] * n_head,
        out_specs=[VMEM] * 2,
        compiler_params=small(6),
    )(shift, *parts)
    returned = exchange(back, "lon", shift, -1)
    if paired:
        part = pl.pallas_call(
            pair_kernel,
            name="pair",
            out_shape=shape((rows.shape[0] + 2 * width, depth), BF16),
            in_specs=[VMEM] * 3,
            out_specs=VMEM,
            compiler_params=small(4),
        )(halves[0], got, rows)
        chips = [part]
        for step in range(1, 4):
            ring = [(i, i ^ (2 * step)) for i in range(n_every)]
            chips.append(lax.ppermute(part, every, ring))
        merged = pl.pallas_call(
            merge_kernel,
            name="merge",
            out_shape=shape((2, rows.shape[0] + width, depth), BF16),
            in_specs=[VMEM] * 4,
            out_specs=VMEM,
            scratch_shapes=[pltpu.VMEM((4, *part.shape), BF16)],
            compiler_params=small(6),
        )(*chips)
        other = lax.ppermute(merged, "lat", [(i, i ^ 1) for i in range(n_lat)])
        gathered = [merged, other]
    else:
        share = pl.pallas_call(
            share_kernel,
            name="share",
            out_shape=shape((rows.shape[0] + shares.shape[1], depth), BF16),
            in_specs=[VMEM] * 2,
            out_specs=VMEM,
            compiler_params=small(4),
        )(shares, rows)
        gathered = [lax.all_gather(share, every, axis=0)]
    feature_grad, attend_grad, output_grad, bias_grad = pl.pallas_call(
        finish_kernel,
        name="finish",
        out_shape=[
            shape((lats, cols, levels, width), BF16),
            shape((3, width, depth), F32),
            shape((width, depth), F32),
            shape((heads, types, count), F32),
        ],
        in_specs=[SMEM] + [VMEM] * (len(gathered) + 2),
        out_specs=[VMEM] * 4,
        scratch_shapes=[pltpu.VMEM((8 * (4 if paired else n_every), dense), BF16)],
        compiler_params=small(16),
    )(shift, *gathered, summed, returned)
    return (
        feature_grad.transpose(2, 0, 1, 3),
        attend_grad.transpose(0, 2, 1),
        output_grad,
        bias_grad.transpose(1, 0, 2),
    )


def solution(mesh):
    placed = (
        P(None, "lat", "lon", None),
        P(None, None, "head"),
        P("head", None),
        P(None, "head", None),
        P(None, "lat"),
        P(),
        P(None, "lat", "lon", None),
    )
    return jax.shard_map(
        per_device,
        mesh=mesh,
        in_specs=placed,
        out_specs=(
            P(None, "lat", "lon", "head"),
            P(None, None, "head"),
            P("head", None),
            P(None, "head", None),
        ),
        check_vma=False,
    )
```

```python
import jax
import jax.numpy as jnp
from jax import lax
from jax.experimental import pallas as pl
from jax.experimental.pallas import tpu as pltpu
from jax.sharding import PartitionSpec as P


WIN_LEVEL = 2
WIN_LAT = 6
WIN_LON = 12
ROWS = WIN_LEVEL * WIN_LAT
PAD = 16
WIDE = WIN_LON * PAD
HALF = WIN_LON // 2
OFFSETS = 2 * WIN_LON - 1
PIECE = WIN_LAT * OFFSETS
LANES = 128
SPAN = -(-OFFSETS * PAD // LANES) * LANES
BIAS_ROWS = 104
MASKED = -1e30
F32 = jnp.float32
BF16 = jnp.bfloat16
SMEM = pl.BlockSpec(memory_space=pltpu.SMEM)
VMEM = pl.BlockSpec(memory_space=pltpu.VMEM)
HBM = pl.BlockSpec(memory_space=pltpu.HBM)


def dot_nn(a, b):
    return lax.dot_general(a, b, (((1,), (0,)), ((), ())), preferred_element_type=F32)


def dot_nt(a, b):
    return lax.dot_general(a, b, (((1,), (1,)), ((), ())), preferred_element_type=F32)


def dot_tn(a, b):
    return lax.dot_general(a, b, (((0,), (0,)), ((), ())), preferred_element_type=F32)


def grid_of(rows, cols):
    shape = (rows, cols)
    return lax.broadcasted_iota(jnp.int32, shape, 0), lax.broadcasted_iota(jnp.int32, shape, 1)


def one_hot(hit):
    return jnp.where(hit, 1.0, 0.0).astype(BF16)


def window_order(levels):
    row, src = grid_of(levels // WIN_LEVEL * PAD, WIN_LAT * levels)
    bits = levels.bit_length() - 1
    lat = lax.shift_right_logical(src, bits)
    level = lax.bitwise_and(src, levels - 1)
    slot = lax.shift_right_logical(level, 1)
    return one_hot(row == slot * PAD + lax.bitwise_and(level, 1) * WIN_LAT + lat)


def offset_order(level_j):
    src, lane = grid_of(2 * LANES, SPAN)
    back = lax.shift_right_logical(lane, 4)
    lat = lax.bitwise_and(lane, PAD - 1) - level_j * WIN_LAT
    hit = (src == lat * OFFSETS + OFFSETS - 1 - back) & (lat >= 0) & (lat < WIN_LAT)
    return one_hot(hit & (back < OFFSETS))


def table_pieces():
    for level_i in range(WIN_LEVEL):
        for level_j in range(WIN_LEVEL):
            for lat_i in range(WIN_LAT):
                index = (level_i * WIN_LEVEL + level_j) * WIN_LAT + lat_i
                yield level_i * WIN_LAT + lat_i, level_j, index * PIECE


def run_all(copies):
    for copy in copies:
        copy.start()
    for copy in copies:
        copy.wait()


def start_kernel(
    shift_ref, x_ref, g_ref, weight_ref, out_weight_ref,
    moved_ref, own_x_ref, own_g_ref, projected_ref, rows_ref, sems,
):
    lats, _, levels, depth = x_ref.shape
    width = out_weight_ref.shape[0]
    moves = [(shift_ref, moved_ref), (x_ref, own_x_ref), (g_ref, own_g_ref)]
    moves += [(weight_ref.at[c], rows_ref.at[pl.ds(c * width, width)]) for c in range(3)]
    moves.append((out_weight_ref, rows_ref.at[pl.ds(3 * width, width)]))
    run_all([pltpu.make_async_copy(a, b, sems.at[i]) for i, (a, b) in enumerate(moves)])
    base = jnp.where(moved_ref[0] <= HALF, 0, WIN_LON - HALF)
    flat = (lats * HALF * levels, depth)
    projected = jnp.concatenate(
        [
            dot_nt(own_x_ref[:, pl.ds(base, HALF)].reshape(flat), rows_ref[: 3 * width, :]),
            dot_nt(own_g_ref[:, pl.ds(base, HALF)].reshape(flat), rows_ref[3 * width :, :]),
        ],
        axis=1,
    ).astype(BF16)
    for lat in range(lats):
        for col in range(HALF):
            start = (lat * HALF + col) * levels
            projected_ref[col, lat * levels : (lat + 1) * levels, :] = projected[
                start : start + levels, :
            ]


def prepare_kernel(
    shift_ref, x_ref, g_ref, rows_ref, kind_ref, table_ref,
    kinds_ref, raw_ref, bias_ref, near_ref, weights_ref,
    chosen_ref, natural_ref, pieces_ref, sems,
):
    lats, cols, levels, depth = x_ref.shape
    heads = table_ref.shape[0]
    slots = kind_ref.shape[1]
    count = table_ref.shape[2]
    width = rows_ref.shape[0] // 4
    number = heads * slots
    run_all([pltpu.make_async_copy(kind_ref, kinds_ref, sems.at[number])])
    copies = []
    for slot in range(slots):
        for h in range(heads):
            row = h * slots + slot
            source = table_ref.at[h, pl.ds(kinds_ref[0, slot], 1), :]
            target = chosen_ref.at[pl.ds(row, 1), :]
            copies.append(pltpu.make_async_copy(source, target, sems.at[row]))
            copies[-1].start()
    base = jnp.where(shift_ref[0] <= HALF, 0, WIN_LON - HALF)
    raw_ref[0] = x_ref[:, pl.ds(base, HALF)]
    raw_ref[1] = g_ref[:, pl.ds(base, HALF)]
    for c in range(4):
        weights_ref[c * LANES : c * LANES + width, :] = rows_ref[c * width : (c + 1) * width, :]
        weights_ref[c * LANES + width : (c + 1) * LANES, :] = jnp.zeros(
            (LANES - width, depth), BF16
        )
    flat = (lats * cols * levels, depth)
    projected = project(x_ref[...].reshape(flat), g_ref[...].reshape(flat), weights_ref[...])
    for lat in range(lats):
        for col in range(cols):
            start = (lat * cols + col) * levels
            near_ref[col, lat * levels : (lat + 1) * levels, :] = projected[
                start : start + levels, :
            ].astype(BF16)
    natural_ref[...] = jnp.zeros(natural_ref.shape, F32)
    pieces_ref[...] = jnp.zeros(pieces_ref.shape, F32)
    for copy in copies:
        copy.wait()
    natural_ref[:number, :count] = chosen_ref[...]
    for place, level_j, start in table_pieces():
        low = start // LANES * LANES
        block = natural_ref[:, low : low + 3 * LANES]
        if start > low:
            block = pltpu.roll(block, 3 * LANES - (start - low), 1)
        for t in range(2):
            pieces_ref[2 * level_j + t, pl.ds(place, number, stride=PAD), :] = block[
                :number, t * LANES : (t + 1) * LANES
            ]
    turned = jnp.zeros((number * PAD, SPAN), F32)
    for level_j in range(WIN_LEVEL):
        order = offset_order(level_j)
        rest = jnp.concatenate([pieces_ref[2 * level_j], pieces_ref[2 * level_j + 1]], axis=1)
        for _ in range(3):
            part = rest.astype(BF16)
            turned = turned + dot_nn(part, order)
            rest = rest - part.astype(F32)
    lane = lax.broadcasted_iota(jnp.int32, turned.shape, 1)
    turned = jnp.where(lax.bitwise_and(lane, PAD - 1) < ROWS, turned, MASKED)
    for h in range(heads):
        for slot in range(slots):
            row = (h * slots + slot) * PAD
            table = turned[row : row + PAD, :]
            for col in range(WIN_LON):
                by = (WIN_LON - 1 - col) * PAD
                moved = table if by == 0 else pltpu.roll(table, SPAN - by, 1)
                start = h * WIDE + col * PAD
                bias_ref[slot, start : start + PAD, :] = moved[:, :WIDE]


def project(rows_x, rows_g, weights):
    width = 3 * LANES
    return jnp.concatenate(
        [dot_nt(rows_x, weights[:width]), dot_nt(rows_g, weights[width:])], axis=1
    )


def column_source(shift, col, cols):
    low = shift <= HALF
    at = col + shift
    inside = jnp.logical_xor(low, at >= cols)
    local = jnp.where(at >= cols, at - cols, at)
    taken = jnp.where(low, at - cols, at - (cols - HALF))
    return inside, local, jnp.clip(taken, 0, HALF - 1)


def main_kernel(shift_ref, far_ref, near_ref, weights_ref, bias_ref, *rest):
    n_head = lax.axis_size("head")
    pieces = rest[:n_head]
    back_ref, folded_ref = rest[n_head : n_head + 2]
    (
        beyond_ref, ordered_ref, score_ref, slope_ref, soft_ref, grad_ref, exact_ref, given_ref,
        chunk_ref,
    ) = rest[n_head + 2 :]
    cols, tall, _ = near_ref.shape
    levels = tall // WIN_LAT
    slots = bias_ref.shape[0]
    heads = bias_ref.shape[1] // WIDE
    width = far_ref.shape[2] // 4
    size = width // heads
    scaling = size ** (-0.5)
    mine = lax.axis_index("head")
    shift = shift_ref[0]
    for c in range(4):
        beyond_ref[:, :, c * LANES : c * LANES + width] = far_ref[
            :, :, c * width : (c + 1) * width
        ]
        beyond_ref[:, :, c * LANES + width : (c + 1) * LANES] = jnp.zeros(
            (HALF, tall, LANES - width), BF16
        )
    order = window_order(levels)
    for col in range(cols):
        inside, local, taken = column_source(shift, col, cols)
        rows = jnp.where(inside, near_ref[local], beyond_ref[taken])
        ordered = dot_nn(order, rows).astype(BF16)
        for slot in range(slots):
            ordered_ref[slot, col * PAD : (col + 1) * PAD, :] = ordered[
                slot * PAD : (slot + 1) * PAD, :
            ]
    lane = lax.broadcasted_iota(jnp.int32, (WIDE, LANES), 1)
    masks = [(lane >= h * size) & (lane < (h + 1) * size) for h in range(heads)]
    none = jnp.zeros((WIDE, LANES), BF16)

    def by_head(array):
        return jnp.concatenate([jnp.where(mask, array, none) for mask in masks], axis=0)

    def own_lanes(array):
        total = jnp.where(masks[0], array[:WIDE, :], 0.0)
        for h in range(1, heads):
            total = jnp.where(masks[h], array[h * WIDE : (h + 1) * WIDE, :], total)
        return total

    block = 3 * PAD
    for slot in range(slots):
        half = slot % 2
        query = ordered_ref[slot, :, :LANES]
        key = ordered_ref[slot, :, LANES : 2 * LANES]
        value = ordered_ref[slot, :, 2 * LANES : 3 * LANES]
        queries = by_head(query)
        grads = by_head(ordered_ref[slot, :, 3 * LANES :])
        score_ref[half] = dot_nt(queries, key)
        slope_ref[half] = dot_nt(grads, value)
        for start in range(0, heads * WIDE, block):
            at = slice(start, start + block)
            scores = score_ref[half, at, :] * scaling + bias_ref[slot, at, :]
            raised = jnp.exp(scores - jnp.max(scores, axis=1, keepdims=True))
            softened = raised * (1.0 / jnp.sum(raised, axis=1, keepdims=True))
            soft_ref[half, at, :] = softened.astype(BF16)
            slope = slope_ref[half, at, :]
            inner = jnp.sum(softened * slope, axis=1, keepdims=True)
            grad_scores = softened * (slope - inner)
            grad_ref[half, at, :] = grad_scores.astype(BF16)
            exact_ref[half, at, :WIDE] = grad_scores
        for h in range(heads):
            total = jnp.zeros((PAD, SPAN), F32)
            for col in range(WIN_LON):
                by = (WIN_LON - 1 - col) * PAD
                start = h * WIDE + col * PAD
                part = jnp.concatenate(
                    [
                        exact_ref[half, start : start + PAD, :WIDE],
                        jnp.zeros((PAD, SPAN - WIDE), F32),
                    ],
                    axis=1,
                )
                total = total + (part if by == 0 else pltpu.roll(part, by, 1))
            folded_ref[h, slot * PAD : (slot + 1) * PAD, :] = total
        results = (
            own_lanes(dot_nn(grad_ref[half], key)) * scaling,
            dot_tn(grad_ref[half], queries) * scaling,
            dot_tn(soft_ref[half], grads),
            own_lanes(dot_nn(soft_ref[half], value)),
        )
        rows = slice(slot * PAD, (slot + 1) * PAD)
        for c, result in enumerate(results):
            rounded = result.astype(BF16)
            for col in range(WIN_LON):
                given_ref[col, rows, c * LANES : (c + 1) * LANES] = rounded[
                    col * PAD : (col + 1) * PAD, :
                ]
    for col in range(WIN_LON):
        back_ref[col * tall : (col + 1) * tall, :] = dot_tn(order, given_ref[col]).astype(BF16)
    piece = dot_nn(back_ref[:, : 3 * LANES], weights_ref[: 3 * LANES, :])
    group = WIN_LON // 4 * tall
    third = width // 3
    for to in range(n_head):
        lanes = piece[:, to * width : (to + 1) * width]
        for g in range(3):
            tail = lanes[3 * group :, g * third : (g + 1) * third]
            chunk_ref[to, g * group : (g + 1) * group, :] = jnp.concatenate(
                [lanes[g * group : (g + 1) * group, :], tail], axis=1
            ).astype(BF16)
    for step in range(n_head):
        pieces[step][...] = chunk_ref[lax.rem(mine + step, n_head)]


def sums_kernel(shift_ref, x_ref, g_ref, far_ref, back_ref, *refs):
    *halves, sums_ref, own_ref = refs
    lats, cols, levels, _ = x_ref.shape
    width = sums_ref.shape[1]
    for col in range(cols):
        inside, local, taken = column_source(shift_ref[0], col, cols)
        for array, ref in enumerate((x_ref, g_ref)):
            for lat in range(lats):
                start = (col * lats + lat) * levels
                own_ref[array, start : start + levels, :] = jnp.where(
                    inside, ref[lat, local], far_ref[array, lat, taken]
                )
    grads = 3 * LANES
    summed = dot_tn(back_ref[:, :grads], own_ref[0])
    for c in range(3):
        sums_ref[c] = summed[c * LANES : c * LANES + width, :].astype(BF16)
    sums_ref[3] = dot_tn(back_ref[:, grads:], own_ref[1])[:width, :].astype(BF16)
    if halves:
        core = lax.rem(lax.axis_index("lat"), 2)
        for ref, side in zip(halves, (core, 1 - core)):
            for i in range(2):
                ref[i * width : (i + 1) * width, :] = sums_ref[2 * side + i]


def pair_kernel(kept_ref, got_ref, rows_ref, first_ref, second_ref):
    count = rows_ref.shape[0]
    cut = first_ref.shape[0] - count
    total = (kept_ref[...].astype(F32) + got_ref[...].astype(F32)).astype(BF16)
    first_ref[:count, :] = rows_ref[...]
    first_ref[count:, :] = total[:cut, :]
    second_ref[...] = total[cut:, :]


def add_kernel(first_ref, got_first_ref, second_ref, got_second_ref, *outs):
    for out, own, got in zip(outs, (first_ref, second_ref), (got_first_ref, got_second_ref)):
        out[...] = (own[...].astype(F32) + got[...].astype(F32)).astype(BF16)


def merge_kernel(first_ref, got_first_ref, second_ref, got_second_ref, out_ref, sums_ref):
    row = lax.rem(lax.div(lax.axis_index("lat"), 2), 2)
    cut = first_ref.shape[0] - BIAS_ROWS
    share = out_ref.shape[1] - BIAS_ROWS
    out_ref[row, :BIAS_ROWS, :] = first_ref[:BIAS_ROWS, :]
    out_ref[1 - row, :BIAS_ROWS, :] = got_first_ref[:BIAS_ROWS, :]
    sums_ref[:cut, :] = first_ref[BIAS_ROWS:, :].astype(F32) + got_first_ref[
        BIAS_ROWS:, :
    ].astype(F32)
    sums_ref[cut:, :] = second_ref[...].astype(F32) + got_second_ref[...].astype(F32)
    for j in range(2):
        out_ref[j, BIAS_ROWS:, :] = sums_ref[j * share : (j + 1) * share, :].astype(BF16)


def bias_kernel(kind_ref, folded_ref, out_ref, pieces_ref, natural_ref, dense_ref):
    heads, slot_rows, span = folded_ref.shape
    slots = slot_rows // PAD
    number = heads * slots
    rows = folded_ref[...].reshape(heads * slot_rows, span).astype(BF16)
    for level_j in range(WIN_LEVEL):
        moved = dot_nt(rows, offset_order(level_j))
        for t in range(2):
            pieces_ref[2 * level_j + t] = moved[:, t * LANES : (t + 1) * LANES]
    natural_ref[...] = jnp.zeros(natural_ref.shape, F32)
    for place, level_j, start in table_pieces():
        low = start // LANES * LANES
        parts = [
            pieces_ref[2 * level_j + t, pl.ds(place, number, stride=PAD), :] for t in range(2)
        ]
        part = jnp.concatenate(parts + [jnp.zeros((number, LANES), F32)], axis=1)
        if start > low:
            part = pltpu.roll(part, start - low, 1)
        at = (slice(0, number), slice(low, low + 3 * LANES))
        natural_ref[at] = natural_ref[at] + part
    count = WIN_LEVEL * WIN_LEVEL * WIN_LAT * PIECE
    low = count // LANES * LANES
    row, lane = grid_of(number, LANES)
    kind = jnp.zeros((number, LANES), F32)
    for slot in range(slots):
        kind = jnp.where(lax.rem(row, slots) == slot, kind_ref[0, slot].astype(F32), kind)
    at = (slice(0, number), slice(low, low + LANES))
    natural_ref[at] = natural_ref[at] + jnp.where(lane == count - low, kind, 0.0)
    full = low + LANES
    middle = full // 2
    dense_ref[:, :full] = natural_ref[0:8, :full]
    dense_ref[0:4, full:] = natural_ref[8:12, :middle]
    dense_ref[4:8, full:] = natural_ref[8:12, middle:full]
    wide = out_ref.shape[1]
    for j in range(out_ref.shape[0] // 8):
        out_ref[j * 8 : (j + 1) * 8, :] = dense_ref[:, j * wide : (j + 1) * wide].astype(BF16)


def sum_kernel(shift_ref, *refs):
    parts = refs[:-2]
    summed_ref, back_ref = refs[-2:]
    shift = shift_ref[0]
    total = parts[0][...].astype(F32)
    for part in parts[1:]:
        total = total + part[...].astype(F32)
    cols, tall, width = summed_ref.shape
    group = cols // 4
    for g in range(3):
        for i in range(group):
            start = (g * group + i) * tall
            summed_ref[g * group + i] = total[start : start + tall, :width].astype(BF16)
    for i in range(group):
        tails = [
            total[(g * group + i) * tall : (g * group + i + 1) * tall, width:] for g in range(3)
        ]
        summed_ref[3 * group + i] = jnp.concatenate(tails, axis=1).astype(BF16)
    for col in range(HALF):
        source = col - shift + jnp.where(shift <= HALF, WIN_LON, WIN_LON - HALF)
        back_ref[col] = summed_ref[jnp.clip(source, 0, WIN_LON - 1)]


def share_kernel(shares_ref, rows_ref, out_ref):
    total = shares_ref[0].astype(F32)
    for i in range(1, shares_ref.shape[0]):
        total = total + shares_ref[i].astype(F32)
    count = rows_ref.shape[0]
    out_ref[:count, :] = rows_ref[...]
    out_ref[count:, :] = total.astype(BF16)


def finish_kernel(shift_ref, *refs):
    *gathered, summed_ref, returned_ref, feature_ref, attend_ref, output_ref, bias_ref, dense_ref = refs
    if len(gathered) == 1:
        devices, height, wide = gathered[0].shape
        copies = 1

        def entry(i, rows):
            return gathered[0][i, rows, :]
    else:
        devices, height, wide = 4, *gathered[0].shape[1:]
        copies = 2
        core = lax.rem(lax.axis_index("lat"), 2)

        def entry(i, rows):
            mine, other = (ref[i % 2, rows, :] for ref in gathered)
            return jnp.where(core == i // 2, mine, other)

    shift = shift_ref[0]
    low = shift <= HALF
    lats, cols, levels, width = feature_ref.shape
    for col in range(cols):
        own = jnp.logical_xor(low, col < shift)
        source = jnp.where(low, col - shift, col + cols - shift)
        given = jnp.where(low, col, col - (cols - HALF))
        rows = jnp.where(
            own,
            summed_ref[jnp.clip(source, 0, cols - 1)],
            returned_ref[jnp.clip(given, 0, HALF - 1)],
        )
        for lat in range(lats):
            feature_ref[lat, col] = rows[lat * levels : (lat + 1) * levels, :]
    _, types, count = bias_ref.shape
    dense = dense_ref.shape[1] // wide
    share = height - 8 * dense
    for i in range(devices):
        start = i * share
        block = entry(i, slice(8 * dense, height)).astype(F32)
        if start < 3 * width:
            attend_ref[start // width, start % width : start % width + share, :] = block
        else:
            output_ref[start - 3 * width : start - 3 * width + share, :] = block
        for j in range(dense):
            dense_ref[i * 8 : (i + 1) * 8, j * wide : (j + 1) * wide] = entry(
                i, slice(j * 8, (j + 1) * 8)
            )
    full = -(-count // LANES) * LANES
    middle = full // 2
    row, lane = grid_of(devices * 8, types)
    row = lax.bitwise_and(row, 7)
    tag = count - (full - LANES)
    lane = lane.astype(F32) * copies
    kind = dense_ref[:, full - LANES : full].astype(F32)[:, tag : tag + 1]
    for h in range(2):
        mine = (row >= 4 * h) & (row < 4 * h + 4)
        sel = one_hot((kind == lane) & mine)
        bias_ref[h] = dot_tn(sel, dense_ref[:, :full])[:, :count]
    block = dense_ref[:, full + middle - LANES : full + middle].astype(F32)
    below = block[:, tag : tag + 1]
    above = pltpu.roll(block, devices * 8 - 4, 0)[:, tag : tag + 1]
    tail = dense_ref[:, full:]
    bias_ref[2, :, :middle] = dot_tn(one_hot((above == lane) & (row < 4)), tail)
    bias_ref[2, :, middle:] = dot_tn(one_hot((below == lane) & (row >= 4)), tail)[
        :, : count - middle
    ]


def small(mebibytes):
    return pltpu.CompilerParams(vmem_limit_bytes=mebibytes << 20)


def exchange(x, axis, shift, sign):
    count = lax.axis_size(axis)
    ahead = lax.ppermute(x, axis, [(i, (i - sign) % count) for i in range(count)])
    if count == 2:
        return ahead
    behind = lax.ppermute(x, axis, [(i, (i + sign) % count) for i in range(count)])
    return jnp.where(shift[0] <= HALF, ahead, behind)


def per_device(
    features, attend_weight, output_weight, bias_table, bias_type, window_shift, grad_out
):
    levels, lats, cols, depth = features.shape
    slots = levels // WIN_LEVEL
    width, heads = output_weight.shape[0], bias_table.shape[1]
    types, count = bias_table.shape[0], bias_table.shape[2]
    assert lats == WIN_LAT and cols == WIN_LON and levels == 8 and heads * slots == 12
    assert count == WIN_LEVEL * WIN_LEVEL * WIN_LAT * PIECE
    n_head = lax.axis_size("head")
    tall = lats * levels
    number = heads * slots
    shape = jax.ShapeDtypeStruct
    x = features.transpose(1, 2, 0, 3)
    g = grad_out.transpose(1, 2, 0, 3)
    weight = attend_weight.transpose(0, 2, 1)
    table = bias_table.transpose(1, 0, 2)

    def stored(array):
        return pltpu.with_memory_space_constraint(array, pltpu.HBM)

    grid = shape(x.shape, BF16)
    shift, own_x, own_g, projected, rows = pl.pallas_call(
        start_kernel,
        name="start",
        out_shape=[
            shape((1,), jnp.int32),
            grid,
            grid,
            shape((HALF, tall, 4 * width), BF16),
            shape((4 * width, depth), BF16),
        ],
        in_specs=[HBM] * 5,
        out_specs=[SMEM] + [VMEM] * 4,
        scratch_shapes=[pltpu.SemaphoreType.DMA((7,))],
        compiler_params=small(8),
    )(window_shift, stored(x), stored(g), stored(weight), stored(output_weight))
    far = exchange(projected, "lon", shift, 1)
    natural = -(-count // LANES) * LANES + LANES
    prepare = pl.pallas_call(
        prepare_kernel,
        name="prepare",
        out_shape=[
            shape((1, slots), jnp.int32),
            shape((2, lats, HALF, levels, depth), BF16),
            shape((slots, heads * WIDE, WIDE), F32),
            shape((cols, tall, 4 * LANES), BF16),
            shape((4 * LANES, depth), BF16),
        ],
        in_specs=[SMEM] + [VMEM] * 3 + [HBM] * 2,
        out_specs=[SMEM] + [VMEM] * 4,
        scratch_shapes=[
            pltpu.VMEM((number, count), F32),
            pltpu.VMEM((PAD, natural), F32),
            pltpu.VMEM((2 * WIN_LEVEL, number * PAD, LANES), F32),
            pltpu.SemaphoreType.DMA((number + 1,)),
        ],
        compiler_params=small(16),
    )
    kinds, raw, bias, near, weights = prepare(
        shift, own_x, own_g, rows, bias_type.reshape(1, slots), stored(table)
    )
    far_raw = exchange(raw, "lon", shift, 1)
    packed = 3 * (cols // 4) * tall
    *pieces, own_back, folded = pl.pallas_call(
        main_kernel,
        name="main",
        out_shape=[shape((packed, LANES), BF16)] * n_head
        + [
            shape((cols * tall, 4 * LANES), BF16),
            shape((heads, slots * PAD, SPAN), F32),
        ],
        in_specs=[SMEM] + [VMEM] * 4,
        out_specs=[VMEM] * (n_head + 2),
        scratch_shapes=[
            pltpu.VMEM((HALF, tall, 4 * LANES), BF16),
            pltpu.VMEM((slots, WIDE, 4 * LANES), BF16),
            pltpu.VMEM((2, heads * WIDE, WIDE), F32),
            pltpu.VMEM((2, heads * WIDE, WIDE), F32),
            pltpu.VMEM((2, heads * WIDE, WIDE), BF16),
            pltpu.VMEM((2, heads * WIDE, WIDE), BF16),
            pltpu.VMEM((2, heads * WIDE, WIDE), F32),
            pltpu.VMEM((cols, slots * PAD, 4 * LANES), BF16),
            pltpu.VMEM((n_head, packed, LANES), BF16),
        ],
        compiler_params=small(24),
    )(shift, far, near, weights, bias)
    parts = [pieces[0]]
    for step in range(1, n_head):
        ring = [(i, (i + step) % n_head) for i in range(n_head)]
        parts.append(lax.ppermute(pieces[step], "head", ring))
    every = ("lon", "lat")
    n_lon, n_lat = lax.axis_size("lon"), lax.axis_size("lat")
    n_every = n_lon * n_lat
    paired = n_lon == 2 and n_lat == 4
    halves = [shape((2 * width, depth), BF16)] * 2 if paired else []
    *halves, sums = pl.pallas_call(
        sums_kernel,
        name="weight_sums",
        out_shape=halves + [shape((4, width, depth), BF16)],
        in_specs=[SMEM] + [VMEM] * 4,
        out_specs=[VMEM] * (len(halves) + 1),
        scratch_shapes=[pltpu.VMEM((2, cols * tall, depth), BF16)],
        compiler_params=small(8),
    )(shift, own_x, own_g, far_raw, own_back)
    if paired:
        got = lax.ppermute(halves[1], "lat", [(i, i ^ 1) for i in range(n_lat)])
    else:
        shares = sums.reshape(n_every, 4 * width // n_every, depth)
        shares = lax.all_to_all(shares, every, 0, 0)
    full = natural - LANES
    dense = full + full // 2
    assert 8 * dense == BIAS_ROWS * depth
    rows = pl.pallas_call(
        bias_kernel,
        name="bias_rows",
        out_shape=shape((8 * dense // depth, depth), BF16),
        in_specs=[SMEM, VMEM],
        out_specs=VMEM,
        scratch_shapes=[
            pltpu.VMEM((2 * WIN_LEVEL, number * PAD, LANES), F32),
            pltpu.VMEM((PAD, natural), F32),
            pltpu.VMEM((8, dense), F32),
        ],
        compiler_params=small(8),
    )(kinds, folded)
    summed, back = pl.pallas_call(
        sum_kernel,
        name="sum_heads",
        out_shape=[shape((cols, tall, width), BF16), shape((HALF, tall, width), BF16)],
        in_specs=[SMEM] + [VMEM] * n_head,
        out_specs=[VMEM] * 2,
        compiler_params=small(6),
    )(shift, *parts)
    returned = exchange(back, "lon", shift, -1)
    if paired:
        cut = width // 2
        pair_shapes = [
            shape((rows.shape[0] + cut, depth), BF16),
            shape((2 * width - cut, depth), BF16),
        ]
        first, second = pl.pallas_call(
            pair_kernel,
            name="pair",
            out_shape=pair_shapes,
            in_specs=[VMEM] * 3,
            out_specs=[VMEM] * 2,
            compiler_params=small(4),
        )(halves[0], got, rows)

        def across(array, mask):
            ring = [(i, i ^ mask) for i in range(n_every)]
            return lax.ppermute(array, every, ring)

        operands = (first, across(first, n_lat), second, across(second, 2))
        first, second = pl.pallas_call(
            add_kernel,
            name="add",
            out_shape=pair_shapes,
            in_specs=[VMEM] * 4,
            out_specs=[VMEM] * 2,
            compiler_params=small(4),
        )(*operands)
        operands = (first, across(first, 2), second, across(second, n_lat))
        merged = pl.pallas_call(
            merge_kernel,
            name="merge",
            out_shape=shape((2, rows.shape[0] + width, depth), BF16),
            in_specs=[VMEM] * 4,
            out_specs=VMEM,
            scratch_shapes=[pltpu.VMEM((2 * width, depth), F32)],
            compiler_params=small(6),
        )(*operands)
        other = lax.ppermute(merged, "lat", [(i, i ^ 1) for i in range(n_lat)])
        gathered = [merged, other]
    else:
        share = pl.pallas_call(
            share_kernel,
            name="share",
            out_shape=shape((rows.shape[0] + shares.shape[1], depth), BF16),
            in_specs=[VMEM] * 2,
            out_specs=VMEM,
            compiler_params=small(4),
        )(shares, rows)
        gathered = [lax.all_gather(share, every, axis=0)]
    feature_grad, attend_grad, output_grad, bias_grad = pl.pallas_call(
        finish_kernel,
        name="finish",
        out_shape=[
            shape((lats, cols, levels, width), BF16),
            shape((3, width, depth), F32),
            shape((width, depth), F32),
            shape((heads, types, count), F32),
        ],
        in_specs=[SMEM] + [VMEM] * (len(gathered) + 2),
        out_specs=[VMEM] * 4,
        scratch_shapes=[pltpu.VMEM((8 * (4 if paired else n_every), dense), BF16)],
        compiler_params=small(16),
    )(shift, *gathered, summed, returned)
    return (
        feature_grad.transpose(2, 0, 1, 3),
        attend_grad.transpose(0, 2, 1),
        output_grad,
        bias_grad.transpose(1, 0, 2),
    )


def solution(mesh):
    placed = (
        P(None, "lat", "lon", None),
        P(None, None, "head"),
        P("head", None),
        P(None, "head", None),
        P(None, "lat"),
        P(),
        P(None, "lat", "lon", None),
    )
    return jax.shard_map(
        per_device,
        mesh=mesh,
        in_specs=placed,
        out_specs=(
            P(None, "lat", "lon", "head"),
            P(None, None, "head"),
            P("head", None),
            P(None, "head", None),
        ),
        check_vma=False,
    )
```

```python
import jax
import jax.numpy as jnp
from jax import lax
from jax.experimental import pallas as pl
from jax.experimental.pallas import tpu as pltpu
from jax.sharding import PartitionSpec as P


WIN_LEVEL = 2
WIN_LAT = 6
WIN_LON = 12
ROWS = WIN_LEVEL * WIN_LAT
PAD = 16
WIDE = WIN_LON * PAD
HALF = WIN_LON // 2
OFFSETS = 2 * WIN_LON - 1
PIECE = WIN_LAT * OFFSETS
LANES = 128
SPAN = -(-OFFSETS * PAD // LANES) * LANES
BIAS_ROWS = 104
MASKED = -1e30
F32 = jnp.float32
BF16 = jnp.bfloat16
SMEM = pl.BlockSpec(memory_space=pltpu.SMEM)
VMEM = pl.BlockSpec(memory_space=pltpu.VMEM)
HBM = pl.BlockSpec(memory_space=pltpu.HBM)


def dot_nn(a, b):
    return lax.dot_general(a, b, (((1,), (0,)), ((), ())), preferred_element_type=F32)


def dot_nt(a, b):
    return lax.dot_general(a, b, (((1,), (1,)), ((), ())), preferred_element_type=F32)


def dot_tn(a, b):
    return lax.dot_general(a, b, (((0,), (0,)), ((), ())), preferred_element_type=F32)


def grid_of(rows, cols):
    shape = (rows, cols)
    return lax.broadcasted_iota(jnp.int32, shape, 0), lax.broadcasted_iota(jnp.int32, shape, 1)


def one_hot(hit):
    return jnp.where(hit, 1.0, 0.0).astype(BF16)


def window_order(levels):
    row, src = grid_of(levels // WIN_LEVEL * PAD, WIN_LAT * levels)
    bits = levels.bit_length() - 1
    lat = lax.shift_right_logical(src, bits)
    level = lax.bitwise_and(src, levels - 1)
    slot = lax.shift_right_logical(level, 1)
    return one_hot(row == slot * PAD + lax.bitwise_and(level, 1) * WIN_LAT + lat)


def offset_order(level_j):
    src, lane = grid_of(2 * LANES, SPAN)
    back = lax.shift_right_logical(lane, 4)
    lat = lax.bitwise_and(lane, PAD - 1) - level_j * WIN_LAT
    hit = (src == lat * OFFSETS + OFFSETS - 1 - back) & (lat >= 0) & (lat < WIN_LAT)
    return one_hot(hit & (back < OFFSETS))


def table_pieces():
    for level_i in range(WIN_LEVEL):
        for level_j in range(WIN_LEVEL):
            for lat_i in range(WIN_LAT):
                index = (level_i * WIN_LEVEL + level_j) * WIN_LAT + lat_i
                yield level_i * WIN_LAT + lat_i, level_j, index * PIECE


def run_all(copies):
    for copy in copies:
        copy.start()
    for copy in copies:
        copy.wait()


def start_kernel(
    shift_ref, x_ref, g_ref, weight_ref, out_weight_ref,
    moved_ref, own_x_ref, own_g_ref, projected_ref, rows_ref, sems,
):
    lats, _, levels, depth = x_ref.shape
    width = out_weight_ref.shape[0]
    moves = [(shift_ref, moved_ref), (x_ref, own_x_ref), (g_ref, own_g_ref)]
    moves += [(weight_ref.at[c], rows_ref.at[pl.ds(c * width, width)]) for c in range(3)]
    moves.append((out_weight_ref, rows_ref.at[pl.ds(3 * width, width)]))
    run_all([pltpu.make_async_copy(a, b, sems.at[i]) for i, (a, b) in enumerate(moves)])
    base = jnp.where(moved_ref[0] <= HALF, 0, WIN_LON - HALF)
    flat = (lats * HALF * levels, depth)
    projected = jnp.concatenate(
        [
            dot_nt(own_x_ref[:, pl.ds(base, HALF)].reshape(flat), rows_ref[: 3 * width, :]),
            dot_nt(own_g_ref[:, pl.ds(base, HALF)].reshape(flat), rows_ref[3 * width :, :]),
        ],
        axis=1,
    ).astype(BF16)
    for lat in range(lats):
        for col in range(HALF):
            start = (lat * HALF + col) * levels
            projected_ref[col, lat * levels : (lat + 1) * levels, :] = projected[
                start : start + levels, :
            ]


def prepare_kernel(
    shift_ref, x_ref, g_ref, rows_ref, kind_ref, table_ref,
    kinds_ref, raw_ref, bias_ref, near_ref, weights_ref,
    chosen_ref, natural_ref, pieces_ref, sems,
):
    lats, cols, levels, depth = x_ref.shape
    heads = table_ref.shape[0]
    slots = kind_ref.shape[1]
    count = table_ref.shape[2]
    width = rows_ref.shape[0] // 4
    number = heads * slots
    run_all([pltpu.make_async_copy(kind_ref, kinds_ref, sems.at[number])])
    copies = []
    for slot in range(slots):
        for h in range(heads):
            row = h * slots + slot
            source = table_ref.at[h, pl.ds(kinds_ref[0, slot], 1), :]
            target = chosen_ref.at[pl.ds(row, 1), :]
            copies.append(pltpu.make_async_copy(source, target, sems.at[row]))
            copies[-1].start()
    base = jnp.where(shift_ref[0] <= HALF, 0, WIN_LON - HALF)
    raw_ref[0] = x_ref[:, pl.ds(base, HALF)]
    raw_ref[1] = g_ref[:, pl.ds(base, HALF)]
    for c in range(4):
        weights_ref[c * LANES : c * LANES + width, :] = rows_ref[c * width : (c + 1) * width, :]
        weights_ref[c * LANES + width : (c + 1) * LANES, :] = jnp.zeros(
            (LANES - width, depth), BF16
        )
    flat = (lats * cols * levels, depth)
    projected = project(x_ref[...].reshape(flat), g_ref[...].reshape(flat), weights_ref[...])
    for lat in range(lats):
        for col in range(cols):
            start = (lat * cols + col) * levels
            near_ref[col, lat * levels : (lat + 1) * levels, :] = projected[
                start : start + levels, :
            ].astype(BF16)
    natural_ref[...] = jnp.zeros(natural_ref.shape, F32)
    pieces_ref[...] = jnp.zeros(pieces_ref.shape, F32)
    for copy in copies:
        copy.wait()
    natural_ref[:number, :count] = chosen_ref[...]
    for place, level_j, start in table_pieces():
        low = start // LANES * LANES
        block = natural_ref[:, low : low + 3 * LANES]
        if start > low:
            block = pltpu.roll(block, 3 * LANES - (start - low), 1)
        for t in range(2):
            pieces_ref[2 * level_j + t, pl.ds(place, number, stride=PAD), :] = block[
                :number, t * LANES : (t + 1) * LANES
            ]
    turned = jnp.zeros((number * PAD, SPAN), F32)
    for level_j in range(WIN_LEVEL):
        order = offset_order(level_j)
        rest = jnp.concatenate([pieces_ref[2 * level_j], pieces_ref[2 * level_j + 1]], axis=1)
        for _ in range(3):
            part = rest.astype(BF16)
            turned = turned + dot_nn(part, order)
            rest = rest - part.astype(F32)
    lane = lax.broadcasted_iota(jnp.int32, turned.shape, 1)
    turned = jnp.where(lax.bitwise_and(lane, PAD - 1) < ROWS, turned, MASKED)
    for h in range(heads):
        for slot in range(slots):
            row = (h * slots + slot) * PAD
            table = turned[row : row + PAD, :]
            for col in range(WIN_LON):
                by = (WIN_LON - 1 - col) * PAD
                moved = table if by == 0 else pltpu.roll(table, SPAN - by, 1)
                start = h * WIDE + col * PAD
                bias_ref[slot, start : start + PAD, :] = moved[:, :WIDE]


def project(rows_x, rows_g, weights):
    width = 3 * LANES
    return jnp.concatenate(
        [dot_nt(rows_x, weights[:width]), dot_nt(rows_g, weights[width:])], axis=1
    )


def column_source(shift, col, cols):
    low = shift <= HALF
    at = col + shift
    inside = jnp.logical_xor(low, at >= cols)
    local = jnp.where(at >= cols, at - cols, at)
    taken = jnp.where(low, at - cols, at - (cols - HALF))
    return inside, local, jnp.clip(taken, 0, HALF - 1)


def main_kernel(shift_ref, far_ref, near_ref, weights_ref, bias_ref, *rest):
    n_head = lax.axis_size("head")
    pieces = rest[:n_head]
    back_ref, folded_ref = rest[n_head : n_head + 2]
    (
        beyond_ref, ordered_ref, score_ref, slope_ref, soft_ref, grad_ref, exact_ref, given_ref,
        chunk_ref,
    ) = rest[n_head + 2 :]
    cols, tall, _ = near_ref.shape
    levels = tall // WIN_LAT
    slots = bias_ref.shape[0]
    heads = bias_ref.shape[1] // WIDE
    width = far_ref.shape[2] // 4
    size = width // heads
    scaling = size ** (-0.5)
    mine = lax.axis_index("head")
    shift = shift_ref[0]
    for c in range(4):
        beyond_ref[:, :, c * LANES : c * LANES + width] = far_ref[
            :, :, c * width : (c + 1) * width
        ]
        beyond_ref[:, :, c * LANES + width : (c + 1) * LANES] = jnp.zeros(
            (HALF, tall, LANES - width), BF16
        )
    order = window_order(levels)
    for col in range(cols):
        inside, local, taken = column_source(shift, col, cols)
        rows = jnp.where(inside, near_ref[local], beyond_ref[taken])
        ordered = dot_nn(order, rows).astype(BF16)
        for slot in range(slots):
            ordered_ref[slot, col * PAD : (col + 1) * PAD, :] = ordered[
                slot * PAD : (slot + 1) * PAD, :
            ]
    lane = lax.broadcasted_iota(jnp.int32, (WIDE, LANES), 1)
    masks = [(lane >= h * size) & (lane < (h + 1) * size) for h in range(heads)]
    none = jnp.zeros((WIDE, LANES), BF16)

    def by_head(array):
        return jnp.concatenate([jnp.where(mask, array, none) for mask in masks], axis=0)

    def own_lanes(array):
        total = jnp.where(masks[0], array[:WIDE, :], 0.0)
        for h in range(1, heads):
            total = jnp.where(masks[h], array[h * WIDE : (h + 1) * WIDE, :], total)
        return total

    block = 3 * PAD
    for slot in range(slots):
        half = slot % 2
        query = ordered_ref[slot, :, :LANES]
        key = ordered_ref[slot, :, LANES : 2 * LANES]
        value = ordered_ref[slot, :, 2 * LANES : 3 * LANES]
        queries = by_head(query)
        grads = by_head(ordered_ref[slot, :, 3 * LANES :])
        score_ref[half] = dot_nt(queries, key)
        slope_ref[half] = dot_nt(grads, value)
        for start in range(0, heads * WIDE, block):
            at = slice(start, start + block)
            scores = score_ref[half, at, :] * scaling + bias_ref[slot, at, :]
            raised = jnp.exp(scores - jnp.max(scores, axis=1, keepdims=True))
            softened = raised * (1.0 / jnp.sum(raised, axis=1, keepdims=True))
            soft_ref[half, at, :] = softened.astype(BF16)
            slope = slope_ref[half, at, :]
            inner = jnp.sum(softened * slope, axis=1, keepdims=True)
            grad_scores = softened * (slope - inner)
            grad_ref[half, at, :] = grad_scores.astype(BF16)
            exact_ref[half, at, :WIDE] = grad_scores
        for h in range(heads):
            total = jnp.zeros((PAD, SPAN), F32)
            apart = LANES // PAD
            for col in range(apart):
                low = h * WIDE + col * PAD
                part = exact_ref[half, low : low + PAD, :WIDE]
                by = (WIN_LON - 1 - col) * PAD
                rest = jnp.zeros((PAD, SPAN - WIDE), F32)
                if col + apart < WIN_LON:
                    by = by - LANES
                    high = low + apart * PAD
                    twin = exact_ref[half, high : high + PAD, :WIDE]
                    moved = jnp.concatenate([rest[:, :LANES], part, rest[:, LANES:]], axis=1)
                    part = moved + jnp.concatenate([twin, rest], axis=1)
                else:
                    part = jnp.concatenate([part, rest], axis=1)
                total = total + (part if by == 0 else pltpu.roll(part, by, 1))
            folded_ref[h, slot * PAD : (slot + 1) * PAD, :] = total
        results = (
            own_lanes(dot_nn(grad_ref[half], key)) * scaling,
            dot_tn(grad_ref[half], queries) * scaling,
            dot_tn(soft_ref[half], grads),
            own_lanes(dot_nn(soft_ref[half], value)),
        )
        rows = slice(slot * PAD, (slot + 1) * PAD)
        for c, result in enumerate(results):
            rounded = result.astype(BF16)
            for col in range(WIN_LON):
                given_ref[col, rows, c * LANES : (c + 1) * LANES] = rounded[
                    col * PAD : (col + 1) * PAD, :
                ]
    for col in range(WIN_LON):
        back_ref[col * tall : (col + 1) * tall, :] = dot_tn(order, given_ref[col]).astype(BF16)
    piece = dot_nn(back_ref[:, : 3 * LANES], weights_ref[: 3 * LANES, :])
    group = WIN_LON // 4 * tall
    third = width // 3
    for to in range(n_head):
        lanes = piece[:, to * width : (to + 1) * width]
        for g in range(3):
            tail = lanes[3 * group :, g * third : (g + 1) * third]
            chunk_ref[to, g * group : (g + 1) * group, :] = jnp.concatenate(
                [lanes[g * group : (g + 1) * group, :], tail], axis=1
            ).astype(BF16)
    for step in range(n_head):
        pieces[step][...] = chunk_ref[lax.rem(mine + step, n_head)]


def sums_kernel(shift_ref, x_ref, g_ref, far_ref, back_ref, *refs):
    *halves, sums_ref, own_ref = refs
    lats, cols, levels, _ = x_ref.shape
    width = sums_ref.shape[1]
    for col in range(cols):
        inside, local, taken = column_source(shift_ref[0], col, cols)
        for array, ref in enumerate((x_ref, g_ref)):
            for lat in range(lats):
                start = (col * lats + lat) * levels
                own_ref[array, start : start + levels, :] = jnp.where(
                    inside, ref[lat, local], far_ref[array, lat, taken]
                )
    grads = 3 * LANES
    summed = dot_tn(back_ref[:, :grads], own_ref[0])
    for c in range(3):
        sums_ref[c] = summed[c * LANES : c * LANES + width, :].astype(BF16)
    sums_ref[3] = dot_tn(back_ref[:, grads:], own_ref[1])[:width, :].astype(BF16)
    if halves:
        core = lax.rem(lax.axis_index("lat"), 2)
        for ref, side in zip(halves, (core, 1 - core)):
            for i in range(2):
                ref[i * width : (i + 1) * width, :] = sums_ref[2 * side + i]


def pair_kernel(kept_ref, got_ref, rows_ref, first_ref, second_ref):
    count = rows_ref.shape[0]
    cut = first_ref.shape[0] - count
    total = (kept_ref[...].astype(F32) + got_ref[...].astype(F32)).astype(BF16)
    first_ref[:count, :] = rows_ref[...]
    first_ref[count:, :] = total[:cut, :]
    second_ref[...] = total[cut:, :]


def add_kernel(first_ref, got_first_ref, second_ref, got_second_ref, *outs):
    for out, own, got in zip(outs, (first_ref, second_ref), (got_first_ref, got_second_ref)):
        out[...] = (own[...].astype(F32) + got[...].astype(F32)).astype(BF16)


def merge_kernel(first_ref, got_first_ref, second_ref, got_second_ref, out_ref, sums_ref):
    row = lax.rem(lax.div(lax.axis_index("lat"), 2), 2)
    cut = first_ref.shape[0] - BIAS_ROWS
    share = out_ref.shape[1] - BIAS_ROWS
    out_ref[row, :BIAS_ROWS, :] = first_ref[:BIAS_ROWS, :]
    out_ref[1 - row, :BIAS_ROWS, :] = got_first_ref[:BIAS_ROWS, :]
    sums_ref[:cut, :] = first_ref[BIAS_ROWS:, :].astype(F32) + got_first_ref[
        BIAS_ROWS:, :
    ].astype(F32)
    sums_ref[cut:, :] = second_ref[...].astype(F32) + got_second_ref[...].astype(F32)
    for j in range(2):
        out_ref[j, BIAS_ROWS:, :] = sums_ref[j * share : (j + 1) * share, :].astype(BF16)


def bias_kernel(kind_ref, folded_ref, out_ref, pieces_ref, natural_ref, dense_ref):
    heads, slot_rows, span = folded_ref.shape
    slots = slot_rows // PAD
    number = heads * slots
    rows = folded_ref[...].reshape(heads * slot_rows, span).astype(BF16)
    for level_j in range(WIN_LEVEL):
        moved = dot_nt(rows, offset_order(level_j))
        for t in range(2):
            pieces_ref[2 * level_j + t] = moved[:, t * LANES : (t + 1) * LANES]
    natural_ref[...] = jnp.zeros(natural_ref.shape, F32)
    for place, level_j, start in table_pieces():
        low = start // LANES * LANES
        parts = [
            pieces_ref[2 * level_j + t, pl.ds(place, number, stride=PAD), :] for t in range(2)
        ]
        part = jnp.concatenate(parts + [jnp.zeros((number, LANES), F32)], axis=1)
        if start > low:
            part = pltpu.roll(part, start - low, 1)
        at = (slice(0, number), slice(low, low + 3 * LANES))
        natural_ref[at] = natural_ref[at] + part
    count = WIN_LEVEL * WIN_LEVEL * WIN_LAT * PIECE
    low = count // LANES * LANES
    row, lane = grid_of(number, LANES)
    kind = jnp.zeros((number, LANES), F32)
    for slot in range(slots):
        kind = jnp.where(lax.rem(row, slots) == slot, kind_ref[0, slot].astype(F32), kind)
    at = (slice(0, number), slice(low, low + LANES))
    natural_ref[at] = natural_ref[at] + jnp.where(lane == count - low, kind, 0.0)
    full = low + LANES
    middle = full // 2
    dense_ref[:, :full] = natural_ref[0:8, :full]
    dense_ref[0:4, full:] = natural_ref[8:12, :middle]
    dense_ref[4:8, full:] = natural_ref[8:12, middle:full]
    wide = out_ref.shape[1]
    for j in range(out_ref.shape[0] // 8):
        out_ref[j * 8 : (j + 1) * 8, :] = dense_ref[:, j * wide : (j + 1) * wide].astype(BF16)


def sum_kernel(shift_ref, *refs):
    parts = refs[:-2]
    summed_ref, back_ref = refs[-2:]
    shift = shift_ref[0]
    total = parts[0][...].astype(F32)
    for part in parts[1:]:
        total = total + part[...].astype(F32)
    cols, tall, width = summed_ref.shape
    group = cols // 4
    for g in range(3):
        for i in range(group):
            start = (g * group + i) * tall
            summed_ref[g * group + i] = total[start : start + tall, :width].astype(BF16)
    for i in range(group):
        tails = [
            total[(g * group + i) * tall : (g * group + i + 1) * tall, width:] for g in range(3)
        ]
        summed_ref[3 * group + i] = jnp.concatenate(tails, axis=1).astype(BF16)
    for col in range(HALF):
        source = col - shift + jnp.where(shift <= HALF, WIN_LON, WIN_LON - HALF)
        back_ref[col] = summed_ref[jnp.clip(source, 0, WIN_LON - 1)]


def share_kernel(shares_ref, rows_ref, out_ref):
    total = shares_ref[0].astype(F32)
    for i in range(1, shares_ref.shape[0]):
        total = total + shares_ref[i].astype(F32)
    count = rows_ref.shape[0]
    out_ref[:count, :] = rows_ref[...]
    out_ref[count:, :] = total.astype(BF16)


def finish_kernel(shift_ref, *refs):
    *gathered, summed_ref, returned_ref, feature_ref, attend_ref, output_ref, bias_ref, dense_ref = refs
    if len(gathered) == 1:
        devices, height, wide = gathered[0].shape
        copies = 1

        def entry(i, rows):
            return gathered[0][i, rows, :]
    else:
        devices, height, wide = 4, *gathered[0].shape[1:]
        copies = 2
        core = lax.rem(lax.axis_index("lat"), 2)

        def entry(i, rows):
            mine, other = (ref[i % 2, rows, :] for ref in gathered)
            return jnp.where(core == i // 2, mine, other)

    shift = shift_ref[0]
    low = shift <= HALF
    lats, cols, levels, width = feature_ref.shape
    for col in range(cols):
        own = jnp.logical_xor(low, col < shift)
        source = jnp.where(low, col - shift, col + cols - shift)
        given = jnp.where(low, col, col - (cols - HALF))
        rows = jnp.where(
            own,
            summed_ref[jnp.clip(source, 0, cols - 1)],
            returned_ref[jnp.clip(given, 0, HALF - 1)],
        )
        for lat in range(lats):
            feature_ref[lat, col] = rows[lat * levels : (lat + 1) * levels, :]
    _, types, count = bias_ref.shape
    dense = dense_ref.shape[1] // wide
    share = height - 8 * dense
    for i in range(devices):
        start = i * share
        block = entry(i, slice(8 * dense, height)).astype(F32)
        if start < 3 * width:
            attend_ref[start // width, start % width : start % width + share, :] = block
        else:
            output_ref[start - 3 * width : start - 3 * width + share, :] = block
        for j in range(dense):
            dense_ref[i * 8 : (i + 1) * 8, j * wide : (j + 1) * wide] = entry(
                i, slice(j * 8, (j + 1) * 8)
            )
    full = -(-count // LANES) * LANES
    middle = full // 2
    row, lane = grid_of(devices * 8, types)
    row = lax.bitwise_and(row, 7)
    tag = count - (full - LANES)
    lane = lane.astype(F32) * copies
    kind = dense_ref[:, full - LANES : full].astype(F32)[:, tag : tag + 1]
    for h in range(2):
        mine = (row >= 4 * h) & (row < 4 * h + 4)
        sel = one_hot((kind == lane) & mine)
        bias_ref[h] = dot_tn(sel, dense_ref[:, :full])[:, :count]
    block = dense_ref[:, full + middle - LANES : full + middle].astype(F32)
    below = block[:, tag : tag + 1]
    above = pltpu.roll(block, devices * 8 - 4, 0)[:, tag : tag + 1]
    tail = dense_ref[:, full:]
    bias_ref[2, :, :middle] = dot_tn(one_hot((above == lane) & (row < 4)), tail)
    bias_ref[2, :, middle:] = dot_tn(one_hot((below == lane) & (row >= 4)), tail)[
        :, : count - middle
    ]


def small(mebibytes):
    return pltpu.CompilerParams(vmem_limit_bytes=mebibytes << 20)


def exchange(x, axis, shift, sign):
    count = lax.axis_size(axis)
    ahead = lax.ppermute(x, axis, [(i, (i - sign) % count) for i in range(count)])
    if count == 2:
        return ahead
    behind = lax.ppermute(x, axis, [(i, (i + sign) % count) for i in range(count)])
    return jnp.where(shift[0] <= HALF, ahead, behind)


def per_device(
    features, attend_weight, output_weight, bias_table, bias_type, window_shift, grad_out
):
    levels, lats, cols, depth = features.shape
    slots = levels // WIN_LEVEL
    width, heads = output_weight.shape[0], bias_table.shape[1]
    types, count = bias_table.shape[0], bias_table.shape[2]
    assert lats == WIN_LAT and cols == WIN_LON and levels == 8 and heads * slots == 12
    assert count == WIN_LEVEL * WIN_LEVEL * WIN_LAT * PIECE
    n_head = lax.axis_size("head")
    tall = lats * levels
    number = heads * slots
    shape = jax.ShapeDtypeStruct
    x = features.transpose(1, 2, 0, 3)
    g = grad_out.transpose(1, 2, 0, 3)
    weight = attend_weight.transpose(0, 2, 1)
    table = bias_table.transpose(1, 0, 2)

    def stored(array):
        return pltpu.with_memory_space_constraint(array, pltpu.HBM)

    grid = shape(x.shape, BF16)
    shift, own_x, own_g, projected, rows = pl.pallas_call(
        start_kernel,
        name="start",
        out_shape=[
            shape((1,), jnp.int32),
            grid,
            grid,
            shape((HALF, tall, 4 * width), BF16),
            shape((4 * width, depth), BF16),
        ],
        in_specs=[HBM] * 5,
        out_specs=[SMEM] + [VMEM] * 4,
        scratch_shapes=[pltpu.SemaphoreType.DMA((7,))],
        compiler_params=small(8),
    )(window_shift, stored(x), stored(g), stored(weight), stored(output_weight))
    far = exchange(projected, "lon", shift, 1)
    natural = -(-count // LANES) * LANES + LANES
    prepare = pl.pallas_call(
        prepare_kernel,
        name="prepare",
        out_shape=[
            shape((1, slots), jnp.int32),
            shape((2, lats, HALF, levels, depth), BF16),
            shape((slots, heads * WIDE, WIDE), F32),
            shape((cols, tall, 4 * LANES), BF16),
            shape((4 * LANES, depth), BF16),
        ],
        in_specs=[SMEM] + [VMEM] * 3 + [HBM] * 2,
        out_specs=[SMEM] + [VMEM] * 4,
        scratch_shapes=[
            pltpu.VMEM((number, count), F32),
            pltpu.VMEM((PAD, natural), F32),
            pltpu.VMEM((2 * WIN_LEVEL, number * PAD, LANES), F32),
            pltpu.SemaphoreType.DMA((number + 1,)),
        ],
        compiler_params=small(16),
    )
    kinds, raw, bias, near, weights = prepare(
        shift, own_x, own_g, rows, bias_type.reshape(1, slots), stored(table)
    )
    far_raw = exchange(raw, "lon", shift, 1)
    packed = 3 * (cols // 4) * tall
    *pieces, own_back, folded = pl.pallas_call(
        main_kernel,
        name="main",
        out_shape=[shape((packed, LANES), BF16)] * n_head
        + [
            shape((cols * tall, 4 * LANES), BF16),
            shape((heads, slots * PAD, SPAN), F32),
        ],
        in_specs=[SMEM] + [VMEM] * 4,
        out_specs=[VMEM] * (n_head + 2),
        scratch_shapes=[
            pltpu.VMEM((HALF, tall, 4 * LANES), BF16),
            pltpu.VMEM((slots, WIDE, 4 * LANES), BF16),
            pltpu.VMEM((2, heads * WIDE, WIDE), F32),
            pltpu.VMEM((2, heads * WIDE, WIDE), F32),
            pltpu.VMEM((2, heads * WIDE, WIDE), BF16),
            pltpu.VMEM((2, heads * WIDE, WIDE), BF16),
            pltpu.VMEM((2, heads * WIDE, WIDE), F32),
            pltpu.VMEM((cols, slots * PAD, 4 * LANES), BF16),
            pltpu.VMEM((n_head, packed, LANES), BF16),
        ],
        compiler_params=small(24),
    )(shift, far, near, weights, bias)
    parts = [pieces[0]]
    for step in range(1, n_head):
        ring = [(i, (i + step) % n_head) for i in range(n_head)]
        parts.append(lax.ppermute(pieces[step], "head", ring))
    every = ("lon", "lat")
    n_lon, n_lat = lax.axis_size("lon"), lax.axis_size("lat")
    n_every = n_lon * n_lat
    paired = n_lon == 2 and n_lat == 4
    halves = [shape((2 * width, depth), BF16)] * 2 if paired else []
    *halves, sums = pl.pallas_call(
        sums_kernel,
        name="weight_sums",
        out_shape=halves + [shape((4, width, depth), BF16)],
        in_specs=[SMEM] + [VMEM] * 4,
        out_specs=[VMEM] * (len(halves) + 1),
        scratch_shapes=[pltpu.VMEM((2, cols * tall, depth), BF16)],
        compiler_params=small(8),
    )(shift, own_x, own_g, far_raw, own_back)
    if paired:
        got = lax.ppermute(halves[1], "lat", [(i, i ^ 1) for i in range(n_lat)])
    else:
        shares = sums.reshape(n_every, 4 * width // n_every, depth)
        shares = lax.all_to_all(shares, every, 0, 0)
    full = natural - LANES
    dense = full + full // 2
    assert 8 * dense == BIAS_ROWS * depth
    rows = pl.pallas_call(
        bias_kernel,
        name="bias_rows",
        out_shape=shape((8 * dense // depth, depth), BF16),
        in_specs=[SMEM, VMEM],
        out_specs=VMEM,
        scratch_shapes=[
            pltpu.VMEM((2 * WIN_LEVEL, number * PAD, LANES), F32),
            pltpu.VMEM((PAD, natural), F32),
            pltpu.VMEM((8, dense), F32),
        ],
        compiler_params=small(8),
    )(kinds, folded)
    summed, back = pl.pallas_call(
        sum_kernel,
        name="sum_heads",
        out_shape=[shape((cols, tall, width), BF16), shape((HALF, tall, width), BF16)],
        in_specs=[SMEM] + [VMEM] * n_head,
        out_specs=[VMEM] * 2,
        compiler_params=small(6),
    )(shift, *parts)
    returned = exchange(back, "lon", shift, -1)
    if paired:
        cut = width // 2
        pair_shapes = [
            shape((rows.shape[0] + cut, depth), BF16),
            shape((2 * width - cut, depth), BF16),
        ]
        first, second = pl.pallas_call(
            pair_kernel,
            name="pair",
            out_shape=pair_shapes,
            in_specs=[VMEM] * 3,
            out_specs=[VMEM] * 2,
            compiler_params=small(4),
        )(halves[0], got, rows)

        def across(array, mask):
            ring = [(i, i ^ mask) for i in range(n_every)]
            return lax.ppermute(array, every, ring)

        operands = (first, across(first, n_lat), second, across(second, 2))
        first, second = pl.pallas_call(
            add_kernel,
            name="add",
            out_shape=pair_shapes,
            in_specs=[VMEM] * 4,
            out_specs=[VMEM] * 2,
            compiler_params=small(4),
        )(*operands)
        operands = (first, across(first, 2), second, across(second, n_lat))
        merged = pl.pallas_call(
            merge_kernel,
            name="merge",
            out_shape=shape((2, rows.shape[0] + width, depth), BF16),
            in_specs=[VMEM] * 4,
            out_specs=VMEM,
            scratch_shapes=[pltpu.VMEM((2 * width, depth), F32)],
            compiler_params=small(6),
        )(*operands)
        other = lax.ppermute(merged, "lat", [(i, i ^ 1) for i in range(n_lat)])
        gathered = [merged, other]
    else:
        share = pl.pallas_call(
            share_kernel,
            name="share",
            out_shape=shape((rows.shape[0] + shares.shape[1], depth), BF16),
            in_specs=[VMEM] * 2,
            out_specs=VMEM,
            compiler_params=small(4),
        )(shares, rows)
        gathered = [lax.all_gather(share, every, axis=0)]
    feature_grad, attend_grad, output_grad, bias_grad = pl.pallas_call(
        finish_kernel,
        name="finish",
        out_shape=[
            shape((lats, cols, levels, width), BF16),
            shape((3, width, depth), F32),
            shape((width, depth), F32),
            shape((heads, types, count), F32),
        ],
        in_specs=[SMEM] + [VMEM] * (len(gathered) + 2),
        out_specs=[VMEM] * 4,
        scratch_shapes=[pltpu.VMEM((8 * (4 if paired else n_every), dense), BF16)],
        compiler_params=small(16),
    )(shift, *gathered, summed, returned)
    return (
        feature_grad.transpose(2, 0, 1, 3),
        attend_grad.transpose(0, 2, 1),
        output_grad,
        bias_grad.transpose(1, 0, 2),
    )


def solution(mesh):
    placed = (
        P(None, "lat", "lon", None),
        P(None, None, "head"),
        P("head", None),
        P(None, "head", None),
        P(None, "lat"),
        P(),
        P(None, "lat", "lon", None),
    )
    return jax.shard_map(
        per_device,
        mesh=mesh,
        in_specs=placed,
        out_specs=(
            P(None, "lat", "lon", "head"),
            P(None, None, "head"),
            P("head", None),
            P(None, "head", None),
        ),
        check_vma=False,
    )
```
